32 devices in a mesh: dp: 1 (over z), ep: 32 (over y, x, core).
Axes of the slice: x: 4, y: 4, z: 1, core: 2. Of those that a mesh axis runs over, the one named last changes fastest.
The devices are a block of a 4x4x8 slice.
Arguments:
- x_disp: bfloat16 [32, 64, 48, 1536], P('dp', 'ep')
- w_gate: bfloat16 [64, 1536, 512], P('ep')
- w_up: bfloat16 [64, 1536, 512], P('ep')
- w_down: bfloat16 [64, 512, 1536], P('ep')
- d_out: bfloat16 [8192, 1536], P(('dp', 'ep'))
- slot_idx: int32 [8192, 6], P(('dp', 'ep'))
- expert_id: int32 [8192, 6], P(('dp', 'ep'))
- gate_wt: float32 [8192, 6], P(('dp', 'ep'))
Outputs:
- output 1: bfloat16 [32, 64, 48, 1536], P('dp', 'ep')
- output 2: bfloat16 [64, 1536, 512], P(('dp', 'ep'))
- output 3: bfloat16 [64, 1536, 512], P(('dp', 'ep'))
- output 4: bfloat16 [64, 512, 1536], P(('dp', 'ep'))
- output 5: float32 [8192, 6], P(('dp', 'ep'))
All inputs are finite; a program needn't handle non-finite values.
Results may differ from the reference program's by a relative error of at most 0.001.
Values are sent between devices in bfloat16 or wider.
A program may use at most 768 MiB of HBM per device.

```python
import jax
import jax.numpy as jnp
from jax import lax

GROUP_SIZE = 32
TOK_DEV = 256
TOP_K = 6
EXPERTS = 64
MODEL_DIM = 1536
FFN_DIM = 512
CAPACITY = 48

TOKENS = GROUP_SIZE * TOK_DEV
SLOT_COUNT = EXPERTS * CAPACITY
PER_SOURCE = TOK_DEV * TOP_K


def draw_routes(key):
    key_noise, key_tilt, key_hot = jax.random.split(key, 3)
    noise_int = jax.random.randint(key_noise, (TOKENS, EXPERTS), 0, 4096)
    tilt_int = jax.random.permutation(key_tilt, EXPERTS) * (1024 // EXPERTS)
    hot_expert = jax.random.randint(key_hot, (), 0, EXPERTS)
    expert_ids = jnp.arange(EXPERTS)[None, :]
    even_tok = (jnp.arange(TOKENS) % 2 == 0)[:, None]
    bonus_int = jnp.where(even_tok & (expert_ids == hot_expert), 1048576, 0)
    scores = (noise_int + tilt_int[None, :] + bonus_int) * EXPERTS + expert_ids
    expert_id = lax.top_k(scores, TOP_K)[1].astype(jnp.int32)
    picked = jnp.zeros((TOKENS, EXPERTS), jnp.int32).at[jnp.arange(TOKENS)[:, None], expert_id].add(1)
    picked = picked.reshape(GROUP_SIZE, TOK_DEV, EXPERTS)
    earlier = jnp.cumsum(picked, axis=1) - picked
    order_pos = jnp.take_along_axis(earlier, expert_id.reshape(GROUP_SIZE, TOK_DEV, TOP_K), axis=2)
    slot_idx = jnp.where(order_pos < CAPACITY, order_pos, -1).reshape(TOKENS, TOP_K).astype(jnp.int32)
    return slot_idx, expert_id


def setup_inputs(seed: int = 0, part: int = 0) -> dict:
    base_key = jax.random.key(seed)
    part_key = jax.random.fold_in(base_key, part)
    key_x, key_out, key_gate, key_route = jax.random.split(part_key, 4)
    key_wg, key_wu, key_wd = jax.random.split(jax.random.key(seed + 1), 3)
    x_disp = jax.random.normal(key_x, (GROUP_SIZE, EXPERTS, CAPACITY, MODEL_DIM), jnp.float32).astype(jnp.bfloat16)
    w_gate = (jax.random.normal(key_wg, (EXPERTS, MODEL_DIM, FFN_DIM), jnp.float32) * MODEL_DIM ** -0.5).astype(jnp.bfloat16)
    w_up = (jax.random.normal(key_wu, (EXPERTS, MODEL_DIM, FFN_DIM), jnp.float32) * MODEL_DIM ** -0.5).astype(jnp.bfloat16)
    w_down = (jax.random.normal(key_wd, (EXPERTS, FFN_DIM, MODEL_DIM), jnp.float32) * FFN_DIM ** -0.5).astype(jnp.bfloat16)
    d_out = jax.random.normal(key_out, (TOKENS, MODEL_DIM), jnp.float32).astype(jnp.bfloat16)
    slot_idx, expert_id = draw_routes(key_route)
    gate_wt = jax.random.uniform(key_gate, (TOKENS, TOP_K), jnp.float32, 0.05, 1.0)
    return {'x_disp': x_disp, 'w_gate': w_gate, 'w_up': w_up, 'w_down': w_down, 'd_out': d_out, 'slot_idx': slot_idx, 'expert_id': expert_id, 'gate_wt': gate_wt}


def one_expert(operands):
    x_rows, out_rows, d_slot, w_gate, w_up, w_down = operands
    pre_gate = jnp.dot(x_rows, w_gate, preferred_element_type=jnp.float32)
    pre_up = jnp.dot(x_rows, w_up, preferred_element_type=jnp.float32)
    gate_sig = jax.nn.sigmoid(pre_gate)
    silu_gate = pre_gate * gate_sig
    hidden = (silu_gate * pre_up).astype(jnp.bfloat16)
    y_rows = jnp.dot(hidden, w_down, preferred_element_type=jnp.float32).astype(jnp.bfloat16)
    grad_hidden = jnp.dot(d_slot, w_down.T, preferred_element_type=jnp.float32).astype(jnp.bfloat16).astype(jnp.float32)
    grad_pre_gate = (grad_hidden * pre_up * gate_sig * (1.0 + pre_gate * (1.0 - gate_sig))).astype(jnp.bfloat16)
    grad_pre_up = (grad_hidden * silu_gate).astype(jnp.bfloat16)
    grad_x = (jnp.dot(grad_pre_gate, w_gate.T, preferred_element_type=jnp.float32) + jnp.dot(grad_pre_up, w_up.T, preferred_element_type=jnp.float32)).astype(jnp.bfloat16)
    grad_w_gate = jnp.dot(x_rows.T, grad_pre_gate, preferred_element_type=jnp.float32).astype(jnp.bfloat16)
    grad_w_up = jnp.dot(x_rows.T, grad_pre_up, preferred_element_type=jnp.float32).astype(jnp.bfloat16)
    grad_w_down = jnp.dot(hidden.T, d_slot, preferred_element_type=jnp.float32).astype(jnp.bfloat16)
    gate_grad_rows = jnp.sum(out_rows.astype(jnp.float32) * y_rows.astype(jnp.float32), axis=1)
    return grad_x, grad_w_gate, grad_w_up, grad_w_down, gate_grad_rows


def by_expert(arr):
    return jnp.moveaxis(arr.reshape(GROUP_SIZE, EXPERTS, CAPACITY, MODEL_DIM), 1, 0).reshape(EXPERTS, GROUP_SIZE * CAPACITY, MODEL_DIM)


def owners(pos_row):
    return jnp.full((SLOT_COUNT,), PER_SOURCE, jnp.int32).at[pos_row].set(jnp.arange(PER_SOURCE, dtype=jnp.int32), mode='drop')


def pick_rows(tok_rows, gate_row, owner_row):
    rows_out = jnp.take(tok_rows, owner_row // TOP_K, axis=0, mode='fill', fill_value=0)
    gates_out = jnp.take(gate_row, owner_row, mode='fill', fill_value=0)
    return rows_out, gates_out


def take_fill(values, index_row):
    return jnp.take(values, index_row, mode='fill', fill_value=0)


def reference(x_disp, w_gate, w_up, w_down, d_out, slot_idx, expert_id, gate_wt):
    flat_pos = jnp.where(slot_idx >= 0, expert_id * CAPACITY + slot_idx, SLOT_COUNT).reshape(GROUP_SIZE, PER_SOURCE)
    owner_ids = jax.vmap(owners)(flat_pos)
    out_rows, gate_rows = jax.vmap(pick_rows)(d_out.reshape(GROUP_SIZE, TOK_DEV, MODEL_DIM), gate_wt.reshape(GROUP_SIZE, PER_SOURCE), owner_ids)
    d_slot = (out_rows.astype(jnp.float32) * gate_rows[:, :, None]).astype(jnp.bfloat16)
    results = lax.map(one_expert, (by_expert(x_disp), by_expert(out_rows), by_expert(d_slot), w_gate, w_up, w_down))
    grad_x, grad_w_gate, grad_w_up, grad_w_down, gate_grad_rows = results
    grad_x_disp = jnp.moveaxis(grad_x.reshape(EXPERTS, GROUP_SIZE, CAPACITY, MODEL_DIM), 0, 1)
    gate_grad_src = jnp.moveaxis(gate_grad_rows.reshape(EXPERTS, GROUP_SIZE, CAPACITY), 0, 1).reshape(GROUP_SIZE, SLOT_COUNT)
    grad_gate = jax.vmap(take_fill)(gate_grad_src, flat_pos).reshape(TOKENS, TOP_K)
    return grad_x_disp, grad_w_gate, grad_w_up, grad_w_down, grad_gate
```

```python
import functools
import math

import jax
import jax.numpy as jnp
from jax import lax
from jax.experimental import pallas as pl
from jax.experimental.pallas import tpu as pltpu
from jax.sharding import PartitionSpec as P

F32 = jnp.float32
BF16 = jnp.bfloat16
MESH = pl.DeviceIdType.MESH

ORDER = [(0, 0), (0, 1), (0, 3), (0, 2), (1, 0), (3, 0), (2, 0), (1, 1),
         (1, 3), (3, 1), (3, 3), (1, 2), (2, 1), (3, 2), (2, 3), (2, 2)]
PLACE = {block: place for place, block in enumerate(ORDER)}
QUARTERS = 4
GROUP_BLOCKS = 4
NT = (((1,), (1,)), ((), ()))
TN = (((0,), (0,)), ((), ()))


def send_lists():
    plus_x = [(0, 0, 0), (0, 0, 1), (0, 0, 2), (0, 1, 0), (0, 0, 3), (0, 1, 2),
              (1, 0, 2), (1, 0, 3), (3, 0, 2), (3, 0, 3), (2, 0, 2), (2, 0, 3),
              (1, 1, 2), (3, 1, 2), (2, 1, 2)]
    flip = (1, 0, 3, 2)
    swap = (2, 3, 0, 1)
    minus_x = [(oy, -ox % 4, flip[q]) for oy, ox, q in plus_x]
    plus_y = [(ox, oy, swap[q]) for oy, ox, q in plus_x]
    minus_y = [(-oy % 4, ox, flip[q]) for oy, ox, q in plus_y]
    return {(0, 1): plus_x, (0, 3): minus_x, (1, 0): plus_y, (3, 0): minus_y}


SENDS = send_lists()
SLOTS = len(SENDS[(0, 1)])


def chain(values, index):
    out = jnp.int32(values[0])
    for k in range(1, len(values)):
        out = jnp.where(index == k, jnp.int32(values[k]), out)
    return out


def expert_kernel(group_size, x_hbm, wg_hbm, wu_hbm, wd_hbm, dout_hbm, route_hbm,
                  dadb_hbm, gu_hbm, dn_hbm, back_hbm, pq_hbm, h_hbm,
                  ag, rt, acc_gu, acc_d, wgu, wd, xb, db, pq, hb, dadb, gs, gg, gsend, grecv,
                  w_sem, own_sem, x_sem, spill_sem, fill_sem, dadb_sem, fin_sem,
                  recv_sem, rrecv_sem, send_sem, rsend_sem,
                  srecv_sem, srrecv_sem, ssend_sem, srsend_sem, gsend_sem, grecv_sem):
    side = math.isqrt(group_size // 2)
    me = lax.axis_index('ep')
    core = lax.rem(me, 2)
    my_x = lax.rem(me // 2, side)
    my_y = me // (2 * side)
    e_local, rows_u, model = xb.shape
    ffn = hb.shape[2]
    cap = x_hbm.shape[2]
    tok = ag.shape[2]
    qrows = tok // QUARTERS
    n_blocks = side * side
    groups = n_blocks // GROUP_BLOCKS
    per_unit = 2 * GROUP_BLOCKS
    tile = 256
    mt_count = model // tile
    ft_count = ffn // tile

    def device(y, x, c):
        return (y * side + x) * 2 + c

    def neighbour(dy, dx):
        return device(lax.rem(my_y + dy, side), lax.rem(my_x + dx, side), core)

    sibling = device(my_y, my_x, 1 - core)

    def origin(p, r):
        oy = chain([b[0] for b in ORDER], p)
        ox = chain([b[1] for b in ORDER], p)
        c = core + r - 2 * core * r
        return device(lax.rem(my_y + side - oy, side), lax.rem(my_x + side - ox, side), c)

    def quarter(r, p, q):
        return ag.at[r, p, pl.ds(q * qrows, qrows)]

    def ici_copy(p_from, p_to, q, to):
        return pltpu.make_async_remote_copy(
            src_ref=quarter(0, p_from, q), dst_ref=quarter(0, p_to, q), send_sem=send_sem,
            recv_sem=recv_sem.at[p_to, q], device_id={'ep': to}, device_id_type=MESH)

    def ici_route(p_from, p_to, to):
        return pltpu.make_async_remote_copy(
            src_ref=rt.at[0, p_from], dst_ref=rt.at[0, p_to], send_sem=rsend_sem,
            recv_sem=rrecv_sem.at[p_to], device_id={'ep': to}, device_id_type=MESH)

    def sib_copy(p, q):
        return pltpu.make_async_remote_copy(
            src_ref=quarter(0, p, q), dst_ref=quarter(1, p, q), send_sem=ssend_sem,
            recv_sem=srecv_sem.at[p, q], device_id={'ep': sibling}, device_id_type=MESH)

    def sib_route(p):
        return pltpu.make_async_remote_copy(
            src_ref=rt.at[0, p], dst_ref=rt.at[1, p], send_sem=srsend_sem,
            recv_sem=srrecv_sem.at[p], device_id={'ep': sibling}, device_id_type=MESH)

    def issue(slot):
        for (dy, dx), sends in SENDS.items():
            oy, ox, q = sends[slot]
            p_from, p_to = PLACE[(oy, ox)], PLACE[((oy + dy) % 4, (ox + dx) % 4)]
            to = neighbour(dy, dx)
            ici_copy(p_from, p_to, q, to).start()
            if q == 0:
                ici_route(p_from, p_to, to).start()

    def service(slot):
        for (dy, dx), sends in SENDS.items():
            oy, ox, q = sends[slot]
            p_to = PLACE[((oy + dy) % 4, (ox + dx) % 4)]
            ici_copy(p_to, p_to, q, me).wait_recv()
            if q == 0:
                ici_route(p_to, p_to, me).wait_recv()
        if slot + 3 < SLOTS:
            issue(slot + 3)
        for (dy, dx), sends in SENDS.items():
            oy, ox, q = sends[slot]
            p_to = PLACE[((oy + dy) % 4, (ox + dx) % 4)]
            sib_copy(p_to, q).start()
            if q == 0:
                sib_route(p_to).start()

    def x_copy(g, e, j):
        src = origin(g * GROUP_BLOCKS + j // 2, j % 2)
        return pltpu.make_async_copy(x_hbm.at[src, e], xb.at[e, pl.ds(j * cap, cap)], x_sem.at[e, j])

    def dadb_copy(g, e, j):
        src = origin(g * GROUP_BLOCKS + j // 2, j % 2)
        return pltpu.make_async_copy(dadb.at[pl.ds(j * cap, cap)], dadb_hbm.at[src, e], dadb_sem.at[j])

    def x_start(g, e):
        for j in range(per_unit):
            x_copy(g, e, j).start()

    def x_wait(g, e):
        for j in range(per_unit):
            x_copy(g, e, j).wait()

    def spill_copies(u, e):
        return (pltpu.make_async_copy(pq.at[e], pq_hbm.at[u], spill_sem.at[e, 0]),
                pltpu.make_async_copy(hb.at[e], h_hbm.at[u], spill_sem.at[e, 1]))

    def fill_copies(u, e):
        return (pltpu.make_async_copy(pq_hbm.at[u], pq.at[e], fill_sem.at[e, 0]),
                pltpu.make_async_copy(h_hbm.at[u], hb.at[e], fill_sem.at[e, 1]))

    w_copies = [pltpu.make_async_copy(wg_hbm, wgu.at[:, :, pl.ds(0, ffn)], w_sem.at[0]),
                pltpu.make_async_copy(wu_hbm, wgu.at[:, :, pl.ds(ffn, ffn)], w_sem.at[1]),
                pltpu.make_async_copy(wd_hbm, wd, w_sem.at[2])]
    own = [pltpu.make_async_copy(dout_hbm, ag.at[0, 0], own_sem.at[0]),
           pltpu.make_async_copy(route_hbm, rt.at[0, 0], own_sem.at[1])]

    for c in own:
        c.start()
    barrier = pltpu.get_barrier_semaphore()

    @pl.loop(1, group_size)
    def _(k):
        pl.semaphore_signal(barrier, inc=1, device_id={'ep': lax.rem(me + k, group_size)}, device_id_type=MESH)

    for c in w_copies[:2]:
        c.start()
    x_start(0, 0)
    x_start(0, 1)
    w_copies[2].start()
    for c in own:
        c.wait()
    pl.semaphore_wait(barrier, group_size - 1)
    for slot in range(3):
        issue(slot)
    for q in range(QUARTERS):
        sib_copy(0, q).start()
    sib_route(0).start()

    @pl.loop(0, mt_count)
    def _(m):
        rows = pl.ds(pl.multiple_of(m * tile, tile), tile)
        for e in range(e_local):
            acc_gu[e, rows] = jnp.zeros((tile, 2 * ffn), F32)

    @pl.loop(0, ft_count)
    def _(m):
        rows = pl.ds(pl.multiple_of(m * tile, tile), tile)
        for e in range(e_local):
            acc_d[e, rows] = jnp.zeros((tile, model), F32)

    for c in w_copies[:2]:
        c.wait()

    @pl.loop(0, groups * e_local)
    def _(u):
        g, e = u // e_local, lax.rem(u, e_local)
        x_wait(g, e)

        @pl.when(u >= e_local)
        def _():
            for c in spill_copies(u - e_local, e):
                c.wait()

        @pl.loop(0, ft_count)
        def _(n):
            lo = pl.ds(pl.multiple_of(n * tile, tile), tile)
            hi = pl.ds(pl.multiple_of(ffn + n * tile, tile), tile)
            x = xb[e]
            a = jnp.dot(x, wgu[e, :, lo], preferred_element_type=F32)
            b = jnp.dot(x, wgu[e, :, hi], preferred_element_type=F32)
            sg = jax.nn.sigmoid(a)
            silu = a * sg
            hb[e, :, lo] = (silu * b).astype(BF16)
            pq[e, :, lo] = b * sg * (1.0 + a * (1.0 - sg))
            pq[e, :, hi] = silu

        for c in spill_copies(u, e):
            c.start()
        nxt = u + e_local
        x_start(lax.rem(nxt // e_local, groups), e)

        for k, at in ((0, 2), (1, 4), (2, 6)):
            @pl.when(u == at)
            def _(k=k):
                service(k)

    for e in range(e_local):
        for c in spill_copies((groups - 1) * e_local + e, e):
            c.wait()
    for e in range(e_local):
        for c in fill_copies(e, e):
            c.start()
    w_copies[2].wait()
    for slot in (3, 4, 5):
        service(slot)

    def hits(r, p, e):
        local = rt[r, p, 0:8] - (me * (e_local * cap) + e * cap).astype(F32)
        hit = (local >= 0.0) & (local < float(cap))
        slot = jnp.max(jnp.where(hit, local, -1.0), axis=0, keepdims=True)
        gate = jnp.sum(jnp.where(hit, rt[r, p, 8:16], 0.0), axis=0, keepdims=True)
        return slot, gate

    @pl.loop(0, groups)
    def _(g):
        def on(step, *slots):
            @pl.when(g == step)
            def _():
                for s in slots:
                    service(s)

        @pl.loop(0, per_unit)
        def _(j):
            p, r = g * GROUP_BLOCKS + j // 2, lax.rem(j, 2)

            @pl.when(r == 1)
            def _():
                for q in range(QUARTERS):
                    sib_copy(p, q).wait_recv()
                sib_route(p).wait_recv()

            rows = pl.ds(pl.multiple_of(j * cap, cap), cap)
            slot_iota = lax.broadcasted_iota(jnp.int32, (cap, tok), 0).astype(F32)
            picks = []
            for e in range(e_local):
                slot, gate = hits(r, p, jnp.int32(e))
                pick = slot_iota == slot
                gs[e, rows] = jnp.broadcast_to(
                    jnp.sum(jnp.where(pick, gate, 0.0), axis=1, keepdims=True), (cap, 128))
                picks.append(jnp.where(pick, 1.0, 0.0).astype(BF16))
            pick = jnp.concatenate(picks, axis=0)
            for n in range(model // 512):
                cols = pl.ds(n * 512, 512)
                d = jnp.dot(pick, ag[r, p, :, cols], preferred_element_type=F32).astype(BF16)
                for e in range(e_local):
                    db[e, rows, cols] = d[e * cap:(e + 1) * cap]

        on(0, 6)
        on(1, 8)

        @pl.loop(0, e_local)
        def _(e):
            x_wait(g, e)
            for c in fill_copies(g * e_local + e, e):
                c.wait()
            gg[...] = jnp.zeros_like(gg)

            @pl.loop(0, mt_count)
            def _(n):
                cols = pl.ds(pl.multiple_of(n * tile, tile), tile)
                y = jnp.dot(hb[e], wd[e, :, cols], preferred_element_type=F32)
                d = db[e, :, cols].astype(F32)
                prod = d * y
                gg[...] += prod[:, :128] + prod[:, 128:]
                gate = gs[e]
                db[e, :, cols] = (d * jnp.concatenate([gate, gate], axis=1)).astype(BF16)

            @pl.when(g * e_local + e > 0)
            def _():
                for j in range(per_unit):
                    dadb_copy(g, e, j).wait()

            @pl.loop(0, ft_count)
            def _(n):
                lo = pl.ds(pl.multiple_of(n * tile, tile), tile)
                hi = pl.ds(pl.multiple_of(ffn + n * tile, tile), tile)
                dh = lax.dot_general(db[e], wd[e, lo, :], NT, preferred_element_type=F32).astype(BF16).astype(F32)
                dadb[:, lo] = (dh * pq[e, :, lo]).astype(BF16)
                dadb[:, hi] = (dh * pq[e, :, hi]).astype(BF16)

            for j in range(per_unit):
                dadb_copy(g, e, j).start()

            gg[...] = jnp.broadcast_to(jnp.sum(gg[...], axis=1, keepdims=True), gg.shape)

            @pl.loop(0, per_unit)
            def _(j):
                p, r = g * GROUP_BLOCKS + j // 2, lax.rem(j, 2)
                rows = pl.ds(pl.multiple_of(j * cap, cap), cap)
                slot, _ = hits(r, p, e)
                pick = lax.broadcasted_iota(jnp.int32, (cap, tok), 0).astype(F32) == slot
                value = jnp.concatenate([gg[rows]] * (tok // 128), axis=1)
                gsend[g * per_unit + j, e] = jnp.sum(jnp.where(pick, value, 0.0), axis=0, keepdims=True)

            @pl.loop(0, mt_count)
            def _(m):
                rows = pl.ds(pl.multiple_of(m * tile, tile), tile)
                for n in range(2):
                    cols = pl.ds(n * ffn, ffn)
                    acc_gu[e, rows, cols] += lax.dot_general(
                        xb[e, :, rows], dadb[:, cols], TN, preferred_element_type=F32)

            @pl.loop(0, ft_count)
            def _(m):
                rows = pl.ds(pl.multiple_of(m * tile, tile), tile)
                for n in range(model // 512):
                    cols = pl.ds(n * 512, 512)
                    acc_d[e, rows, cols] += lax.dot_general(
                        hb[e, :, rows], db[e, :, cols], TN, preferred_element_type=F32)

            @pl.when(g + 1 < groups)
            def _():
                x_start(g + 1, e)
                for c in fill_copies((g + 1) * e_local + e, e):
                    c.start()

            @pl.when(g + 1 == groups)
            def _():
                @pl.loop(0, mt_count)
                def _(m):
                    rows = pl.ds(pl.multiple_of(m * tile, tile), tile)
                    wgu[e, rows] = acc_gu[e, rows].astype(BF16)

                @pl.loop(0, ft_count)
                def _(m):
                    rows = pl.ds(pl.multiple_of(m * tile, tile), tile)
                    wd[e, rows] = acc_d[e, rows].astype(BF16)

                pltpu.make_async_copy(wgu.at[e], gu_hbm.at[e], fin_sem.at[e, 0]).start()
                pltpu.make_async_copy(wd.at[e], dn_hbm.at[e], fin_sem.at[e, 1]).start()

            for at, first, second in ((0, 7, None), (1, 9, 10), (2, 13, 14)):
                slots = (first, second)
                for which in range(2):
                    if slots[which] is not None:
                        @pl.when((g == at) & (e == which))
                        def _(s=slots[which]):
                            service(s)

        on(1, 11, 12)

        @pl.when(g == 0)
        def _():
            grecv[me] = gsend[0]

        @pl.loop(jnp.where(g == 0, 1, 0), per_unit)
        def _(j):
            to = origin(g * GROUP_BLOCKS + j // 2, lax.rem(j, 2))
            pltpu.make_async_remote_copy(
                src_ref=gsend.at[g * per_unit + j], dst_ref=grecv.at[me], send_sem=gsend_sem,
                recv_sem=grecv_sem, device_id={'ep': to}, device_id_type=MESH).start()

    for j in range(per_unit):
        dadb_copy(groups - 1, e_local - 1, j).wait()

    def drain(ref, sem):
        pltpu.make_async_copy(ref, ref, sem).wait()

    drain(ag.at[0, pl.ds(0, n_blocks - 1)], send_sem)
    drain(rt.at[0, pl.ds(0, n_blocks - 1)], rsend_sem)
    drain(ag.at[0], ssend_sem)
    drain(rt.at[0], srsend_sem)
    drain(gsend.at[pl.ds(0, group_size - 1)], gsend_sem)
    drain(grecv.at[pl.ds(0, group_size - 1)], grecv_sem)
    back = pltpu.make_async_copy(grecv, back_hbm, own_sem.at[0])
    back.start()
    back.wait()
    for e in range(e_local):
        pltpu.make_async_copy(wgu.at[e], gu_hbm.at[e], fin_sem.at[e, 0]).wait()
        pltpu.make_async_copy(wd.at[e], dn_hbm.at[e], fin_sem.at[e, 1]).wait()


def run_experts(x_disp, w_gate, w_up, w_down, d_out, route, group_size):
    sources, e_local, cap, model = x_disp.shape
    ffn = w_gate.shape[2]
    tok = d_out.shape[0]
    n_blocks = group_size // 2
    per_unit = 2 * GROUP_BLOCKS
    rows_u = per_unit * cap
    units = n_blocks // GROUP_BLOCKS * e_local
    dma = pltpu.SemaphoreType.DMA
    any_spec = pl.BlockSpec(memory_space=pl.ANY)
    out_shape = [
        jax.ShapeDtypeStruct((sources, e_local, cap, 2 * ffn), BF16),
        jax.ShapeDtypeStruct((e_local, model, 2 * ffn), BF16),
        jax.ShapeDtypeStruct((e_local, ffn, model), BF16),
        jax.ShapeDtypeStruct((group_size, e_local, 1, tok), F32),
        jax.ShapeDtypeStruct((units, rows_u, 2 * ffn), F32),
        jax.ShapeDtypeStruct((units, rows_u, ffn), BF16),
    ]
    scratch = [
        pltpu.VMEM((2, n_blocks, tok, model), BF16),
        pltpu.VMEM((2, n_blocks, 16, tok), F32),
        pltpu.VMEM((e_local, model, 2 * ffn), F32),
        pltpu.VMEM((e_local, ffn, model), F32),
        pltpu.VMEM((e_local, model, 2 * ffn), BF16),
        pltpu.VMEM((e_local, ffn, model), BF16),
        pltpu.VMEM((e_local, rows_u, model), BF16),
        pltpu.VMEM((e_local, rows_u, model), BF16),
        pltpu.VMEM((e_local, rows_u, 2 * ffn), F32),
        pltpu.VMEM((e_local, rows_u, ffn), BF16),
        pltpu.VMEM((rows_u, 2 * ffn), BF16),
        pltpu.VMEM((e_local, rows_u, 128), F32),
        pltpu.VMEM((rows_u, 128), F32),
        pltpu.VMEM((group_size, e_local, 1, tok), F32),
        pltpu.VMEM((group_size, e_local, 1, tok), F32),
        dma((3,)), dma((2,)), dma((e_local, per_unit)), dma((e_local, 2)), dma((e_local, 2)),
        dma((per_unit,)), dma((e_local, 2)),
        dma((n_blocks, QUARTERS)), dma((n_blocks,)), dma, dma,
        dma((n_blocks, QUARTERS)), dma((n_blocks,)), dma, dma, dma, dma,
    ]
    return pl.pallas_call(
        functools.partial(expert_kernel, group_size),
        out_shape=out_shape, in_specs=[any_spec] * 6, out_specs=[any_spec] * 6, scratch_shapes=scratch,
        compiler_params=pltpu.CompilerParams(collective_id=0, has_side_effects=True, vmem_limit_bytes=67043328),
    )(x_disp, w_gate, w_up, w_down, d_out, route)


def finish_kernel(group_size, dadb, wg, wu, gu, dn, back, ids, slots, gx, gg_w, gu_w, gd_w, gate_out):
    sources, _, cap, width = dadb.shape
    ffn = width // 2
    model = gx.shape[3]
    both = dadb[...].reshape(sources * cap, width)
    for n in range(model // 512):
        rows = pl.ds(n * 512, 512)
        out = (lax.dot_general(both[:, :ffn], wg[0, rows], NT, preferred_element_type=F32)
               + lax.dot_general(both[:, ffn:], wu[0, rows], NT, preferred_element_type=F32))
        gx[:, 0, :, rows] = out.astype(BF16).reshape(sources, cap, 512)
    gg_w[...] = gu[:, :, :ffn]
    gu_w[...] = gu[:, :, ffn:]
    gd_w[...] = dn[...]

    @pl.when((pl.program_id(0) == 0) & (pl.program_id(1) == 0))
    def _():
        e_local = back.shape[1]
        total = jnp.zeros(gate_out.shape, F32)
        for d in range(group_size):
            for e in range(e_local):
                total += jnp.where(ids[...] == d * e_local + e, back[d, e], 0.0)
        gate_out[...] = jnp.where(slots[...] >= 0, total, 0.0)


def run_finish(dadb, w_gate, w_up, gu, dn, back, ids, slots, group_size):
    sources, e_local, cap, width = dadb.shape
    model, ffn = w_gate.shape[1:]
    steps = 4
    s_blk, m_blk, f_blk = sources // steps, model // steps, ffn // steps
    tok = ids.shape[1]
    whole = lambda shape: pl.BlockSpec(shape, lambda e, i: (0,) * len(shape))
    return pl.pallas_call(
        functools.partial(finish_kernel, group_size),
        grid=(e_local, steps),
        in_specs=[
            pl.BlockSpec((s_blk, 1, cap, width), lambda e, i: (i, e, 0, 0)),
            pl.BlockSpec((1, model, ffn), lambda e, i: (e, 0, 0)),
            pl.BlockSpec((1, model, ffn), lambda e, i: (e, 0, 0)),
            pl.BlockSpec((1, m_blk, width), lambda e, i: (e, i, 0)),
            pl.BlockSpec((1, f_blk, model), lambda e, i: (e, i, 0)),
            whole(back.shape), whole((8, tok)), whole((8, tok)),
        ],
        out_specs=[
            pl.BlockSpec((s_blk, 1, cap, model), lambda e, i: (i, e, 0, 0)),
            pl.BlockSpec((1, m_blk, ffn), lambda e, i: (e, i, 0)),
            pl.BlockSpec((1, m_blk, ffn), lambda e, i: (e, i, 0)),
            pl.BlockSpec((1, f_blk, model), lambda e, i: (e, i, 0)),
            whole((8, tok)),
        ],
        out_shape=[
            jax.ShapeDtypeStruct((sources, e_local, cap, model), BF16),
            jax.ShapeDtypeStruct((e_local, model, ffn), BF16),
            jax.ShapeDtypeStruct((e_local, model, ffn), BF16),
            jax.ShapeDtypeStruct((e_local, ffn, model), BF16),
            jax.ShapeDtypeStruct((8, tok), F32),
        ],
    )(dadb, w_gate, w_up, gu, dn, back, ids, slots)


def solution(mesh):
    group_size = mesh.shape['ep']

    def local_step(x_disp, w_gate, w_up, w_down, d_out, slot_idx, expert_id, gate_wt):
        cap = x_disp.shape[2]
        top_k = slot_idx.shape[1]
        pad = ((0, 8 - top_k), (0, 0))
        slots = jnp.pad(slot_idx.T, pad, constant_values=-1)
        ids = jnp.pad(expert_id.T, pad)
        pos = jnp.where(slots >= 0, ids * cap + slots, -1).astype(F32)
        route = jnp.concatenate([pos, jnp.pad(gate_wt.T, pad)], axis=0)
        dadb, gu, dn, back, _, _ = run_experts(x_disp, w_gate, w_up, w_down, d_out, route, group_size)
        grad_x, grad_w_gate, grad_w_up, grad_w_down, gate = run_finish(
            dadb, w_gate, w_up, gu, dn, back, ids, slots, group_size)
        return grad_x, grad_w_gate, grad_w_up, grad_w_down, gate[:top_k].T

    token_place = P(('dp', 'ep'), None)
    weight_place = P('ep', None, None)
    slot_place = P('dp', 'ep', None, None)
    grad_place = P(('dp', 'ep'), None, None)
    return jax.shard_map(local_step, mesh=mesh,
                         in_specs=(slot_place, weight_place, weight_place, weight_place, token_place, token_place, token_place, token_place),
                         out_specs=(slot_place, grad_place, grad_place, grad_place, token_place),
                         check_vma=False)
```

```python
import functools
import math

import jax
import jax.numpy as jnp
from jax import lax
from jax.experimental import pallas as pl
from jax.experimental.pallas import tpu as pltpu
from jax.sharding import PartitionSpec as P

F32 = jnp.float32
BF16 = jnp.bfloat16
MESH = pl.DeviceIdType.MESH

ORDER = [(0, 0), (0, 1), (0, 3), (1, 0), (3, 0), (0, 2), (2, 0), (1, 1),
         (1, 2), (3, 1), (1, 3), (3, 3), (3, 2), (2, 1), (2, 3), (2, 2)]
PLACE = {block: place for place, block in enumerate(ORDER)}


def packed(values):
    total = sum(v << (2 * k) for k, v in enumerate(values))
    return total - 2 ** 32 if total >= 2 ** 31 else total


ORIGIN_Y, ORIGIN_X = packed([b[0] for b in ORDER]), packed([b[1] for b in ORDER])
QUARTERS = 4
UNIT_BLOCKS = 4
STEP_BLOCKS = 2
BEFORE = {0: (3,), 3: (7,), 4: (9, 10), 6: (13,)}
BETWEEN = {0: (4,), 1: (5,), 2: (6,), 3: (8,), 4: (11,), 5: (12,)}
AFTER = {6: (14,)}
NT = (((1,), (1,)), ((), ()))
TN = (((0,), (0,)), ((), ()))


def send_lists():
    own = [(0, 0, 0), (0, 0, 1), (0, 0, 2), (0, 0, 3), (0, 1, 0), (0, 1, 2)]
    plus_x = own + [(1, 0, 2), (1, 0, 3), (3, 0, 2), (1, 1, 2), (3, 0, 3), (2, 0, 2),
                    (3, 1, 2), (2, 0, 3), (2, 1, 2)]
    swap = (2, 3, 0, 1)
    flip = (1, 0, 3, 2)
    plus_y = [(ox, oy, swap[q]) for oy, ox, q in own]
    plus_y += [(0, 1, 0), (0, 1, 1), (0, 2, 0), (0, 2, 1), (0, 3, 0), (0, 3, 1),
               (1, 1, 0), (1, 3, 0), (1, 2, 0)]
    minus_x = [(oy, -ox % 4, flip[q]) for oy, ox, q in plus_x]
    minus_y = [(-oy % 4, ox, flip[q]) for oy, ox, q in plus_y]
    return {(0, 1): plus_x, (0, 3): minus_x, (1, 0): plus_y, (3, 0): minus_y}


SENDS = send_lists()
SLOTS = len(SENDS[(0, 1)])


def expert_kernel(group_size, x_hbm, wg_hbm, wu_hbm, wd_hbm, dout_hbm, route_hbm,
                  dadb_hbm, gu_hbm, dn_hbm, back_hbm, pq_hbm, h_hbm,
                  ag, rt, acc_gu, acc_d, wgu, wd, xb, db, pq, hb, dadb, gg, gsend, grecv,
                  w_sem, own_sem, x_sem, spill_sem, fill_sem, dadb_sem, fin_sem,
                  recv_sem, rrecv_sem, send_sem, rsend_sem,
                  srecv_sem, srrecv_sem, ssend_sem, srsend_sem, gsend_sem, grecv_sem):
    side = math.isqrt(group_size // 2)
    me = lax.axis_index('ep')
    core = lax.rem(me, 2)
    my_x = lax.rem(me // 2, side)
    my_y = me // (2 * side)
    e_local, rows_u, model = xb.shape
    rows_s = dadb.shape[1]
    ffn = hb.shape[2]
    cap = x_hbm.shape[2]
    tok = ag.shape[2]
    qrows = tok // QUARTERS
    n_blocks = side * side
    units = n_blocks // UNIT_BLOCKS
    steps = n_blocks // STEP_BLOCKS
    per_unit = 2 * UNIT_BLOCKS
    per_step = 2 * STEP_BLOCKS
    tile = 256
    mt_count = model // tile
    ft_count = ffn // tile

    def device(y, x, c):
        return (y * side + x) * 2 + c

    def neighbour(dy, dx):
        return device(lax.rem(my_y + dy, side), lax.rem(my_x + dx, side), core)

    sibling = device(my_y, my_x, 1 - core)

    def origin(p, r):
        oy = lax.shift_right_logical(jnp.int32(ORIGIN_Y), 2 * p) & 3
        ox = lax.shift_right_logical(jnp.int32(ORIGIN_X), 2 * p) & 3
        c = core + r - 2 * core * r
        return device(lax.rem(my_y + side - oy, side), lax.rem(my_x + side - ox, side), c)

    def quarter(r, p, q):
        return ag.at[r, p, pl.ds(q * qrows, qrows)]

    def ici_copy(p_from, p_to, q, to):
        return pltpu.make_async_remote_copy(
            src_ref=quarter(0, p_from, q), dst_ref=quarter(0, p_to, q), send_sem=send_sem,
            recv_sem=recv_sem.at[p_to, q], device_id={'ep': to}, device_id_type=MESH)

    def ici_route(p_from, p_to, to):
        return pltpu.make_async_remote_copy(
            src_ref=rt.at[0, p_from], dst_ref=rt.at[0, p_to], send_sem=rsend_sem,
            recv_sem=rrecv_sem.at[p_to], device_id={'ep': to}, device_id_type=MESH)

    def sib_copy(p, q):
        return pltpu.make_async_remote_copy(
            src_ref=quarter(0, p, q), dst_ref=quarter(1, p, q), send_sem=ssend_sem,
            recv_sem=srecv_sem.at[p, q], device_id={'ep': sibling}, device_id_type=MESH)

    def sib_route(p):
        return pltpu.make_async_remote_copy(
            src_ref=rt.at[0, p], dst_ref=rt.at[1, p], send_sem=srsend_sem,
            recv_sem=srrecv_sem.at[p], device_id={'ep': sibling}, device_id_type=MESH)

    def issue(slot):
        for (dy, dx), sends in SENDS.items():
            oy, ox, q = sends[slot]
            p_from, p_to = PLACE[(oy, ox)], PLACE[((oy + dy) % 4, (ox + dx) % 4)]
            to = neighbour(dy, dx)
            ici_copy(p_from, p_to, q, to).start()
            if q == 0:
                ici_route(p_from, p_to, to).start()

    def service(slot):
        for (dy, dx), sends in SENDS.items():
            oy, ox, q = sends[slot]
            p_to = PLACE[((oy + dy) % 4, (ox + dx) % 4)]
            ici_copy(p_to, p_to, q, me).wait_recv()
            if q == 0:
                ici_route(p_to, p_to, me).wait_recv()
        if slot + 3 < SLOTS:
            issue(slot + 3)
        for (dy, dx), sends in SENDS.items():
            oy, ox, q = sends[slot]
            p_to = PLACE[((oy + dy) % 4, (ox + dx) % 4)]
            sib_copy(p_to, q).start()
            if q == 0:
                sib_route(p_to).start()

    def x_copy(block, j, e, row, sem):
        src = origin(block + j // 2, j % 2)
        return pltpu.make_async_copy(x_hbm.at[src, e], xb.at[e, pl.ds(row + j * cap, cap)], x_sem.at[e, sem + j])

    def unit_x(g, e):
        return [x_copy(g * UNIT_BLOCKS, j, e, 0, 0) for j in range(per_unit)]

    def half_rows(t):
        return pl.multiple_of(lax.rem(t, 2) * rows_s, rows_s)

    def step_fill(t, e):
        row = half_rows(t)
        here, u = pl.ds(row, rows_s), (t // 2) * e_local + e
        half = lax.rem(t, 2)
        return ([x_copy(t * STEP_BLOCKS, j, e, row, half * per_step) for j in range(per_step)]
                + [pltpu.make_async_copy(pq_hbm.at[u, here], pq.at[e, here], fill_sem.at[e, half, 0]),
                   pltpu.make_async_copy(h_hbm.at[u, here], hb.at[e, here], fill_sem.at[e, half, 1])])

    def dadb_copy(t, e, j):
        src = origin(t * STEP_BLOCKS + j // 2, j % 2)
        return pltpu.make_async_copy(dadb.at[e, pl.ds(j * cap, cap)], dadb_hbm.at[src, e], dadb_sem.at[e, j])

    def spill_copies(u, e):
        return (pltpu.make_async_copy(pq.at[e], pq_hbm.at[u], spill_sem.at[e, 0]),
                pltpu.make_async_copy(hb.at[e], h_hbm.at[u], spill_sem.at[e, 1]))

    w_copies = [pltpu.make_async_copy(wg_hbm, wgu.at[:, :, pl.ds(0, ffn)], w_sem.at[0]),
                pltpu.make_async_copy(wu_hbm, wgu.at[:, :, pl.ds(ffn, ffn)], w_sem.at[1]),
                pltpu.make_async_copy(wd_hbm, wd, w_sem.at[2])]
    own = [pltpu.make_async_copy(dout_hbm, ag.at[0, 0], own_sem.at[0]),
           pltpu.make_async_copy(route_hbm, rt.at[0, 0], own_sem.at[1])]

    for c in own:
        c.start()
    barrier = pltpu.get_barrier_semaphore()

    @pl.loop(1, group_size)
    def _(k):
        pl.semaphore_signal(barrier, inc=1, device_id={'ep': lax.rem(me + k, group_size)}, device_id_type=MESH)

    for c in w_copies[:2]:
        c.start()
    for e in range(e_local):
        for c in unit_x(0, e):
            c.start()
    w_copies[2].start()
    for c in own:
        c.wait()
    pl.semaphore_wait(barrier, group_size - 1)
    for slot in range(3):
        issue(slot)
    for q in range(QUARTERS):
        sib_copy(0, q).start()
    sib_route(0).start()

    @pl.loop(0, mt_count)
    def _(m):
        rows = pl.ds(pl.multiple_of(m * tile, tile), tile)
        for e in range(e_local):
            acc_gu[e, rows] = jnp.zeros((tile, 2 * ffn), F32)

    @pl.loop(0, ft_count)
    def _(m):
        rows = pl.ds(pl.multiple_of(m * tile, tile), tile)
        for e in range(e_local):
            acc_d[e, rows] = jnp.zeros((tile, model), F32)

    for c in w_copies[:2]:
        c.wait()

    @pl.loop(0, units * e_local)
    def _(u):
        g, e = u // e_local, lax.rem(u, e_local)
        for c in unit_x(g, e):
            c.wait()

        @pl.when(u >= e_local)
        def _():
            for c in spill_copies(u - e_local, e):
                c.wait()

        @pl.loop(0, ft_count)
        def _(n):
            lo = pl.ds(pl.multiple_of(n * tile, tile), tile)
            hi = pl.ds(pl.multiple_of(ffn + n * tile, tile), tile)
            x = xb[e]
            a = jnp.dot(x, wgu[e, :, lo], preferred_element_type=F32)
            b = jnp.dot(x, wgu[e, :, hi], preferred_element_type=F32)
            sg = jax.nn.sigmoid(a)
            silu = a * sg
            hb[e, :, lo] = (silu * b).astype(BF16)
            pq[e, :, lo] = b * sg * (1.0 + a * (1.0 - sg))
            pq[e, :, hi] = silu

        for c in spill_copies(u, e):
            c.start()

        @pl.when(g + 1 < units)
        def _():
            for c in unit_x(g + 1, e):
                c.start()

        for k, at in ((0, 2), (1, 4), (2, 6)):
            @pl.when(u == at)
            def _(k=k):
                service(k)

    for e in range(e_local):
        for c in spill_copies((units - 1) * e_local + e, e):
            c.wait()
    for t in range(2):
        for e in range(e_local):
            for c in step_fill(jnp.int32(t), e):
                c.start()
    w_copies[2].wait()

    def hits(r, p, e):
        local = rt[r, p, 0:8] - (me * (e_local * cap) + e * cap).astype(F32)
        hit = (local >= 0.0) & (local < float(cap))
        slot = jnp.max(jnp.where(hit, local, -1.0), axis=0, keepdims=True)
        gate = jnp.sum(jnp.where(hit, rt[r, p, 8:16], 0.0), axis=0, keepdims=True)
        return slot, gate

    def on(table, t):
        for step, slots in table.items():
            @pl.when(t == step)
            def _(slots=slots):
                for k in slots:
                    service(k)

    slot_iota = lax.broadcasted_iota(jnp.int32, (cap, tok), 0).astype(F32)

    @pl.loop(0, steps)
    def _(t):
        on(BEFORE, t)
        half = half_rows(t)
        here = pl.ds(half, rows_s)

        @pl.loop(0, STEP_BLOCKS)
        def _(i):
            p = t * STEP_BLOCKS + i
            for q in range(QUARTERS):
                sib_copy(p, q).wait_recv()
            sib_route(p).wait_recv()
            for r in range(2):
                picks, gates = [], []
                for e in range(e_local):
                    slot, gate = hits(r, p, e)
                    pick = slot_iota == slot
                    gates.append(jnp.sum(jnp.where(pick, gate, 0.0), axis=1, keepdims=True))
                    picks.append(jnp.where(pick, 1.0, 0.0).astype(BF16))
                pick = jnp.concatenate(picks, axis=0)
                row = pl.multiple_of((2 * i + r) * cap, cap)
                for n in range(model // 512):
                    cols = pl.ds(n * 512, 512)
                    d = jnp.dot(pick, ag[r, p, :, cols], preferred_element_type=F32)
                    for e in range(e_local):
                        d_e = d[e * cap:(e + 1) * cap]
                        db[e, pl.ds(row, cap), cols] = d_e.astype(BF16)
                        db[e, pl.ds(rows_s + row, cap), cols] = (d_e * gates[e]).astype(BF16)

        @pl.loop(0, e_local)
        def _(e):
            for c in step_fill(t, e):
                c.wait()

            @pl.when(t > 0)
            def _():
                for j in range(per_step):
                    dadb_copy(t, e, j).wait()

            gg[...] = jnp.zeros_like(gg)

            @pl.loop(0, ft_count)
            def _(n):
                lo = pl.ds(pl.multiple_of(n * tile, tile), tile)
                hi = pl.ds(pl.multiple_of(ffn + n * tile, tile), tile)
                both = lax.dot_general(db[e], wd[e, lo, :], NT, preferred_element_type=F32)
                prod = hb[e, here, lo].astype(F32) * both[:rows_s]
                gg[...] += prod[:, :128] + prod[:, 128:]
                dh = both[rows_s:].astype(BF16).astype(F32)
                dadb[e, :, lo] = (dh * pq[e, here, lo]).astype(BF16)
                dadb[e, :, hi] = (dh * pq[e, here, hi]).astype(BF16)

            for j in range(per_step):
                dadb_copy(t, e, j).start()

            total = jnp.broadcast_to(jnp.sum(gg[...], axis=1, keepdims=True), gg.shape)
            for j in range(per_step):
                slot, _ = hits(j % 2, t * STEP_BLOCKS + j // 2, e)
                value = jnp.concatenate([total[j * cap:(j + 1) * cap]] * (tok // 128), axis=1)
                gsend[t * per_step + j, e] = jnp.sum(
                    jnp.where(slot_iota == slot, value, 0.0), axis=0, keepdims=True)

            @pl.loop(0, model // 512)
            def _(m):
                rows = pl.ds(pl.multiple_of(m * 512, 512), 512)
                for n in range(2):
                    cols = pl.ds(n * ffn, ffn)
                    acc_gu[e, rows, cols] += lax.dot_general(
                        xb[e, here, rows], dadb[e, :, cols], TN, preferred_element_type=F32)

            for n in range(model // 512):
                cols = pl.ds(n * 512, 512)
                acc_d[e, :, cols] += lax.dot_general(
                    hb[e, here, :], db[e, rows_s:, cols], TN, preferred_element_type=F32)

            @pl.when(t + 2 < steps)
            def _():
                for c in step_fill(t + 2, e):
                    c.start()

            @pl.when(t + 1 == steps)
            def _():
                @pl.loop(0, mt_count)
                def _(m):
                    rows = pl.ds(pl.multiple_of(m * tile, tile), tile)
                    wgu[e, rows] = acc_gu[e, rows].astype(BF16)

                @pl.loop(0, ft_count)
                def _(m):
                    rows = pl.ds(pl.multiple_of(m * tile, tile), tile)
                    wd[e, rows] = acc_d[e, rows].astype(BF16)

                pltpu.make_async_copy(wgu.at[e], gu_hbm.at[e], fin_sem.at[e, 0]).start()
                pltpu.make_async_copy(wd.at[e], dn_hbm.at[e], fin_sem.at[e, 1]).start()

            for step, slots in BETWEEN.items():
                @pl.when((t == step) & (e == 0))
                def _(slots=slots):
                    for k in slots:
                        service(k)

        on(AFTER, t)

        @pl.when(t == 0)
        def _():
            grecv[me] = gsend[0]

        @pl.loop(jnp.where(t == 0, 1, 0), per_step)
        def _(j):
            to = origin(t * STEP_BLOCKS + j // 2, lax.rem(j, 2))
            pltpu.make_async_remote_copy(
                src_ref=gsend.at[t * per_step + j], dst_ref=grecv.at[me], send_sem=gsend_sem,
                recv_sem=grecv_sem, device_id={'ep': to}, device_id_type=MESH).start()

    for e in range(e_local):
        for j in range(per_step):
            dadb_copy(jnp.int32(steps - 1), e, j).wait()

    def drain(ref, sem):
        pltpu.make_async_copy(ref, ref, sem).wait()

    drain(ag.at[0, pl.ds(0, n_blocks - 1)], send_sem)
    drain(rt.at[0, pl.ds(0, n_blocks - 1)], rsend_sem)
    drain(ag.at[0], ssend_sem)
    drain(rt.at[0], srsend_sem)
    drain(gsend.at[pl.ds(0, group_size - 1)], gsend_sem)
    drain(grecv.at[pl.ds(0, group_size - 1)], grecv_sem)
    back = pltpu.make_async_copy(grecv, back_hbm, own_sem.at[0])
    back.start()
    back.wait()
    for e in range(e_local):
        pltpu.make_async_copy(wgu.at[e], gu_hbm.at[e], fin_sem.at[e, 0]).wait()
        pltpu.make_async_copy(wd.at[e], dn_hbm.at[e], fin_sem.at[e, 1]).wait()


def run_experts(x_disp, w_gate, w_up, w_down, d_out, route, group_size):
    sources, e_local, cap, model = x_disp.shape
    ffn = w_gate.shape[2]
    tok = d_out.shape[0]
    n_blocks = group_size // 2
    per_unit = 2 * UNIT_BLOCKS
    rows_u = per_unit * cap
    per_step = 2 * STEP_BLOCKS
    rows_s = per_step * cap
    units = n_blocks // UNIT_BLOCKS * e_local
    dma = pltpu.SemaphoreType.DMA
    any_spec = pl.BlockSpec(memory_space=pl.ANY)
    out_shape = [
        jax.ShapeDtypeStruct((sources, e_local, cap, 2 * ffn), BF16),
        jax.ShapeDtypeStruct((e_local, model, 2 * ffn), BF16),
        jax.ShapeDtypeStruct((e_local, ffn, model), BF16),
        jax.ShapeDtypeStruct((group_size, e_local, 1, tok), F32),
        jax.ShapeDtypeStruct((units, rows_u, 2 * ffn), F32),
        jax.ShapeDtypeStruct((units, rows_u, ffn), BF16),
    ]
    scratch = [
        pltpu.VMEM((2, n_blocks, tok, model), BF16),
        pltpu.VMEM((2, n_blocks, 16, tok), F32),
        pltpu.VMEM((e_local, model, 2 * ffn), F32),
        pltpu.VMEM((e_local, ffn, model), F32),
        pltpu.VMEM((e_local, model, 2 * ffn), BF16),
        pltpu.VMEM((e_local, ffn, model), BF16),
        pltpu.VMEM((e_local, rows_u, model), BF16),
        pltpu.VMEM((e_local, 2 * rows_s, model), BF16),
        pltpu.VMEM((e_local, rows_u, 2 * ffn), F32),
        pltpu.VMEM((e_local, rows_u, ffn), BF16),
        pltpu.VMEM((e_local, rows_s, 2 * ffn), BF16),
        pltpu.VMEM((rows_s, 128), F32),
        pltpu.VMEM((group_size, e_local, 1, tok), F32),
        pltpu.VMEM((group_size, e_local, 1, tok), F32),
        dma((3,)), dma((2,)), dma((e_local, per_unit)), dma((e_local, 2)), dma((e_local, 2, 2)),
        dma((e_local, per_step)), dma((e_local, 2)),
        dma((n_blocks, QUARTERS)), dma((n_blocks,)), dma, dma,
        dma((n_blocks, QUARTERS)), dma((n_blocks,)), dma, dma, dma, dma,
    ]
    return pl.pallas_call(
        functools.partial(expert_kernel, group_size),
        out_shape=out_shape, in_specs=[any_spec] * 6, out_specs=[any_spec] * 6, scratch_shapes=scratch,
        compiler_params=pltpu.CompilerParams(collective_id=0, has_side_effects=True, vmem_limit_bytes=67043328),
    )(x_disp, w_gate, w_up, w_down, d_out, route)


def finish_kernel(group_size, dadb, wg, wu, gu, dn, back, ids, slots, gx, gg_w, gu_w, gd_w, gate_out):
    sources, _, cap, width = dadb.shape
    ffn = width // 2
    model = gx.shape[3]
    both = dadb[...].reshape(sources * cap, width)
    for n in range(model // 512):
        rows = pl.ds(n * 512, 512)
        out = (lax.dot_general(both[:, :ffn], wg[0, rows], NT, preferred_element_type=F32)
               + lax.dot_general(both[:, ffn:], wu[0, rows], NT, preferred_element_type=F32))
        gx[:, 0, :, rows] = out.astype(BF16).reshape(sources, cap, 512)
    gg_w[...] = gu[:, :, :ffn]
    gu_w[...] = gu[:, :, ffn:]
    gd_w[...] = dn[...]

    @pl.when((pl.program_id(0) == 0) & (pl.program_id(1) == 0))
    def _():
        e_local = back.shape[1]
        total = jnp.zeros(gate_out.shape, F32)
        for d in range(group_size):
            for e in range(e_local):
                total += jnp.where(ids[...] == d * e_local + e, back[d, e], 0.0)
        gate_out[...] = jnp.where(slots[...] >= 0, total, 0.0)


def run_finish(dadb, w_gate, w_up, gu, dn, back, ids, slots, group_size):
    sources, e_local, cap, width = dadb.shape
    model, ffn = w_gate.shape[1:]
    steps = 4
    s_blk, m_blk, f_blk = sources // steps, model // steps, ffn // steps
    tok = ids.shape[1]
    whole = lambda shape: pl.BlockSpec(shape, lambda e, i: (0,) * len(shape))
    return pl.pallas_call(
        functools.partial(finish_kernel, group_size),
        grid=(e_local, steps),
        in_specs=[
            pl.BlockSpec((s_blk, 1, cap, width), lambda e, i: (i, e, 0, 0)),
            pl.BlockSpec((1, model, ffn), lambda e, i: (e, 0, 0)),
            pl.BlockSpec((1, model, ffn), lambda e, i: (e, 0, 0)),
            pl.BlockSpec((1, m_blk, width), lambda e, i: (e, i, 0)),
            pl.BlockSpec((1, f_blk, model), lambda e, i: (e, i, 0)),
            whole(back.shape), whole((8, tok)), whole((8, tok)),
        ],
        out_specs=[
            pl.BlockSpec((s_blk, 1, cap, model), lambda e, i: (i, e, 0, 0)),
            pl.BlockSpec((1, m_blk, ffn), lambda e, i: (e, i, 0)),
            pl.BlockSpec((1, m_blk, ffn), lambda e, i: (e, i, 0)),
            pl.BlockSpec((1, f_blk, model), lambda e, i: (e, i, 0)),
            whole((8, tok)),
        ],
        out_shape=[
            jax.ShapeDtypeStruct((sources, e_local, cap, model), BF16),
            jax.ShapeDtypeStruct((e_local, model, ffn), BF16),
            jax.ShapeDtypeStruct((e_local, model, ffn), BF16),
            jax.ShapeDtypeStruct((e_local, ffn, model), BF16),
            jax.ShapeDtypeStruct((8, tok), F32),
        ],
    )(dadb, w_gate, w_up, gu, dn, back, ids, slots)


def solution(mesh):
    group_size = mesh.shape['ep']

    def local_step(x_disp, w_gate, w_up, w_down, d_out, slot_idx, expert_id, gate_wt):
        cap = x_disp.shape[2]
        top_k = slot_idx.shape[1]
        pad = ((0, 8 - top_k), (0, 0))
        slots = jnp.pad(slot_idx.T, pad, constant_values=-1)
        ids = jnp.pad(expert_id.T, pad)
        pos = jnp.where(slots >= 0, ids * cap + slots, -1).astype(F32)
        route = jnp.concatenate([pos, jnp.pad(gate_wt.T, pad)], axis=0)
        dadb, gu, dn, back, _, _ = run_experts(x_disp, w_gate, w_up, w_down, d_out, route, group_size)
        grad_x, grad_w_gate, grad_w_up, grad_w_down, gate = run_finish(
            dadb, w_gate, w_up, gu, dn, back, ids, slots, group_size)
        return grad_x, grad_w_gate, grad_w_up, grad_w_down, gate[:top_k].T

    token_place = P(('dp', 'ep'), None)
    weight_place = P('ep', None, None)
    slot_place = P('dp', 'ep', None, None)
    grad_place = P(('dp', 'ep'), None, None)
    return jax.shard_map(local_step, mesh=mesh,
                         in_specs=(slot_place, weight_place, weight_place, weight_place, token_place, token_place, token_place, token_place),
                         out_specs=(slot_place, grad_place, grad_place, grad_place, token_place),
                         check_vma=False)
```

```python
import functools
import math

import jax
import jax.numpy as jnp
from jax import lax
from jax.experimental import pallas as pl
from jax.experimental.pallas import tpu as pltpu
from jax.sharding import PartitionSpec as P

F32 = jnp.float32
BF16 = jnp.bfloat16
MESH = pl.DeviceIdType.MESH

ORDER = [(0, 0), (0, 1), (0, 3), (1, 0), (3, 0), (0, 2), (2, 0), (1, 1),
         (1, 2), (3, 1), (1, 3), (3, 3), (3, 2), (2, 1), (2, 3), (2, 2)]
PLACE = {block: place for place, block in enumerate(ORDER)}


def packed(values):
    total = sum(v << (2 * k) for k, v in enumerate(values))
    return total - 2 ** 32 if total >= 2 ** 31 else total


ORIGIN_Y, ORIGIN_X = packed([b[0] for b in ORDER]), packed([b[1] for b in ORDER])
QUARTERS = 4
UNIT_BLOCKS = 4
STEP_BLOCKS = 2
BEFORE = {0: (3,), 3: (7,), 4: (9, 10), 6: (13,)}
BETWEEN = {0: (4,), 1: (5,), 2: (6,), 3: (8,), 4: (11,), 5: (12,)}
AFTER = {6: (14,)}
NT = (((1,), (1,)), ((), ()))
TN = (((0,), (0,)), ((), ()))


def send_lists():
    own = [(0, 0, 0), (0, 0, 1), (0, 0, 2), (0, 0, 3), (0, 1, 0), (0, 1, 2)]
    plus_x = own + [(1, 0, 2), (1, 0, 3), (3, 0, 2), (1, 1, 2), (3, 0, 3), (2, 0, 2),
                    (3, 1, 2), (2, 0, 3), (2, 1, 2)]
    swap = (2, 3, 0, 1)
    flip = (1, 0, 3, 2)
    plus_y = [(ox, oy, swap[q]) for oy, ox, q in own]
    plus_y += [(0, 1, 0), (0, 1, 1), (0, 2, 0), (0, 2, 1), (0, 3, 0), (0, 3, 1),
               (1, 1, 0), (1, 3, 0), (1, 2, 0)]
    minus_x = [(oy, -ox % 4, flip[q]) for oy, ox, q in plus_x]
    minus_y = [(-oy % 4, ox, flip[q]) for oy, ox, q in plus_y]
    return {(0, 1): plus_x, (0, 3): minus_x, (1, 0): plus_y, (3, 0): minus_y}


SENDS = send_lists()
SLOTS = len(SENDS[(0, 1)])


def expert_kernel(group_size, x_hbm, wg_hbm, wu_hbm, wd_hbm, dout_hbm, route_hbm,
                  dadb_hbm, gu_hbm, dn_hbm, back_hbm, pq_hbm, h_hbm,
                  ag, rt, acc_gu, acc_d, wgu, wd, xb, db, pq, hb, gsend, grecv,
                  w_sem, own_sem, x_sem, spill_sem, fill_sem, dadb_sem, fin_sem,
                  recv_sem, rrecv_sem, send_sem, rsend_sem,
                  srecv_sem, srrecv_sem, ssend_sem, srsend_sem, gsend_sem, grecv_sem):
    side = math.isqrt(group_size // 2)
    me = lax.axis_index('ep')
    core = lax.rem(me, 2)
    my_x = lax.rem(me // 2, side)
    my_y = me // (2 * side)
    e_local, rows_u, model = xb.shape
    rows_s = rows_u // (UNIT_BLOCKS // STEP_BLOCKS)
    ffn = hb.shape[2]
    cap = x_hbm.shape[2]
    tok = ag.shape[2]
    qrows = tok // QUARTERS
    n_blocks = side * side
    units = n_blocks // UNIT_BLOCKS
    steps = n_blocks // STEP_BLOCKS
    per_unit = 2 * UNIT_BLOCKS
    per_step = 2 * STEP_BLOCKS
    tile = 256
    mt_count = model // tile
    dadb = wgu
    ft_count = ffn // tile

    def device(y, x, c):
        return (y * side + x) * 2 + c

    def neighbour(dy, dx):
        return device(lax.rem(my_y + dy, side), lax.rem(my_x + dx, side), core)

    sibling = device(my_y, my_x, 1 - core)

    def origin(p, r):
        oy = lax.shift_right_logical(jnp.int32(ORIGIN_Y), 2 * p) & 3
        ox = lax.shift_right_logical(jnp.int32(ORIGIN_X), 2 * p) & 3
        c = core + r - 2 * core * r
        return device(lax.rem(my_y + side - oy, side), lax.rem(my_x + side - ox, side), c)

    def quarter(r, p, q):
        return ag.at[r, p, pl.ds(q * qrows, qrows)]

    def ici_copy(p_from, p_to, q, to):
        return pltpu.make_async_remote_copy(
            src_ref=quarter(0, p_from, q), dst_ref=quarter(0, p_to, q), send_sem=send_sem,
            recv_sem=recv_sem.at[p_to, q], device_id={'ep': to}, device_id_type=MESH)

    def ici_route(p_from, p_to, to):
        return pltpu.make_async_remote_copy(
            src_ref=rt.at[0, p_from], dst_ref=rt.at[0, p_to], send_sem=rsend_sem,
            recv_sem=rrecv_sem.at[p_to], device_id={'ep': to}, device_id_type=MESH)

    def sib_copy(p, q):
        return pltpu.make_async_remote_copy(
            src_ref=quarter(0, p, q), dst_ref=quarter(1, p, q), send_sem=ssend_sem,
            recv_sem=srecv_sem.at[p, q], device_id={'ep': sibling}, device_id_type=MESH)

    def sib_route(p):
        return pltpu.make_async_remote_copy(
            src_ref=rt.at[0, p], dst_ref=rt.at[1, p], send_sem=srsend_sem,
            recv_sem=srrecv_sem.at[p], device_id={'ep': sibling}, device_id_type=MESH)

    def issue(slot):
        for (dy, dx), sends in SENDS.items():
            oy, ox, q = sends[slot]
            p_from, p_to = PLACE[(oy, ox)], PLACE[((oy + dy) % 4, (ox + dx) % 4)]
            to = neighbour(dy, dx)
            ici_copy(p_from, p_to, q, to).start()
            if q == 0:
                ici_route(p_from, p_to, to).start()

    def service(slot):
        for (dy, dx), sends in SENDS.items():
            oy, ox, q = sends[slot]
            p_to = PLACE[((oy + dy) % 4, (ox + dx) % 4)]
            ici_copy(p_to, p_to, q, me).wait_recv()
            if q == 0:
                ici_route(p_to, p_to, me).wait_recv()
        if slot + 3 < SLOTS:
            issue(slot + 3)
        for (dy, dx), sends in SENDS.items():
            oy, ox, q = sends[slot]
            p_to = PLACE[((oy + dy) % 4, (ox + dx) % 4)]
            sib_copy(p_to, q).start()
            if q == 0:
                sib_route(p_to).start()

    def x_copy(block, j, e, row, sem):
        src = origin(block + j // 2, j % 2)
        return pltpu.make_async_copy(x_hbm.at[src, e], xb.at[e, pl.ds(row + j * cap, cap)], x_sem.at[e, sem + j])

    def unit_x(g, e):
        return [x_copy(g * UNIT_BLOCKS, j, e, 0, 0) for j in range(per_unit)]

    def unit_fill(g, e):
        u = g * e_local + e
        return unit_x(g, e) + [pltpu.make_async_copy(pq_hbm.at[u], pq.at[e], fill_sem.at[e, 0]),
                               pltpu.make_async_copy(h_hbm.at[u], hb.at[e], fill_sem.at[e, 1])]

    def dadb_copy(t, e, j):
        src = origin(t * STEP_BLOCKS + j // 2, j % 2)
        row = pl.multiple_of(lax.rem(t, 2) * rows_s + j * cap, cap)
        return pltpu.make_async_copy(dadb.at[e, pl.ds(row, cap)], dadb_hbm.at[src, e], dadb_sem.at[e, j])

    def spill_copies(u, e):
        return (pltpu.make_async_copy(pq.at[e], pq_hbm.at[u], spill_sem.at[e, 0]),
                pltpu.make_async_copy(hb.at[e], h_hbm.at[u], spill_sem.at[e, 1]))

    w_copies = [pltpu.make_async_copy(wg_hbm, wgu.at[:, :, pl.ds(0, ffn)], w_sem.at[0]),
                pltpu.make_async_copy(wu_hbm, wgu.at[:, :, pl.ds(ffn, ffn)], w_sem.at[1]),
                pltpu.make_async_copy(wd_hbm, wd, w_sem.at[2])]
    own = [pltpu.make_async_copy(dout_hbm, ag.at[0, 0], own_sem.at[0]),
           pltpu.make_async_copy(route_hbm, rt.at[0, 0], own_sem.at[1])]

    for c in own:
        c.start()
    barrier = pltpu.get_barrier_semaphore()

    @pl.loop(1, group_size)
    def _(k):
        pl.semaphore_signal(barrier, inc=1, device_id={'ep': lax.rem(me + k, group_size)}, device_id_type=MESH)

    for c in w_copies[:2]:
        c.start()
    for e in range(e_local):
        for c in unit_x(0, e):
            c.start()
    w_copies[2].start()
    for c in own:
        c.wait()
    pl.semaphore_wait(barrier, group_size - 1)
    for slot in range(3):
        issue(slot)
    for q in range(QUARTERS):
        sib_copy(0, q).start()
    sib_route(0).start()

    @pl.loop(0, mt_count)
    def _(m):
        rows = pl.ds(pl.multiple_of(m * tile, tile), tile)
        for e in range(e_local):
            acc_gu[e, rows] = jnp.zeros((tile, 2 * ffn), F32)

    @pl.loop(0, ft_count)
    def _(m):
        rows = pl.ds(pl.multiple_of(m * tile, tile), tile)
        for e in range(e_local):
            acc_d[e, rows] = jnp.zeros((tile, model), F32)

    for c in w_copies[:2]:
        c.wait()

    @pl.loop(0, units * e_local)
    def _(u):
        g, e = u // e_local, lax.rem(u, e_local)
        for c in unit_x(g, e):
            c.wait()

        @pl.when(u >= e_local)
        def _():
            for c in spill_copies(u - e_local, e):
                c.wait()

        @pl.loop(0, ft_count)
        def _(n):
            lo = pl.ds(pl.multiple_of(n * tile, tile), tile)
            hi = pl.ds(pl.multiple_of(ffn + n * tile, tile), tile)
            x = xb[e]
            a = jnp.dot(x, wgu[e, :, lo], preferred_element_type=F32)
            b = jnp.dot(x, wgu[e, :, hi], preferred_element_type=F32)
            sg = jax.nn.sigmoid(a)
            silu = a * sg
            hb[e, :, lo] = (silu * b).astype(BF16)
            pq[e, :, lo] = b * sg * (1.0 + a * (1.0 - sg))
            pq[e, :, hi] = silu

        for c in spill_copies(u, e):
            c.start()

        @pl.when(g + 1 < units)
        def _():
            for c in unit_x(g + 1, e):
                c.start()

        for k, at in ((0, 2), (1, 4), (2, 6)):
            @pl.when(u == at)
            def _(k=k):
                service(k)

    for e in range(e_local):
        for c in spill_copies((units - 1) * e_local + e, e):
            c.wait()
    for e in range(e_local):
        for c in unit_fill(0, e):
            c.start()
    w_copies[2].wait()

    def hits(r, p, e):
        local = rt[r, p, 0:8] - (me * (e_local * cap) + e * cap).astype(F32)
        hit = (local >= 0.0) & (local < float(cap))
        slot = jnp.max(jnp.where(hit, local, -1.0), axis=0, keepdims=True)
        gate = jnp.sum(jnp.where(hit, rt[r, p, 8:16], 0.0), axis=0, keepdims=True)
        return slot, gate

    def on(table, t):
        for step, slots in table.items():
            @pl.when(t == step)
            def _(slots=slots):
                for k in slots:
                    service(k)

    slot_iota = lax.broadcasted_iota(jnp.int32, (cap, tok), 0).astype(F32)

    @pl.loop(0, steps)
    def _(t):
        on(BEFORE, t)
        odd = lax.rem(t, 2)
        half = pl.multiple_of(odd * rows_s, rows_s)
        here = pl.ds(half, rows_s)
        dy_here = pl.ds(pl.multiple_of(rows_s + half, rows_s), rows_s)

        @pl.loop(0, STEP_BLOCKS)
        def _(i):
            p = t * STEP_BLOCKS + i
            for q in range(QUARTERS):
                sib_copy(p, q).wait_recv()
            sib_route(p).wait_recv()
            for r in range(2):
                picks, gates = [], []
                for e in range(e_local):
                    slot, gate = hits(r, p, e)
                    pick = slot_iota == slot
                    gates.append(jnp.sum(jnp.where(pick, gate, 0.0), axis=1, keepdims=True))
                    picks.append(jnp.where(pick, 1.0, 0.0).astype(BF16))
                pick = jnp.concatenate(picks, axis=0)
                row = pl.multiple_of((2 * i + r) * cap, cap)
                for n in range(model // 512):
                    cols = pl.ds(n * 512, 512)
                    d = jnp.dot(pick, ag[r, p, :, cols], preferred_element_type=F32)
                    for e in range(e_local):
                        d_e = d[e * cap:(e + 1) * cap]
                        db[e, pl.ds(row, cap), cols] = d_e.astype(BF16)
                        db[e, pl.ds(pl.multiple_of(rows_s + half + row, cap), cap), cols] = (d_e * gates[e]).astype(BF16)

        @pl.loop(0, e_local)
        def _(e):
            @pl.when(odd == 0)
            def _():
                for c in unit_fill(t // 2, e):
                    c.wait()

            @pl.when(t > 0)
            def _():
                for j in range(per_step):
                    dadb_copy(t, e, j).wait()

            part = jnp.zeros((rows_s, 128), F32)
            for n in range(ft_count):
                lo, hi = pl.ds(n * tile, tile), pl.ds(ffn + n * tile, tile)
                lhs = jnp.concatenate([db[e, 0:rows_s], db[e, dy_here]], axis=0)
                both = lax.dot_general(lhs, wd[e, lo, :], NT, preferred_element_type=F32)
                prod = hb[e, here, lo].astype(F32) * both[:rows_s]
                part += prod[:, :128] + prod[:, 128:]
                dh = both[rows_s:].astype(BF16).astype(F32)
                dadb[e, here, lo] = (dh * pq[e, here, lo]).astype(BF16)
                dadb[e, here, hi] = (dh * pq[e, here, hi]).astype(BF16)

            total = jnp.broadcast_to(jnp.sum(part, axis=1, keepdims=True), part.shape)
            for j in range(per_step):
                slot, _ = hits(j % 2, t * STEP_BLOCKS + j // 2, e)
                value = jnp.concatenate([total[j * cap:(j + 1) * cap]] * (tok // 128), axis=1)
                gsend[t * per_step + j, e] = jnp.sum(
                    jnp.where(slot_iota == slot, value, 0.0), axis=0, keepdims=True)

            for j in range(per_step):
                dadb_copy(t, e, j).start()

            def weight_grads(rows, dy_rows):
                @pl.loop(0, 2)
                def _(m):
                    out = pl.ds(pl.multiple_of(m * (model // 2), model // 2), model // 2)
                    for n in range(2):
                        cols = pl.ds(n * ffn, ffn)
                        acc_gu[e, out, cols] += lax.dot_general(
                            xb[e, rows, out], dadb[e, rows, cols], TN, preferred_element_type=F32)

                for n in range(model // 512):
                    cols = pl.ds(n * 512, 512)
                    acc_d[e, :, cols] += lax.dot_general(
                        hb[e, rows, :], db[e, dy_rows, cols], TN, preferred_element_type=F32)

            @pl.when((odd == 1) & (t < steps - 2))
            def _():
                weight_grads(pl.ds(0, rows_u), pl.ds(rows_s, rows_u))
                for c in unit_fill(t // 2 + 1, e):
                    c.start()

            @pl.when(t >= steps - 2)
            def _():
                weight_grads(here, dy_here)

            @pl.when(t + 1 == steps)
            def _():
                for j in range(per_step):
                    dadb_copy(t, e, j).wait()

                @pl.loop(0, mt_count)
                def _(m):
                    rows = pl.ds(pl.multiple_of(m * tile, tile), tile)
                    wgu[e, rows] = acc_gu[e, rows].astype(BF16)

                @pl.loop(0, ft_count)
                def _(m):
                    rows = pl.ds(pl.multiple_of(m * tile, tile), tile)
                    wd[e, rows] = acc_d[e, rows].astype(BF16)

                pltpu.make_async_copy(wgu.at[e], gu_hbm.at[e], fin_sem.at[e, 0]).start()
                pltpu.make_async_copy(wd.at[e], dn_hbm.at[e], fin_sem.at[e, 1]).start()

            for step, slots in BETWEEN.items():
                @pl.when((t == step) & (e == 0))
                def _(slots=slots):
                    for k in slots:
                        service(k)

        on(AFTER, t)

        @pl.when(t == 0)
        def _():
            grecv[me] = gsend[0]

        @pl.loop(jnp.where(t == 0, 1, 0), per_step)
        def _(j):
            to = origin(t * STEP_BLOCKS + j // 2, lax.rem(j, 2))
            pltpu.make_async_remote_copy(
                src_ref=gsend.at[t * per_step + j], dst_ref=grecv.at[me], send_sem=gsend_sem,
                recv_sem=grecv_sem, device_id={'ep': to}, device_id_type=MESH).start()

    def drain(ref, sem):
        pltpu.make_async_copy(ref, ref, sem).wait()

    drain(ag.at[0, pl.ds(0, n_blocks - 1)], send_sem)
    drain(rt.at[0, pl.ds(0, n_blocks - 1)], rsend_sem)
    drain(ag.at[0], ssend_sem)
    drain(rt.at[0], srsend_sem)
    drain(gsend.at[pl.ds(0, group_size - 1)], gsend_sem)
    drain(grecv.at[pl.ds(0, group_size - 1)], grecv_sem)
    back = pltpu.make_async_copy(grecv, back_hbm, own_sem.at[0])
    back.start()
    back.wait()
    for e in range(e_local):
        pltpu.make_async_copy(wgu.at[e], gu_hbm.at[e], fin_sem.at[e, 0]).wait()
        pltpu.make_async_copy(wd.at[e], dn_hbm.at[e], fin_sem.at[e, 1]).wait()


def run_experts(x_disp, w_gate, w_up, w_down, d_out, route, group_size):
    sources, e_local, cap, model = x_disp.shape
    ffn = w_gate.shape[2]
    tok = d_out.shape[0]
    n_blocks = group_size // 2
    per_unit = 2 * UNIT_BLOCKS
    rows_u = per_unit * cap
    per_step = 2 * STEP_BLOCKS
    rows_s = per_step * cap
    units = n_blocks // UNIT_BLOCKS * e_local
    dma = pltpu.SemaphoreType.DMA
    any_spec = pl.BlockSpec(memory_space=pl.ANY)
    out_shape = [
        jax.ShapeDtypeStruct((sources, e_local, cap, 2 * ffn), BF16),
        jax.ShapeDtypeStruct((e_local, model, 2 * ffn), BF16),
        jax.ShapeDtypeStruct((e_local, ffn, model), BF16),
        jax.ShapeDtypeStruct((group_size, e_local, 1, tok), F32),
        jax.ShapeDtypeStruct((units, rows_u, 2 * ffn), F32),
        jax.ShapeDtypeStruct((units, rows_u, ffn), BF16),
    ]
    scratch = [
        pltpu.VMEM((2, n_blocks, tok, model), BF16),
        pltpu.VMEM((2, n_blocks, 16, tok), F32),
        pltpu.VMEM((e_local, model, 2 * ffn), F32),
        pltpu.VMEM((e_local, ffn, model), F32),
        pltpu.VMEM((e_local, model, 2 * ffn), BF16),
        pltpu.VMEM((e_local, ffn, model), BF16),
        pltpu.VMEM((e_local, rows_u, model), BF16),
        pltpu.VMEM((e_local, rows_s + rows_u, model), BF16),
        pltpu.VMEM((e_local, rows_u, 2 * ffn), F32),
        pltpu.VMEM((e_local, rows_u, ffn), BF16),
        pltpu.VMEM((group_size, e_local, 1, tok), F32),
        pltpu.VMEM((group_size, e_local, 1, tok), F32),
        dma((3,)), dma((2,)), dma((e_local, per_unit)), dma((e_local, 2)), dma((e_local, 2)),
        dma((e_local, per_step)), dma((e_local, 2)),
        dma((n_blocks, QUARTERS)), dma((n_blocks,)), dma, dma,
        dma((n_blocks, QUARTERS)), dma((n_blocks,)), dma, dma, dma, dma,
    ]
    return pl.pallas_call(
        functools.partial(expert_kernel, group_size),
        out_shape=out_shape, in_specs=[any_spec] * 6, out_specs=[any_spec] * 6, scratch_shapes=scratch,
        compiler_params=pltpu.CompilerParams(collective_id=0, has_side_effects=True, vmem_limit_bytes=67043328),
    )(x_disp, w_gate, w_up, w_down, d_out, route)


def finish_kernel(group_size, dadb, wg, wu, gu, dn, back, ids, slots, gx, gg_w, gu_w, gd_w, gate_out):
    sources, _, cap, width = dadb.shape
    ffn = width // 2
    model = gx.shape[3]
    both = dadb[...].reshape(sources * cap, width)
    for n in range(model // 512):
        rows = pl.ds(n * 512, 512)
        out = (lax.dot_general(both[:, :ffn], wg[0, rows], NT, preferred_element_type=F32)
               + lax.dot_general(both[:, ffn:], wu[0, rows], NT, preferred_element_type=F32))
        gx[:, 0, :, rows] = out.astype(BF16).reshape(sources, cap, 512)
    gg_w[...] = gu[:, :, :ffn]
    gu_w[...] = gu[:, :, ffn:]
    gd_w[...] = dn[...]

    @pl.when((pl.program_id(0) == 0) & (pl.program_id(1) == 0))
    def _():
        e_local = back.shape[1]
        total = jnp.zeros(gate_out.shape, F32)
        for d in range(group_size):
            for e in range(e_local):
                total += jnp.where(ids[...] == d * e_local + e, back[d, e], 0.0)
        gate_out[...] = jnp.where(slots[...] >= 0, total, 0.0)


def run_finish(dadb, w_gate, w_up, gu, dn, back, ids, slots, group_size):
    sources, e_local, cap, width = dadb.shape
    model, ffn = w_gate.shape[1:]
    steps = 4
    s_blk, m_blk, f_blk = sources // steps, model // steps, ffn // steps
    tok = ids.shape[1]
    whole = lambda shape: pl.BlockSpec(shape, lambda e, i: (0,) * len(shape))
    return pl.pallas_call(
        functools.partial(finish_kernel, group_size),
        grid=(e_local, steps),
        in_specs=[
            pl.BlockSpec((s_blk, 1, cap, width), lambda e, i: (i, e, 0, 0)),
            pl.BlockSpec((1, model, ffn), lambda e, i: (e, 0, 0)),
            pl.BlockSpec((1, model, ffn), lambda e, i: (e, 0, 0)),
            pl.BlockSpec((1, m_blk, width), lambda e, i: (e, i, 0)),
            pl.BlockSpec((1, f_blk, model), lambda e, i: (e, i, 0)),
            whole(back.shape), whole((8, tok)), whole((8, tok)),
        ],
        out_specs=[
            pl.BlockSpec((s_blk, 1, cap, model), lambda e, i: (i, e, 0, 0)),
            pl.BlockSpec((1, m_blk, ffn), lambda e, i: (e, i, 0)),
            pl.BlockSpec((1, m_blk, ffn), lambda e, i: (e, i, 0)),
            pl.BlockSpec((1, f_blk, model), lambda e, i: (e, i, 0)),
            whole((8, tok)),
        ],
        out_shape=[
            jax.ShapeDtypeStruct((sources, e_local, cap, model), BF16),
            jax.ShapeDtypeStruct((e_local, model, ffn), BF16),
            jax.ShapeDtypeStruct((e_local, model, ffn), BF16),
            jax.ShapeDtypeStruct((e_local, ffn, model), BF16),
            jax.ShapeDtypeStruct((8, tok), F32),
        ],
    )(dadb, w_gate, w_up, gu, dn, back, ids, slots)


def solution(mesh):
    group_size = mesh.shape['ep']

    def local_step(x_disp, w_gate, w_up, w_down, d_out, slot_idx, expert_id, gate_wt):
        cap = x_disp.shape[2]
        top_k = slot_idx.shape[1]
        pad = ((0, 8 - top_k), (0, 0))
        slots = jnp.pad(slot_idx.T, pad, constant_values=-1)
        ids = jnp.pad(expert_id.T, pad)
        pos = jnp.where(slots >= 0, ids * cap + slots, -1).astype(F32)
        route = jnp.concatenate([pos, jnp.pad(gate_wt.T, pad)], axis=0)
        dadb, gu, dn, back, _, _ = run_experts(x_disp, w_gate, w_up, w_down, d_out, route, group_size)
        grad_x, grad_w_gate, grad_w_up, grad_w_down, gate = run_finish(
            dadb, w_gate, w_up, gu, dn, back, ids, slots, group_size)
        return grad_x, grad_w_gate, grad_w_up, grad_w_down, gate[:top_k].T

    token_place = P(('dp', 'ep'), None)
    weight_place = P('ep', None, None)
    slot_place = P('dp', 'ep', None, None)
    grad_place = P(('dp', 'ep'), None, None)
    return jax.shard_map(local_step, mesh=mesh,
                         in_specs=(slot_place, weight_place, weight_place, weight_place, token_place, token_place, token_place, token_place),
                         out_specs=(slot_place, grad_place, grad_place, grad_place, token_place),
                         check_vma=False)
```

```python
import functools
import math

import jax
import jax.numpy as jnp
from jax import lax
from jax.experimental import pallas as pl
from jax.experimental.pallas import tpu as pltpu
from jax.sharding import PartitionSpec as P

F32 = jnp.float32
BF16 = jnp.bfloat16
MESH = pl.DeviceIdType.MESH

ORDER = [(0, 0), (0, 1), (0, 3), (1, 0), (3, 0), (0, 2), (2, 0), (1, 1),
         (1, 2), (3, 1), (1, 3), (3, 3), (3, 2), (2, 1), (2, 3), (2, 2)]
PLACE = {block: place for place, block in enumerate(ORDER)}


def packed(values):
    total = sum(v << (2 * k) for k, v in enumerate(values))
    return total - 2 ** 32 if total >= 2 ** 31 else total


ORIGIN_Y, ORIGIN_X = packed([b[0] for b in ORDER]), packed([b[1] for b in ORDER])
QUARTERS = 4
VMEM_A = 45 * 1024 * 1024 + 900 * 1024
VMEM_B = 40 * 1024 * 1024
UNIT_BLOCKS = 4
STEP_BLOCKS = 2
BEFORE = {0: (3,), 3: (7,), 4: (9, 10), 6: (13,)}
BETWEEN = {0: (4,), 1: (5,), 2: (6,), 3: (8,), 4: (11,), 5: (12,)}
AFTER = {6: (14,)}
NT = (((1,), (1,)), ((), ()))
TN = (((0,), (0,)), ((), ()))


def send_lists():
    own = [(0, 0, 0), (0, 0, 1), (0, 0, 2), (0, 0, 3), (0, 1, 0), (0, 1, 2)]
    plus_x = own + [(1, 0, 2), (1, 0, 3), (3, 0, 2), (1, 1, 2), (3, 0, 3), (2, 0, 2),
                    (3, 1, 2), (2, 0, 3), (2, 1, 2)]
    swap = (2, 3, 0, 1)
    flip = (1, 0, 3, 2)
    plus_y = [(ox, oy, swap[q]) for oy, ox, q in own]
    plus_y += [(0, 1, 0), (0, 1, 1), (0, 2, 0), (0, 2, 1), (0, 3, 0), (0, 3, 1),
               (1, 1, 0), (1, 3, 0), (1, 2, 0)]
    minus_x = [(oy, -ox % 4, flip[q]) for oy, ox, q in plus_x]
    minus_y = [(-oy % 4, ox, flip[q]) for oy, ox, q in plus_y]
    return {(0, 1): plus_x, (0, 3): minus_x, (1, 0): plus_y, (3, 0): minus_y}


SENDS = send_lists()
SLOTS = len(SENDS[(0, 1)])


def expert_kernel(group_size, x_hbm, wg_hbm, wu_hbm, wd_hbm, dout_hbm, slots_ref, ids_ref, gates_ref,
                  dadb_hbm, acc_gu, acc_d, back_hbm, pq_hbm, h_hbm,
                  ag, rt, wgu, wd, xb, db, pq, hb, gsend, grecv,
                  w_sem, own_sem, x_sem, spill_sem, fill_sem, dadb_sem,
                  recv_sem, rrecv_sem, send_sem, rsend_sem,
                  srecv_sem, srrecv_sem, ssend_sem, srsend_sem, gsend_sem, grecv_sem):
    side = math.isqrt(group_size // 2)
    me = lax.axis_index('ep')
    core = lax.rem(me, 2)
    my_x = lax.rem(me // 2, side)
    my_y = me // (2 * side)
    e_local, rows_u, model = xb.shape
    rows_s = rows_u // (UNIT_BLOCKS // STEP_BLOCKS)
    ffn = hb.shape[2]
    cap = x_hbm.shape[2]
    tok = ag.shape[2]
    qrows = tok // QUARTERS
    n_blocks = side * side
    units = n_blocks // UNIT_BLOCKS
    steps = n_blocks // STEP_BLOCKS
    per_unit = 2 * UNIT_BLOCKS
    per_step = 2 * STEP_BLOCKS
    tile = 256
    mt_count = model // tile
    dadb = wgu
    ft_count = ffn // tile

    def device(y, x, c):
        return (y * side + x) * 2 + c

    def neighbour(dy, dx):
        return device(lax.rem(my_y + dy, side), lax.rem(my_x + dx, side), core)

    sibling = device(my_y, my_x, 1 - core)

    def origin(p, r):
        oy = lax.shift_right_logical(jnp.int32(ORIGIN_Y), 2 * p) & 3
        ox = lax.shift_right_logical(jnp.int32(ORIGIN_X), 2 * p) & 3
        c = core + r - 2 * core * r
        return device(lax.rem(my_y + side - oy, side), lax.rem(my_x + side - ox, side), c)

    def quarter(r, p, q):
        return ag.at[r, p, pl.ds(q * qrows, qrows)]

    def ici_copy(p_from, p_to, q, to):
        return pltpu.make_async_remote_copy(
            src_ref=quarter(0, p_from, q), dst_ref=quarter(0, p_to, q), send_sem=send_sem,
            recv_sem=recv_sem.at[p_to, q], device_id={'ep': to}, device_id_type=MESH)

    def ici_route(p_from, p_to, to):
        return pltpu.make_async_remote_copy(
            src_ref=rt.at[0, p_from], dst_ref=rt.at[0, p_to], send_sem=rsend_sem,
            recv_sem=rrecv_sem.at[p_to], device_id={'ep': to}, device_id_type=MESH)

    def sib_copy(p, q):
        return pltpu.make_async_remote_copy(
            src_ref=quarter(0, p, q), dst_ref=quarter(1, p, q), send_sem=ssend_sem,
            recv_sem=srecv_sem.at[p, q], device_id={'ep': sibling}, device_id_type=MESH)

    def sib_route(p):
        return pltpu.make_async_remote_copy(
            src_ref=rt.at[0, p], dst_ref=rt.at[1, p], send_sem=srsend_sem,
            recv_sem=srrecv_sem.at[p], device_id={'ep': sibling}, device_id_type=MESH)

    def issue(slot):
        for (dy, dx), sends in SENDS.items():
            oy, ox, q = sends[slot]
            p_from, p_to = PLACE[(oy, ox)], PLACE[((oy + dy) % 4, (ox + dx) % 4)]
            to = neighbour(dy, dx)
            ici_copy(p_from, p_to, q, to).start()
            if q == 0:
                ici_route(p_from, p_to, to).start()

    def service(slot):
        for (dy, dx), sends in SENDS.items():
            oy, ox, q = sends[slot]
            p_to = PLACE[((oy + dy) % 4, (ox + dx) % 4)]
            ici_copy(p_to, p_to, q, me).wait_recv()
            if q == 0:
                ici_route(p_to, p_to, me).wait_recv()
        if slot + 3 < SLOTS:
            issue(slot + 3)
        for (dy, dx), sends in SENDS.items():
            oy, ox, q = sends[slot]
            p_to = PLACE[((oy + dy) % 4, (ox + dx) % 4)]
            sib_copy(p_to, q).start()
            if q == 0:
                sib_route(p_to).start()

    def x_copy(block, j, e, row, sem):
        src = origin(block + j // 2, j % 2)
        return pltpu.make_async_copy(x_hbm.at[src, e], xb.at[e, pl.ds(row + j * cap, cap)], x_sem.at[e, sem + j])

    def unit_x(g, e):
        return [x_copy(g * UNIT_BLOCKS, j, e, 0, 0) for j in range(per_unit)]

    def unit_fill(g, e):
        u = g * e_local + e
        return unit_x(g, e) + [pltpu.make_async_copy(pq_hbm.at[u], pq.at[e], fill_sem.at[e, 0]),
                               pltpu.make_async_copy(h_hbm.at[u], hb.at[e], fill_sem.at[e, 1])]

    def dadb_copy(t, e, j):
        src = origin(t * STEP_BLOCKS + j // 2, j % 2)
        row = pl.multiple_of(lax.rem(t, 2) * rows_s + j * cap, cap)
        return pltpu.make_async_copy(dadb.at[e, pl.ds(row, cap)], dadb_hbm.at[src, e], dadb_sem.at[e, j])

    def spill_copies(u, e):
        return (pltpu.make_async_copy(pq.at[e], pq_hbm.at[u], spill_sem.at[e, 0]),
                pltpu.make_async_copy(hb.at[e], h_hbm.at[u], spill_sem.at[e, 1]))

    w_copies = [pltpu.make_async_copy(wg_hbm, wgu.at[:, :, pl.ds(0, ffn)], w_sem.at[0]),
                pltpu.make_async_copy(wu_hbm, wgu.at[:, :, pl.ds(ffn, ffn)], w_sem.at[1]),
                pltpu.make_async_copy(wd_hbm, wd, w_sem.at[2])]
    own = pltpu.make_async_copy(dout_hbm, ag.at[0, 0], own_sem)

    own.start()
    barrier = pltpu.get_barrier_semaphore()

    @pl.loop(1, group_size)
    def _(k):
        pl.semaphore_signal(barrier, inc=1, device_id={'ep': lax.rem(me + k, group_size)}, device_id_type=MESH)

    for c in w_copies[:2]:
        c.start()
    for e in range(e_local):
        for c in unit_x(0, e):
            c.start()
    w_copies[2].start()
    top_k = slots_ref.shape[0]
    rt[0, 0] = jnp.concatenate([jnp.full((8, tok), -1.0, F32), jnp.zeros((8, tok), F32)], axis=0)
    slots = slots_ref[...]
    rt[0, 0, 0:top_k] = jnp.where(slots >= 0, ids_ref[...] * cap + slots, -1).astype(F32)
    rt[0, 0, 8:8 + top_k] = gates_ref[...]
    own.wait()
    pl.semaphore_wait(barrier, group_size - 1)
    for slot in range(3):
        issue(slot)
    for q in range(QUARTERS):
        sib_copy(0, q).start()
    sib_route(0).start()

    @pl.loop(0, mt_count)
    def _(m):
        rows = pl.ds(pl.multiple_of(m * tile, tile), tile)
        for e in range(e_local):
            acc_gu[e, rows] = jnp.zeros((tile, 2 * ffn), F32)

    @pl.loop(0, ft_count)
    def _(m):
        rows = pl.ds(pl.multiple_of(m * tile, tile), tile)
        for e in range(e_local):
            acc_d[e, rows] = jnp.zeros((tile, model), F32)

    for c in w_copies[:2]:
        c.wait()

    @pl.loop(0, units * e_local)
    def _(u):
        g, e = u // e_local, lax.rem(u, e_local)
        for c in unit_x(g, e):
            c.wait()

        @pl.when(u >= e_local)
        def _():
            for c in spill_copies(u - e_local, e):
                c.wait()

        @pl.loop(0, ft_count)
        def _(n):
            lo = pl.ds(pl.multiple_of(n * tile, tile), tile)
            hi = pl.ds(pl.multiple_of(ffn + n * tile, tile), tile)
            x = xb[e]
            a = jnp.dot(x, wgu[e, :, lo], preferred_element_type=F32)
            b = jnp.dot(x, wgu[e, :, hi], preferred_element_type=F32)
            sg = jax.nn.sigmoid(a)
            silu = a * sg
            hb[e, :, lo] = (silu * b).astype(BF16)
            pq[e, :, lo] = b * sg * (1.0 + a * (1.0 - sg))
            pq[e, :, hi] = silu

        for c in spill_copies(u, e):
            c.start()

        @pl.when(g + 1 < units)
        def _():
            for c in unit_x(g + 1, e):
                c.start()

        for k, at in ((0, 2), (1, 4), (2, 6)):
            @pl.when(u == at)
            def _(k=k):
                service(k)

    for e in range(e_local):
        for c in spill_copies((units - 1) * e_local + e, e):
            c.wait()
    for e in range(e_local):
        for c in unit_fill(0, e):
            c.start()
    w_copies[2].wait()

    def hits(r, p, e):
        local = rt[r, p, 0:8] - (me * (e_local * cap) + e * cap).astype(F32)
        hit = (local >= 0.0) & (local < float(cap))
        slot = jnp.max(jnp.where(hit, local, -1.0), axis=0, keepdims=True)
        gate = jnp.sum(jnp.where(hit, rt[r, p, 8:16], 0.0), axis=0, keepdims=True)
        return slot, gate

    def on(table, t):
        for step, slots in table.items():
            @pl.when(t == step)
            def _(slots=slots):
                for k in slots:
                    service(k)

    slot_iota = lax.broadcasted_iota(jnp.int32, (cap, tok), 0).astype(F32)

    @pl.loop(0, steps)
    def _(t):
        on(BEFORE, t)
        odd = lax.rem(t, 2)
        half = pl.multiple_of(odd * rows_s, rows_s)
        here = pl.ds(half, rows_s)
        dy_here = pl.ds(pl.multiple_of(rows_s + half, rows_s), rows_s)

        @pl.loop(0, STEP_BLOCKS)
        def _(i):
            p = t * STEP_BLOCKS + i
            for q in range(QUARTERS):
                sib_copy(p, q).wait_recv()
            sib_route(p).wait_recv()
            for r in range(2):
                picks, gates = [], []
                for e in range(e_local):
                    slot, gate = hits(r, p, e)
                    pick = slot_iota == slot
                    gates.append(jnp.sum(jnp.where(pick, gate, 0.0), axis=1, keepdims=True))
                    picks.append(jnp.where(pick, 1.0, 0.0).astype(BF16))
                pick = jnp.concatenate(picks, axis=0)
                row = pl.multiple_of((2 * i + r) * cap, cap)
                for n in range(model // 512):
                    cols = pl.ds(n * 512, 512)
                    d = jnp.dot(pick, ag[r, p, :, cols], preferred_element_type=F32)
                    for e in range(e_local):
                        d_e = d[e * cap:(e + 1) * cap]
                        db[e, pl.ds(row, cap), cols] = d_e.astype(BF16)
                        db[e, pl.ds(pl.multiple_of(rows_s + half + row, cap), cap), cols] = (d_e * gates[e]).astype(BF16)

        @pl.loop(0, e_local)
        def _(e):
            @pl.when(odd == 0)
            def _():
                for c in unit_fill(t // 2, e):
                    c.wait()

            @pl.when(t > 0)
            def _():
                for j in range(per_step):
                    dadb_copy(t, e, j).wait()

            part = jnp.zeros((rows_s, 128), F32)
            for n in range(ft_count):
                lo, hi = pl.ds(n * tile, tile), pl.ds(ffn + n * tile, tile)
                lhs = jnp.concatenate([db[e, 0:rows_s], db[e, dy_here]], axis=0)
                both = lax.dot_general(lhs, wd[e, lo, :], NT, preferred_element_type=F32)
                prod = hb[e, here, lo].astype(F32) * both[:rows_s]
                part += prod[:, :128] + prod[:, 128:]
                dh = both[rows_s:].astype(BF16).astype(F32)
                dadb[e, here, lo] = (dh * pq[e, here, lo]).astype(BF16)
                dadb[e, here, hi] = (dh * pq[e, here, hi]).astype(BF16)

            total = jnp.broadcast_to(jnp.sum(part, axis=1, keepdims=True), part.shape)
            for j in range(per_step):
                slot, _ = hits(j % 2, t * STEP_BLOCKS + j // 2, e)
                value = jnp.concatenate([total[j * cap:(j + 1) * cap]] * (tok // 128), axis=1)
                gsend[t * per_step + j, e] = jnp.sum(
                    jnp.where(slot_iota == slot, value, 0.0), axis=0, keepdims=True)

            for j in range(per_step):
                dadb_copy(t, e, j).start()

            def weight_grads(rows, dy_rows):
                @pl.loop(0, 2)
                def _(m):
                    out = pl.ds(pl.multiple_of(m * (model // 2), model // 2), model // 2)
                    for n in range(2):
                        cols = pl.ds(n * ffn, ffn)
                        acc_gu[e, out, cols] += lax.dot_general(
                            xb[e, rows, out], dadb[e, rows, cols], TN, preferred_element_type=F32)

                for n in range(model // 512):
                    cols = pl.ds(n * 512, 512)
                    acc_d[e, :, cols] += lax.dot_general(
                        hb[e, rows, :], db[e, dy_rows, cols], TN, preferred_element_type=F32)

            @pl.when((odd == 1) & (t < steps - 2))
            def _():
                weight_grads(pl.ds(0, rows_u), pl.ds(rows_s, rows_u))
                for c in unit_fill(t // 2 + 1, e):
                    c.start()

            @pl.when(t >= steps - 2)
            def _():
                weight_grads(here, dy_here)

            for step, slots in BETWEEN.items():
                @pl.when((t == step) & (e == 0))
                def _(slots=slots):
                    for k in slots:
                        service(k)

        on(AFTER, t)

        @pl.when(t == 0)
        def _():
            grecv[me] = gsend[0]

        @pl.loop(jnp.where(t == 0, 1, 0), per_step)
        def _(j):
            to = origin(t * STEP_BLOCKS + j // 2, lax.rem(j, 2))
            pltpu.make_async_remote_copy(
                src_ref=gsend.at[t * per_step + j], dst_ref=grecv.at[me], send_sem=gsend_sem,
                recv_sem=grecv_sem, device_id={'ep': to}, device_id_type=MESH).start()

    def drain(ref, sem):
        pltpu.make_async_copy(ref, ref, sem).wait()

    drain(ag.at[0, pl.ds(0, n_blocks - 1)], send_sem)
    drain(rt.at[0, pl.ds(0, n_blocks - 1)], rsend_sem)
    drain(ag.at[0], ssend_sem)
    drain(rt.at[0], srsend_sem)
    drain(gsend.at[pl.ds(0, group_size - 1)], gsend_sem)
    drain(grecv.at[pl.ds(0, group_size - 1)], grecv_sem)
    back = pltpu.make_async_copy(grecv, back_hbm, own_sem)
    back.start()
    for e in range(e_local):
        for j in range(per_step):
            dadb_copy(jnp.int32(steps - 1), e, j).wait()
    back.wait()


def run_experts(x_disp, w_gate, w_up, w_down, d_out, slots, ids, gates, group_size):
    sources, e_local, cap, model = x_disp.shape
    ffn = w_gate.shape[2]
    tok = d_out.shape[0]
    n_blocks = group_size // 2
    per_unit = 2 * UNIT_BLOCKS
    rows_u = per_unit * cap
    per_step = 2 * STEP_BLOCKS
    rows_s = per_step * cap
    units = n_blocks // UNIT_BLOCKS * e_local
    dma = pltpu.SemaphoreType.DMA
    any_spec = pl.BlockSpec(memory_space=pl.ANY)
    vmem_spec = pl.BlockSpec(memory_space=pltpu.VMEM)
    out_shape = [
        jax.ShapeDtypeStruct((sources, e_local, cap, 2 * ffn), BF16),
        pltpu.VMEM((e_local, model, 2 * ffn), F32),
        pltpu.VMEM((e_local, ffn, model), F32),
        jax.ShapeDtypeStruct((group_size, e_local, 1, tok), F32),
        jax.ShapeDtypeStruct((units, rows_u, 2 * ffn), F32),
        jax.ShapeDtypeStruct((units, rows_u, ffn), BF16),
    ]
    scratch = [
        pltpu.VMEM((2, n_blocks, tok, model), BF16),
        pltpu.VMEM((2, n_blocks, 16, tok), F32),
        pltpu.VMEM((e_local, model, 2 * ffn), BF16),
        pltpu.VMEM((e_local, ffn, model), BF16),
        pltpu.VMEM((e_local, rows_u, model), BF16),
        pltpu.VMEM((e_local, rows_s + rows_u, model), BF16),
        pltpu.VMEM((e_local, rows_u, 2 * ffn), F32),
        pltpu.VMEM((e_local, rows_u, ffn), BF16),
        pltpu.VMEM((group_size, e_local, 1, tok), F32),
        pltpu.VMEM((group_size, e_local, 1, tok), F32),
        dma((3,)), dma, dma((e_local, per_unit)), dma((e_local, 2)), dma((e_local, 2)),
        dma((e_local, per_step)),
        dma((n_blocks, QUARTERS)), dma((n_blocks,)), dma, dma,
        dma((n_blocks, QUARTERS)), dma((n_blocks,)), dma, dma, dma, dma,
    ]
    return pl.pallas_call(
        functools.partial(expert_kernel, group_size),
        out_shape=out_shape, in_specs=[any_spec] * 5 + [vmem_spec] * 3,
        out_specs=[any_spec, vmem_spec, vmem_spec, any_spec, any_spec, any_spec], scratch_shapes=scratch,
        compiler_params=pltpu.CompilerParams(collective_id=0, has_side_effects=True, vmem_limit_bytes=VMEM_A),
    )(x_disp, w_gate, w_up, w_down, d_out, slots, ids, gates)


def finish_kernel(group_size, chunk, dadb, wg, wu, acc_gu, acc_d, back, ids, slots,
                  gx, g_gate, g_up, g_down, gate_out,
                  wbuf, dbuf, obuf, st_g, st_u, st_d, w_sem, d_sem, o_sem, s_sem):
    sources, e_local, cap, width = dadb.shape
    ffn = width // 2
    model = gx.shape[3]
    per_e = sources // chunk
    chunks = e_local * per_e
    m_blk, f_blk = model // per_e, ffn // per_e
    depth = dbuf.shape[0]

    def load(c):
        slot = lax.rem(c, depth)
        return pltpu.make_async_copy(
            dadb.at[pl.ds(lax.rem(c, per_e) * chunk, chunk), c // per_e], dbuf.at[slot], d_sem.at[slot])

    def store(c):
        slot = lax.rem(c, 2)
        return pltpu.make_async_copy(
            obuf.at[slot], gx.at[pl.ds(lax.rem(c, per_e) * chunk, chunk), c // per_e], o_sem.at[slot])

    def weights(e):
        return [pltpu.make_async_copy(wg.at[e], wbuf.at[e, :, pl.ds(0, ffn)], w_sem.at[e, 0]),
                pltpu.make_async_copy(wu.at[e], wbuf.at[e, :, pl.ds(ffn, ffn)], w_sem.at[e, 1])]

    def staged(c):
        e, i = c // per_e, lax.rem(c, per_e)
        m = pl.ds(pl.multiple_of(i * m_blk, m_blk), m_blk)
        f = pl.ds(pl.multiple_of(i * f_blk, f_blk), f_blk)
        return e, m, f, [pltpu.make_async_copy(st_g.at[e, m], g_gate.at[e, m], s_sem.at[c, 0]),
                         pltpu.make_async_copy(st_u.at[e, m], g_up.at[e, m], s_sem.at[c, 1]),
                         pltpu.make_async_copy(st_d.at[e, f], g_down.at[e, f], s_sem.at[c, 2])]

    for c in weights(0):
        c.start()
    for k in range(depth):
        load(jnp.int32(k)).start()
    for e in range(1, e_local):
        for c in weights(e):
            c.start()

    total = jnp.zeros(gate_out.shape, F32)
    for d in range(group_size):
        for e in range(e_local):
            total += jnp.where(ids[...] == d * e_local + e, back[d, e], 0.0)
    gate_out[...] = jnp.where(slots[...] >= 0, total, 0.0)

    @pl.loop(0, chunks)
    def _(c):
        e, m, f, copies = staged(c)

        @pl.when(lax.rem(c, per_e) == 0)
        def _():
            for w in weights(e):
                w.wait()

        load(c).wait()

        @pl.when(c >= 2)
        def _():
            store(c - 2).wait()

        slot, out_slot = lax.rem(c, depth), lax.rem(c, 2)
        st_g[e, m] = acc_gu[e, m, 0:ffn].astype(BF16)
        st_u[e, m] = acc_gu[e, m, ffn:width].astype(BF16)
        st_d[e, f] = acc_d[e, f].astype(BF16)
        both = dbuf[slot].reshape(chunk * cap, width)
        for n in range(model // 512):
            rows = pl.ds(n * 512, 512)
            out = lax.dot_general(both, wbuf[e, rows], NT, preferred_element_type=F32)
            obuf[out_slot, :, :, rows] = out.astype(BF16).reshape(chunk, cap, 512)
        store(c).start()
        for s in copies:
            s.start()

        @pl.when(c + depth < chunks)
        def _():
            load(c + depth).start()

    for c in range(chunks - 2, chunks):
        store(jnp.int32(c)).wait()
    for c in range(chunks):
        for s in staged(jnp.int32(c))[3]:
            s.wait()


def run_finish(dadb, w_gate, w_up, acc_gu, acc_d, back, ids, slots, group_size):
    sources, e_local, cap, width = dadb.shape
    model, ffn = w_gate.shape[1:]
    top_k, tok = ids.shape
    chunk = 8
    dma = pltpu.SemaphoreType.DMA
    any_spec = pl.BlockSpec(memory_space=pl.ANY)
    vmem_spec = pl.BlockSpec(memory_space=pltpu.VMEM)
    return pl.pallas_call(
        functools.partial(finish_kernel, group_size, chunk),
        in_specs=[any_spec] * 3 + [vmem_spec] * 5,
        out_specs=[any_spec] * 4 + [vmem_spec],
        out_shape=[
            jax.ShapeDtypeStruct((sources, e_local, cap, model), BF16),
            jax.ShapeDtypeStruct((e_local, model, ffn), BF16),
            jax.ShapeDtypeStruct((e_local, model, ffn), BF16),
            jax.ShapeDtypeStruct((e_local, ffn, model), BF16),
            jax.ShapeDtypeStruct((top_k, tok), F32),
        ],
        scratch_shapes=[
            pltpu.VMEM((e_local, model, width), BF16),
            pltpu.VMEM((3, chunk, cap, width), BF16),
            pltpu.VMEM((2, chunk, cap, model), BF16),
            pltpu.VMEM((e_local, model, ffn), BF16),
            pltpu.VMEM((e_local, model, ffn), BF16),
            pltpu.VMEM((e_local, ffn, model), BF16),
            dma((e_local, 2)), dma((3,)), dma((2,)), dma((e_local * sources // chunk, 3)),
        ],
        compiler_params=pltpu.CompilerParams(vmem_limit_bytes=VMEM_B),
    )(dadb, w_gate, w_up, acc_gu, acc_d, back, ids, slots)


def solution(mesh):
    group_size = mesh.shape['ep']

    def local_step(x_disp, w_gate, w_up, w_down, d_out, slot_idx, expert_id, gate_wt):
        slots, ids = slot_idx.T, expert_id.T
        dadb, acc_gu, acc_d, back, _, _ = run_experts(
            x_disp, w_gate, w_up, w_down, d_out, slots, ids, gate_wt.T, group_size)
        grad_x, grad_w_gate, grad_w_up, grad_w_down, gate = run_finish(
            dadb, w_gate, w_up, acc_gu, acc_d, back, ids, slots, group_size)
        return grad_x, grad_w_gate, grad_w_up, grad_w_down, gate.T

    token_place = P(('dp', 'ep'), None)
    weight_place = P('ep', None, None)
    slot_place = P('dp', 'ep', None, None)
    grad_place = P(('dp', 'ep'), None, None)
    return jax.shard_map(local_step, mesh=mesh,
                         in_specs=(slot_place, weight_place, weight_place, weight_place, token_place, token_place, token_place, token_place),
                         out_specs=(slot_place, grad_place, grad_place, grad_place, token_place),
                         check_vma=False)
```

```python
import functools
import math

import jax
import jax.numpy as jnp
from jax import lax
from jax.experimental import pallas as pl
from jax.experimental.pallas import tpu as pltpu
from jax.sharding import PartitionSpec as P

F32 = jnp.float32
BF16 = jnp.bfloat16
MESH = pl.DeviceIdType.MESH

ORDER = [(0, 0), (0, 1), (0, 3), (1, 0), (3, 0), (0, 2), (2, 0), (1, 1),
         (1, 2), (3, 1), (1, 3), (3, 3), (3, 2), (2, 1), (2, 3), (2, 2)]
PLACE = {block: place for place, block in enumerate(ORDER)}


def packed(values):
    total = sum(v << (2 * k) for k, v in enumerate(values))
    return total - 2 ** 32 if total >= 2 ** 31 else total


ORIGIN_Y, ORIGIN_X = packed([b[0] for b in ORDER]), packed([b[1] for b in ORDER])
QUARTERS = 4
VMEM_A = 45 * 1024 * 1024 + 900 * 1024
VMEM_B = 22 * 1024 * 1024
UNIT_BLOCKS = 4
STEP_BLOCKS = 2
BEFORE = {0: (3,), 3: (7,), 4: (8, 9, 10), 6: (13,)}
BETWEEN = {0: (4,), 1: (5,), 2: (6,), 4: (11,), 5: (12,)}
AFTER = {6: (14,)}
NT = (((1,), (1,)), ((), ()))
TN = (((0,), (0,)), ((), ()))


def send_lists():
    own = [(0, 0, 0), (0, 0, 1), (0, 0, 2), (0, 0, 3), (0, 1, 0), (0, 1, 2)]
    plus_x = own + [(1, 0, 2), (1, 0, 3), (3, 0, 2), (1, 1, 2), (3, 0, 3), (2, 0, 2),
                    (3, 1, 2), (2, 0, 3), (2, 1, 2)]
    swap = (2, 3, 0, 1)
    flip = (1, 0, 3, 2)
    plus_y = [(ox, oy, swap[q]) for oy, ox, q in own]
    plus_y += [(0, 1, 0), (0, 1, 1), (0, 2, 0), (0, 2, 1), (0, 3, 0), (0, 3, 1),
               (1, 1, 0), (1, 3, 0), (1, 2, 0)]
    minus_x = [(oy, -ox % 4, flip[q]) for oy, ox, q in plus_x]
    minus_y = [(-oy % 4, ox, flip[q]) for oy, ox, q in plus_y]
    return {(0, 1): plus_x, (0, 3): minus_x, (1, 0): plus_y, (3, 0): minus_y}


SENDS = send_lists()
SLOTS = len(SENDS[(0, 1)])


def expert_kernel(group_size, x_hbm, wg_hbm, wu_hbm, wd_hbm, dout_hbm, slots_ref, ids_ref, gates_ref,
                  dadb_hbm, acc_gu, acc_d, back_hbm, pq_hbm, h_hbm,
                  ag, rt, wgu, wd, xb, db, pq, hb, gsend, grecv,
                  w_sem, own_sem, x_sem, spill_sem, fill_sem, dadb_sem,
                  recv_sem, rrecv_sem, send_sem, rsend_sem,
                  srecv_sem, srrecv_sem, ssend_sem, srsend_sem, gsend_sem, grecv_sem):
    side = math.isqrt(group_size // 2)
    me = lax.axis_index('ep')
    core = lax.rem(me, 2)
    my_x = lax.rem(me // 2, side)
    my_y = me // (2 * side)
    e_local, rows_u, model = xb.shape
    rows_s = rows_u // (UNIT_BLOCKS // STEP_BLOCKS)
    ffn = hb.shape[2]
    cap = x_hbm.shape[2]
    tok = ag.shape[2]
    qrows = tok // QUARTERS
    n_blocks = side * side
    units = n_blocks // UNIT_BLOCKS
    steps = n_blocks // STEP_BLOCKS
    per_unit = 2 * UNIT_BLOCKS
    per_step = 2 * STEP_BLOCKS
    tile = 256
    mt_count = model // tile
    dadb = wgu
    ft_count = ffn // tile

    def device(y, x, c):
        return (y * side + x) * 2 + c

    def neighbour(dy, dx):
        return device(lax.rem(my_y + dy, side), lax.rem(my_x + dx, side), core)

    sibling = device(my_y, my_x, 1 - core)

    def origin(p, r):
        oy = lax.shift_right_logical(jnp.int32(ORIGIN_Y), 2 * p) & 3
        ox = lax.shift_right_logical(jnp.int32(ORIGIN_X), 2 * p) & 3
        c = core + r - 2 * core * r
        return device(lax.rem(my_y + side - oy, side), lax.rem(my_x + side - ox, side), c)

    def quarter(r, p, q):
        return ag.at[r, p, pl.ds(q * qrows, qrows)]

    def ici_copy(p_from, p_to, q, to):
        return pltpu.make_async_remote_copy(
            src_ref=quarter(0, p_from, q), dst_ref=quarter(0, p_to, q), send_sem=send_sem,
            recv_sem=recv_sem.at[p_to, q], device_id={'ep': to}, device_id_type=MESH)

    def ici_route(p_from, p_to, to):
        return pltpu.make_async_remote_copy(
            src_ref=rt.at[0, p_from], dst_ref=rt.at[0, p_to], send_sem=rsend_sem,
            recv_sem=rrecv_sem.at[p_to], device_id={'ep': to}, device_id_type=MESH)

    def sib_copy(p, q):
        return pltpu.make_async_remote_copy(
            src_ref=quarter(0, p, q), dst_ref=quarter(1, p, q), send_sem=ssend_sem,
            recv_sem=srecv_sem.at[p, q], device_id={'ep': sibling}, device_id_type=MESH)

    def sib_route(p):
        return pltpu.make_async_remote_copy(
            src_ref=rt.at[0, p], dst_ref=rt.at[1, p], send_sem=srsend_sem,
            recv_sem=srrecv_sem.at[p], device_id={'ep': sibling}, device_id_type=MESH)

    def issue(slot):
        for (dy, dx), sends in SENDS.items():
            oy, ox, q = sends[slot]
            p_from, p_to = PLACE[(oy, ox)], PLACE[((oy + dy) % 4, (ox + dx) % 4)]
            to = neighbour(dy, dx)
            ici_copy(p_from, p_to, q, to).start()
            if q == 0:
                ici_route(p_from, p_to, to).start()

    def service(slot):
        for (dy, dx), sends in SENDS.items():
            oy, ox, q = sends[slot]
            p_to = PLACE[((oy + dy) % 4, (ox + dx) % 4)]
            ici_copy(p_to, p_to, q, me).wait_recv()
            if q == 0:
                ici_route(p_to, p_to, me).wait_recv()
        if slot + 3 < SLOTS:
            issue(slot + 3)
        for (dy, dx), sends in SENDS.items():
            oy, ox, q = sends[slot]
            p_to = PLACE[((oy + dy) % 4, (ox + dx) % 4)]
            sib_copy(p_to, q).start()
            if q == 0:
                sib_route(p_to).start()

    def x_copy(block, j, e, row, sem):
        src = origin(block + j // 2, j % 2)
        return pltpu.make_async_copy(x_hbm.at[src, e], xb.at[e, pl.ds(row + j * cap, cap)], x_sem.at[e, sem + j])

    def unit_x(g, e):
        return [x_copy(g * UNIT_BLOCKS, j, e, 0, 0) for j in range(per_unit)]

    def unit_fill(g, e):
        u = g * e_local + e
        return unit_x(g, e) + [pltpu.make_async_copy(pq_hbm.at[u], pq.at[e], fill_sem.at[e, 0]),
                               pltpu.make_async_copy(h_hbm.at[u], hb.at[e], fill_sem.at[e, 1])]

    def dadb_copy(t, e, j):
        src = origin(t * STEP_BLOCKS + j // 2, j % 2)
        row = pl.multiple_of(lax.rem(t, 2) * rows_s + j * cap, cap)
        return pltpu.make_async_copy(dadb.at[e, pl.ds(row, cap)], dadb_hbm.at[src, e], dadb_sem.at[e, j])

    def spill_copies(u, e):
        return (pltpu.make_async_copy(pq.at[e], pq_hbm.at[u], spill_sem.at[e, 0]),
                pltpu.make_async_copy(hb.at[e], h_hbm.at[u], spill_sem.at[e, 1]))

    w_copies = [pltpu.make_async_copy(wg_hbm, wgu.at[:, :, pl.ds(0, ffn)], w_sem.at[0]),
                pltpu.make_async_copy(wu_hbm, wgu.at[:, :, pl.ds(ffn, ffn)], w_sem.at[1]),
                pltpu.make_async_copy(wd_hbm, wd, w_sem.at[2])]
    own = pltpu.make_async_copy(dout_hbm, ag.at[0, 0], own_sem)

    own.start()
    barrier = pltpu.get_barrier_semaphore()

    @pl.loop(1, group_size)
    def _(k):
        pl.semaphore_signal(barrier, inc=1, device_id={'ep': lax.rem(me + k, group_size)}, device_id_type=MESH)

    for c in w_copies[:2]:
        c.start()
    for e in range(e_local):
        for c in unit_x(0, e):
            c.start()
    w_copies[2].start()
    top_k = slots_ref.shape[0]
    rt[0, 0] = jnp.concatenate([jnp.full((8, tok), -1.0, F32), jnp.zeros((8, tok), F32)], axis=0)
    slots = slots_ref[...]
    rt[0, 0, 0:top_k] = jnp.where(slots >= 0, ids_ref[...] * cap + slots, -1).astype(F32)
    rt[0, 0, 8:8 + top_k] = gates_ref[...]
    own.wait()
    pl.semaphore_wait(barrier, group_size - 1)
    for slot in range(3):
        issue(slot)
    for q in range(QUARTERS):
        sib_copy(0, q).start()
    sib_route(0).start()

    @pl.loop(0, mt_count)
    def _(m):
        rows = pl.ds(pl.multiple_of(m * tile, tile), tile)
        for e in range(e_local):
            acc_gu[e, rows] = jnp.zeros((tile, 2 * ffn), F32)

    @pl.loop(0, ft_count)
    def _(m):
        rows = pl.ds(pl.multiple_of(m * tile, tile), tile)
        for e in range(e_local):
            acc_d[e, rows] = jnp.zeros((tile, model), F32)

    for c in w_copies[:2]:
        c.wait()

    @pl.loop(0, units * e_local)
    def _(u):
        g, e = u // e_local, lax.rem(u, e_local)
        for c in unit_x(g, e):
            c.wait()

        @pl.when(u >= e_local)
        def _():
            for c in spill_copies(u - e_local, e):
                c.wait()

        @pl.loop(0, ft_count)
        def _(n):
            lo = pl.ds(pl.multiple_of(n * tile, tile), tile)
            hi = pl.ds(pl.multiple_of(ffn + n * tile, tile), tile)
            x = xb[e]
            a = jnp.dot(x, wgu[e, :, lo], preferred_element_type=F32)
            b = jnp.dot(x, wgu[e, :, hi], preferred_element_type=F32)
            sg = jax.nn.sigmoid(a)
            silu = a * sg
            hb[e, :, lo] = (silu * b).astype(BF16)
            pq[e, :, lo] = b * sg * (1.0 + a * (1.0 - sg))
            pq[e, :, hi] = silu

        for c in spill_copies(u, e):
            c.start()

        @pl.when(g + 1 < units)
        def _():
            for c in unit_x(g + 1, e):
                c.start()

        for k, at in ((0, 2), (1, 4), (2, 6)):
            @pl.when(u == at)
            def _(k=k):
                service(k)

    for e in range(e_local):
        for c in spill_copies((units - 1) * e_local + e, e):
            c.wait()
    for e in range(e_local):
        for c in unit_fill(0, e):
            c.start()
    w_copies[2].wait()

    def hits(r, p, e):
        local = rt[r, p, 0:8] - (me * (e_local * cap) + e * cap).astype(F32)
        hit = (local >= 0.0) & (local < float(cap))
        slot = jnp.max(jnp.where(hit, local, -1.0), axis=0, keepdims=True)
        gate = jnp.sum(jnp.where(hit, rt[r, p, 8:16], 0.0), axis=0, keepdims=True)
        return slot, gate

    def on(table, t):
        for step, slots in table.items():
            @pl.when(t == step)
            def _(slots=slots):
                for k in slots:
                    service(k)

    slot_iota = lax.broadcasted_iota(jnp.int32, (cap, tok), 0).astype(F32)

    @pl.loop(0, steps)
    def _(t):
        on(BEFORE, t)
        odd = lax.rem(t, 2)
        half = pl.multiple_of(odd * rows_s, rows_s)
        here = pl.ds(half, rows_s)
        dy_here = pl.ds(pl.multiple_of(rows_s + half, rows_s), rows_s)

        @pl.loop(0, STEP_BLOCKS)
        def _(i):
            p = t * STEP_BLOCKS + i
            for q in range(QUARTERS):
                sib_copy(p, q).wait_recv()
            sib_route(p).wait_recv()
            for r in range(2):
                picks, gates = [], []
                for e in range(e_local):
                    slot, gate = hits(r, p, e)
                    pick = slot_iota == slot
                    gates.append(jnp.sum(jnp.where(pick, gate, 0.0), axis=1, keepdims=True))
                    picks.append(jnp.where(pick, 1.0, 0.0).astype(BF16))
                pick = jnp.concatenate(picks, axis=0)
                row = pl.multiple_of((2 * i + r) * cap, cap)
                for n in range(model // 512):
                    cols = pl.ds(n * 512, 512)
                    d = jnp.dot(pick, ag[r, p, :, cols], preferred_element_type=F32)
                    for e in range(e_local):
                        d_e = d[e * cap:(e + 1) * cap]
                        db[e, pl.ds(row, cap), cols] = d_e.astype(BF16)
                        db[e, pl.ds(pl.multiple_of(rows_s + half + row, cap), cap), cols] = (d_e * gates[e]).astype(BF16)

        @pl.loop(0, e_local)
        def _(e):
            @pl.when(odd == 0)
            def _():
                for c in unit_fill(t // 2, e):
                    c.wait()

            @pl.when(t > 0)
            def _():
                for j in range(per_step):
                    dadb_copy(t, e, j).wait()

            part = jnp.zeros((rows_s, 128), F32)
            for n in range(ft_count):
                lo, hi = pl.ds(n * tile, tile), pl.ds(ffn + n * tile, tile)
                lhs = jnp.concatenate([db[e, 0:rows_s], db[e, dy_here]], axis=0)
                both = lax.dot_general(lhs, wd[e, lo, :], NT, preferred_element_type=F32)
                prod = hb[e, here, lo].astype(F32) * both[:rows_s]
                part += prod[:, :128] + prod[:, 128:]
                dh = both[rows_s:].astype(BF16).astype(F32)
                dadb[e, here, lo] = (dh * pq[e, here, lo]).astype(BF16)
                dadb[e, here, hi] = (dh * pq[e, here, hi]).astype(BF16)

            total = jnp.broadcast_to(jnp.sum(part, axis=1, keepdims=True), part.shape)
            for j in range(per_step):
                slot, _ = hits(j % 2, t * STEP_BLOCKS + j // 2, e)
                value = jnp.concatenate([total[j * cap:(j + 1) * cap]] * (tok // 128), axis=1)
                gsend[t * per_step + j, e] = jnp.sum(
                    jnp.where(slot_iota == slot, value, 0.0), axis=0, keepdims=True)

            for j in range(per_step):
                dadb_copy(t, e, j).start()

            def weight_grads(rows, dy_rows):
                @pl.loop(0, 2)
                def _(m):
                    out = pl.ds(pl.multiple_of(m * (model // 2), model // 2), model // 2)
                    for n in range(2):
                        cols = pl.ds(n * ffn, ffn)
                        acc_gu[e, out, cols] += lax.dot_general(
                            xb[e, rows, out], dadb[e, rows, cols], TN, preferred_element_type=F32)

                for n in range(model // 512):
                    cols = pl.ds(n * 512, 512)
                    acc_d[e, :, cols] += lax.dot_general(
                        hb[e, rows, :], db[e, dy_rows, cols], TN, preferred_element_type=F32)

            @pl.when((odd == 1) & (t < steps - 2))
            def _():
                weight_grads(pl.ds(0, rows_u), pl.ds(rows_s, rows_u))
                for c in unit_fill(t // 2 + 1, e):
                    c.start()

            @pl.when(t >= steps - 2)
            def _():
                weight_grads(here, dy_here)

            for step, slots in BETWEEN.items():
                @pl.when((t == step) & (e == 0))
                def _(slots=slots):
                    for k in slots:
                        service(k)

        on(AFTER, t)

        @pl.when(t == 0)
        def _():
            grecv[me] = gsend[0]

        @pl.loop(jnp.where(t == 0, 1, 0), per_step)
        def _(j):
            to = origin(t * STEP_BLOCKS + j // 2, lax.rem(j, 2))
            pltpu.make_async_remote_copy(
                src_ref=gsend.at[t * per_step + j], dst_ref=grecv.at[me], send_sem=gsend_sem,
                recv_sem=grecv_sem, device_id={'ep': to}, device_id_type=MESH).start()

    def drain(ref, sem):
        pltpu.make_async_copy(ref, ref, sem).wait()

    drain(ag.at[0, pl.ds(0, n_blocks - 1)], send_sem)
    drain(rt.at[0, pl.ds(0, n_blocks - 1)], rsend_sem)
    drain(ag.at[0], ssend_sem)
    drain(rt.at[0], srsend_sem)
    drain(gsend.at[pl.ds(0, group_size - 1)], gsend_sem)
    drain(grecv.at[pl.ds(0, group_size - 1)], grecv_sem)
    back = pltpu.make_async_copy(grecv, back_hbm, own_sem)
    back.start()
    for e in range(e_local):
        for j in range(per_step):
            dadb_copy(jnp.int32(steps - 1), e, j).wait()
    back.wait()


def run_experts(x_disp, w_gate, w_up, w_down, d_out, slots, ids, gates, group_size):
    sources, e_local, cap, model = x_disp.shape
    ffn = w_gate.shape[2]
    tok = d_out.shape[0]
    n_blocks = group_size // 2
    per_unit = 2 * UNIT_BLOCKS
    rows_u = per_unit * cap
    per_step = 2 * STEP_BLOCKS
    rows_s = per_step * cap
    units = n_blocks // UNIT_BLOCKS * e_local
    dma = pltpu.SemaphoreType.DMA
    any_spec = pl.BlockSpec(memory_space=pl.ANY)
    vmem_spec = pl.BlockSpec(memory_space=pltpu.VMEM)
    out_shape = [
        jax.ShapeDtypeStruct((sources, e_local, cap, 2 * ffn), BF16),
        pltpu.VMEM((e_local, model, 2 * ffn), F32),
        pltpu.VMEM((e_local, ffn, model), F32),
        jax.ShapeDtypeStruct((group_size, e_local, 1, tok), F32),
        jax.ShapeDtypeStruct((units, rows_u, 2 * ffn), F32),
        jax.ShapeDtypeStruct((units, rows_u, ffn), BF16),
    ]
    scratch = [
        pltpu.VMEM((2, n_blocks, tok, model), BF16),
        pltpu.VMEM((2, n_blocks, 16, tok), F32),
        pltpu.VMEM((e_local, model, 2 * ffn), BF16),
        pltpu.VMEM((e_local, ffn, model), BF16),
        pltpu.VMEM((e_local, rows_u, model), BF16),
        pltpu.VMEM((e_local, rows_s + rows_u, model), BF16),
        pltpu.VMEM((e_local, rows_u, 2 * ffn), F32),
        pltpu.VMEM((e_local, rows_u, ffn), BF16),
        pltpu.VMEM((group_size, e_local, 1, tok), F32),
        pltpu.VMEM((group_size, e_local, 1, tok), F32),
        dma((3,)), dma, dma((e_local, per_unit)), dma((e_local, 2)), dma((e_local, 2)),
        dma((e_local, per_step)),
        dma((n_blocks, QUARTERS)), dma((n_blocks,)), dma, dma,
        dma((n_blocks, QUARTERS)), dma((n_blocks,)), dma, dma, dma, dma,
    ]
    return pl.pallas_call(
        functools.partial(expert_kernel, group_size),
        out_shape=out_shape, in_specs=[any_spec] * 5 + [vmem_spec] * 3,
        out_specs=[any_spec, vmem_spec, vmem_spec, any_spec, any_spec, any_spec], scratch_shapes=scratch,
        compiler_params=pltpu.CompilerParams(collective_id=0, has_side_effects=True, vmem_limit_bytes=VMEM_A),
    )(x_disp, w_gate, w_up, w_down, d_out, slots, ids, gates)


def finish_kernel(group_size, chunk, dadb, wg, wu, back_hbm, acc_gu, acc_d, ids, slots,
                  gx, g_gate, g_up, g_down, gate_out,
                  wbuf, dbuf, obuf, st_g, st_u, st_d, back, w_sem, d_sem, o_sem, s_sem, b_sem):
    sources, e_local, cap, width = dadb.shape
    ffn = width // 2
    model = gx.shape[3]
    per_e = sources // chunk
    chunks = e_local * per_e
    m_blk, f_blk = model // per_e, ffn // per_e
    depth = dbuf.shape[0]

    def load(c):
        slot = lax.rem(c, depth)
        return pltpu.make_async_copy(
            dadb.at[pl.ds(lax.rem(c, per_e) * chunk, chunk), c // per_e], dbuf.at[slot], d_sem.at[slot])

    def store(c):
        slot = lax.rem(c, 2)
        return pltpu.make_async_copy(
            obuf.at[slot], gx.at[pl.ds(lax.rem(c, per_e) * chunk, chunk), c // per_e], o_sem.at[slot])

    def weights(e):
        return [pltpu.make_async_copy(wg.at[e], wbuf.at[e, :, pl.ds(0, ffn)], w_sem.at[e, 0]),
                pltpu.make_async_copy(wu.at[e], wbuf.at[e, :, pl.ds(ffn, ffn)], w_sem.at[e, 1])]

    def staged(c):
        e, i = c // per_e, lax.rem(c, per_e)
        m = pl.ds(pl.multiple_of(i * m_blk, m_blk), m_blk)
        f = pl.ds(pl.multiple_of(i * f_blk, f_blk), f_blk)
        return e, m, f, [pltpu.make_async_copy(st_g.at[e, m], g_gate.at[e, m], s_sem.at[c, 0]),
                         pltpu.make_async_copy(st_u.at[e, m], g_up.at[e, m], s_sem.at[c, 1]),
                         pltpu.make_async_copy(st_d.at[e, f], g_down.at[e, f], s_sem.at[c, 2])]

    for c in weights(0):
        c.start()
    for k in range(depth):
        load(jnp.int32(k)).start()
    for e in range(1, e_local):
        for c in weights(e):
            c.start()

    back_copy = pltpu.make_async_copy(back_hbm, back, b_sem)
    back_copy.start()

    @pl.loop(0, chunks)
    def _(c):
        e, m, f, copies = staged(c)

        @pl.when(lax.rem(c, per_e) == 0)
        def _():
            for w in weights(e):
                w.wait()

        load(c).wait()

        @pl.when(c >= 2)
        def _():
            store(c - 2).wait()

        slot, out_slot = lax.rem(c, depth), lax.rem(c, 2)
        st_g[e, m] = acc_gu[e, m, 0:ffn].astype(BF16)
        st_u[e, m] = acc_gu[e, m, ffn:width].astype(BF16)
        st_d[e, f] = acc_d[e, f].astype(BF16)
        both = dbuf[slot].reshape(chunk * cap, width)
        for n in range(model // 512):
            rows = pl.ds(n * 512, 512)
            out = lax.dot_general(both, wbuf[e, rows], NT, preferred_element_type=F32)
            obuf[out_slot, :, :, rows] = out.astype(BF16).reshape(chunk, cap, 512)
        store(c).start()
        for s in copies:
            s.start()

        @pl.when(c + depth < chunks)
        def _():
            load(c + depth).start()

    back_copy.wait()
    total = jnp.zeros(gate_out.shape, F32)
    for d in range(group_size):
        for e in range(e_local):
            total += jnp.where(ids[...] == d * e_local + e, back[d, e], 0.0)
    gate_out[...] = jnp.where(slots[...] >= 0, total, 0.0)

    for c in range(chunks - 2, chunks):
        store(jnp.int32(c)).wait()
    for c in range(chunks):
        for s in staged(jnp.int32(c))[3]:
            s.wait()


def run_finish(dadb, w_gate, w_up, acc_gu, acc_d, back, ids, slots, group_size):
    sources, e_local, cap, width = dadb.shape
    model, ffn = w_gate.shape[1:]
    top_k, tok = ids.shape
    chunk = 8
    dma = pltpu.SemaphoreType.DMA
    any_spec = pl.BlockSpec(memory_space=pl.ANY)
    vmem_spec = pl.BlockSpec(memory_space=pltpu.VMEM)
    return pl.pallas_call(
        functools.partial(finish_kernel, group_size, chunk),
        in_specs=[any_spec] * 4 + [vmem_spec] * 4,
        out_specs=[any_spec] * 4 + [vmem_spec],
        out_shape=[
            jax.ShapeDtypeStruct((sources, e_local, cap, model), BF16),
            jax.ShapeDtypeStruct((e_local, model, ffn), BF16),
            jax.ShapeDtypeStruct((e_local, model, ffn), BF16),
            jax.ShapeDtypeStruct((e_local, ffn, model), BF16),
            jax.ShapeDtypeStruct((top_k, tok), F32),
        ],
        scratch_shapes=[
            pltpu.VMEM((e_local, model, width), BF16),
            pltpu.VMEM((3, chunk, cap, width), BF16),
            pltpu.VMEM((2, chunk, cap, model), BF16),
            pltpu.VMEM((e_local, model, ffn), BF16),
            pltpu.VMEM((e_local, model, ffn), BF16),
            pltpu.VMEM((e_local, ffn, model), BF16),
            pltpu.VMEM(back.shape, F32),
            dma((e_local, 2)), dma((3,)), dma((2,)), dma((e_local * sources // chunk, 3)), dma,
        ],
        compiler_params=pltpu.CompilerParams(vmem_limit_bytes=VMEM_B),
    )(*[pltpu.with_memory_space_constraint(a, pltpu.HBM) for a in (dadb, w_gate, w_up, back)],
      *[pltpu.with_memory_space_constraint(a, pltpu.VMEM) for a in (acc_gu, acc_d)], ids, slots)


def solution(mesh):
    group_size = mesh.shape['ep']

    def local_step(x_disp, w_gate, w_up, w_down, d_out, slot_idx, expert_id, gate_wt):
        slots, ids = slot_idx.T, expert_id.T
        dadb, acc_gu, acc_d, back, _, _ = run_experts(
            x_disp, w_gate, w_up, w_down, d_out, slots, ids, gate_wt.T, group_size)
        grad_x, grad_w_gate, grad_w_up, grad_w_down, gate = run_finish(
            dadb, w_gate, w_up, acc_gu, acc_d, back, ids, slots, group_size)
        return grad_x, grad_w_gate, grad_w_up, grad_w_down, gate.T

    token_place = P(('dp', 'ep'), None)
    weight_place = P('ep', None, None)
    slot_place = P('dp', 'ep', None, None)
    grad_place = P(('dp', 'ep'), None, None)
    return jax.shard_map(local_step, mesh=mesh,
                         in_specs=(slot_place, weight_place, weight_place, weight_place, token_place, token_place, token_place, token_place),
                         out_specs=(slot_place, grad_place, grad_place, grad_place, token_place),
                         check_vma=False)
```

```python
import functools
import math

import jax
import jax.numpy as jnp
from jax import lax
from jax.experimental import pallas as pl
from jax.experimental.pallas import tpu as pltpu
from jax.sharding import PartitionSpec as P

F32 = jnp.float32
BF16 = jnp.bfloat16
MESH = pl.DeviceIdType.MESH

ORDER = [(0, 0), (0, 1), (0, 3), (1, 0), (3, 0), (0, 2), (2, 0), (1, 1),
         (1, 2), (3, 1), (1, 3), (3, 3), (3, 2), (2, 1), (2, 3), (2, 2)]
PLACE = {block: place for place, block in enumerate(ORDER)}


def packed(values):
    total = sum(v << (2 * k) for k, v in enumerate(values))
    return total - 2 ** 32 if total >= 2 ** 31 else total


ORIGIN_Y, ORIGIN_X = packed([b[0] for b in ORDER]), packed([b[1] for b in ORDER])
QUARTERS = 4
VMEM_A = 45 * 1024 * 1024 + 832 * 1024
VMEM_B = 22 * 1024 * 1024
UNIT_BLOCKS = 4
STEP_BLOCKS = 2
BEFORE = {0: (3,), 3: (7,), 4: (8, 9, 10), 6: (13,)}
BETWEEN = {0: (4,), 1: (5,), 2: (6,), 4: (11,), 5: (12,)}
AFTER = {6: (14,)}
NT = (((1,), (1,)), ((), ()))
TN = (((0,), (0,)), ((), ()))


def send_lists():
    own = [(0, 0, 0), (0, 0, 1), (0, 0, 2), (0, 0, 3), (0, 1, 0), (0, 1, 2)]
    plus_x = own + [(1, 0, 2), (1, 0, 3), (3, 0, 2), (1, 1, 2), (3, 0, 3), (2, 0, 2),
                    (3, 1, 2), (2, 0, 3), (2, 1, 2)]
    swap = (2, 3, 0, 1)
    flip = (1, 0, 3, 2)
    plus_y = [(ox, oy, swap[q]) for oy, ox, q in own]
    plus_y += [(0, 1, 0), (0, 1, 1), (0, 2, 0), (0, 2, 1), (0, 3, 0), (0, 3, 1),
               (1, 1, 0), (1, 3, 0), (1, 2, 0)]
    minus_x = [(oy, -ox % 4, flip[q]) for oy, ox, q in plus_x]
    minus_y = [(-oy % 4, ox, flip[q]) for oy, ox, q in plus_y]
    return {(0, 1): plus_x, (0, 3): minus_x, (1, 0): plus_y, (3, 0): minus_y}


SENDS = send_lists()
SLOTS = len(SENDS[(0, 1)])


def expert_kernel(group_size, x_hbm, wg_hbm, wu_hbm, wd_hbm, dout_hbm, slots_ref, ids_ref, gates_ref,
                  dadb_hbm, acc_gu, acc_d, grecv, pq_hbm, h_hbm,
                  ag, rt, wgu, wd, xb, db, pq, hb, gsend,
                  w_sem, own_sem, x_sem, spill_sem, fill_sem, dadb_sem,
                  recv_sem, rrecv_sem, send_sem, rsend_sem,
                  srecv_sem, srrecv_sem, ssend_sem, srsend_sem, gsend_sem, grecv_sem):
    side = math.isqrt(group_size // 2)
    me = lax.axis_index('ep')
    core = lax.rem(me, 2)
    my_x = lax.rem(me // 2, side)
    my_y = me // (2 * side)
    e_local, rows_u, model = xb.shape
    rows_s = rows_u // (UNIT_BLOCKS // STEP_BLOCKS)
    ffn = hb.shape[2]
    cap = x_hbm.shape[2]
    tok = ag.shape[2]
    qrows = tok // QUARTERS
    n_blocks = side * side
    units = n_blocks // UNIT_BLOCKS
    steps = n_blocks // STEP_BLOCKS
    per_unit = 2 * UNIT_BLOCKS
    per_step = 2 * STEP_BLOCKS
    tile = 256
    mt_count = model // tile
    dadb = wgu
    ft_count = ffn // tile

    def device(y, x, c):
        return (y * side + x) * 2 + c

    def neighbour(dy, dx):
        return device(lax.rem(my_y + dy, side), lax.rem(my_x + dx, side), core)

    sibling = device(my_y, my_x, 1 - core)

    def origin(p, r):
        oy = lax.shift_right_logical(jnp.int32(ORIGIN_Y), 2 * p) & 3
        ox = lax.shift_right_logical(jnp.int32(ORIGIN_X), 2 * p) & 3
        c = core + r - 2 * core * r
        return device(lax.rem(my_y + side - oy, side), lax.rem(my_x + side - ox, side), c)

    def quarter(r, p, q):
        return ag.at[r, p, pl.ds(q * qrows, qrows)]

    def ici_copy(p_from, p_to, q, to):
        return pltpu.make_async_remote_copy(
            src_ref=quarter(0, p_from, q), dst_ref=quarter(0, p_to, q), send_sem=send_sem,
            recv_sem=recv_sem.at[p_to, q], device_id={'ep': to}, device_id_type=MESH)

    def ici_route(p_from, p_to, to):
        return pltpu.make_async_remote_copy(
            src_ref=rt.at[0, p_from], dst_ref=rt.at[0, p_to], send_sem=rsend_sem,
            recv_sem=rrecv_sem.at[p_to], device_id={'ep': to}, device_id_type=MESH)

    def sib_copy(p, q):
        return pltpu.make_async_remote_copy(
            src_ref=quarter(0, p, q), dst_ref=quarter(1, p, q), send_sem=ssend_sem,
            recv_sem=srecv_sem.at[p, q], device_id={'ep': sibling}, device_id_type=MESH)

    def sib_route(p):
        return pltpu.make_async_remote_copy(
            src_ref=rt.at[0, p], dst_ref=rt.at[1, p], send_sem=srsend_sem,
            recv_sem=srrecv_sem.at[p], device_id={'ep': sibling}, device_id_type=MESH)

    def issue(slot):
        for (dy, dx), sends in SENDS.items():
            oy, ox, q = sends[slot]
            p_from, p_to = PLACE[(oy, ox)], PLACE[((oy + dy) % 4, (ox + dx) % 4)]
            to = neighbour(dy, dx)
            ici_copy(p_from, p_to, q, to).start()
            if q == 0:
                ici_route(p_from, p_to, to).start()

    def service(slot):
        for (dy, dx), sends in SENDS.items():
            oy, ox, q = sends[slot]
            p_to = PLACE[((oy + dy) % 4, (ox + dx) % 4)]
            ici_copy(p_to, p_to, q, me).wait_recv()
            if q == 0:
                ici_route(p_to, p_to, me).wait_recv()
        if slot + 3 < SLOTS:
            issue(slot + 3)
        for (dy, dx), sends in SENDS.items():
            oy, ox, q = sends[slot]
            p_to = PLACE[((oy + dy) % 4, (ox + dx) % 4)]
            sib_copy(p_to, q).start()
            if q == 0:
                sib_route(p_to).start()

    def x_copy(block, j, e, row, sem):
        src = origin(block + j // 2, j % 2)
        return pltpu.make_async_copy(x_hbm.at[src, e], xb.at[e, pl.ds(row + j * cap, cap)], x_sem.at[e, sem + j])

    def unit_x(g, e):
        return [x_copy(g * UNIT_BLOCKS, j, e, 0, 0) for j in range(per_unit)]

    def unit_fill(g, e):
        u = g * e_local + e
        return unit_x(g, e) + [pltpu.make_async_copy(pq_hbm.at[u], pq.at[e], fill_sem.at[e, 0]),
                               pltpu.make_async_copy(h_hbm.at[u], hb.at[e], fill_sem.at[e, 1])]

    def dadb_copy(t, e, j):
        src = origin(t * STEP_BLOCKS + j // 2, j % 2)
        row = pl.multiple_of(lax.rem(t, 2) * rows_s + j * cap, cap)
        return pltpu.make_async_copy(dadb.at[e, pl.ds(row, cap)], dadb_hbm.at[src, e], dadb_sem.at[e, j])

    def spill_copies(u, e):
        return (pltpu.make_async_copy(pq.at[e], pq_hbm.at[u], spill_sem.at[e, 0]),
                pltpu.make_async_copy(hb.at[e], h_hbm.at[u], spill_sem.at[e, 1]))

    w_copies = [pltpu.make_async_copy(wg_hbm, wgu.at[:, :, pl.ds(0, ffn)], w_sem.at[0]),
                pltpu.make_async_copy(wu_hbm, wgu.at[:, :, pl.ds(ffn, ffn)], w_sem.at[1]),
                pltpu.make_async_copy(wd_hbm, wd, w_sem.at[2])]
    own = pltpu.make_async_copy(dout_hbm, ag.at[0, 0], own_sem)

    own.start()
    barrier = pltpu.get_barrier_semaphore()

    partners = [neighbour(dy, dx) for dy, dx in SENDS] + [sibling]
    for to in partners:
        pl.semaphore_signal(barrier, inc=1, device_id={'ep': to}, device_id_type=MESH)

    for c in w_copies[:2]:
        c.start()
    for e in range(e_local):
        for c in unit_x(0, e):
            c.start()
    w_copies[2].start()
    top_k = slots_ref.shape[0]
    rt[0, 0] = jnp.concatenate([jnp.full((8, tok), -1.0, F32), jnp.zeros((8, tok), F32)], axis=0)
    slots = slots_ref[...]
    rt[0, 0, 0:top_k] = jnp.where(slots >= 0, ids_ref[...] * cap + slots, -1).astype(F32)
    rt[0, 0, 8:8 + top_k] = gates_ref[...]
    own.wait()
    pl.semaphore_wait(barrier, len(partners))
    for slot in range(3):
        issue(slot)
    for q in range(QUARTERS):
        sib_copy(0, q).start()
    sib_route(0).start()

    @pl.loop(0, mt_count)
    def _(m):
        rows = pl.ds(pl.multiple_of(m * tile, tile), tile)
        for e in range(e_local):
            acc_gu[e, rows] = jnp.zeros((tile, 2 * ffn), F32)

    @pl.loop(0, ft_count)
    def _(m):
        rows = pl.ds(pl.multiple_of(m * tile, tile), tile)
        for e in range(e_local):
            acc_d[e, rows] = jnp.zeros((tile, model), F32)

    for c in w_copies[:2]:
        c.wait()

    @pl.loop(0, units * e_local)
    def _(u):
        g, e = u // e_local, lax.rem(u, e_local)
        for c in unit_x(g, e):
            c.wait()

        @pl.when(u >= e_local)
        def _():
            for c in spill_copies(u - e_local, e):
                c.wait()

        @pl.loop(0, ft_count)
        def _(n):
            lo = pl.ds(pl.multiple_of(n * tile, tile), tile)
            hi = pl.ds(pl.multiple_of(ffn + n * tile, tile), tile)
            x = xb[e]
            a = jnp.dot(x, wgu[e, :, lo], preferred_element_type=F32)
            b = jnp.dot(x, wgu[e, :, hi], preferred_element_type=F32)
            sg = jax.nn.sigmoid(a)
            silu = a * sg
            hb[e, :, lo] = (silu * b).astype(BF16)
            pq[e, :, lo] = b * sg * (1.0 + a * (1.0 - sg))
            pq[e, :, hi] = silu

        for c in spill_copies(u, e):
            c.start()

        @pl.when(g + 1 < units)
        def _():
            for c in unit_x(g + 1, e):
                c.start()

        for k, at in ((0, 2), (1, 4), (2, 6)):
            @pl.when(u == at)
            def _(k=k):
                service(k)

    for e in range(e_local):
        for c in spill_copies((units - 1) * e_local + e, e):
            c.wait()
    for e in range(e_local):
        for c in unit_fill(0, e):
            c.start()
    w_copies[2].wait()

    def hits(r, p, e):
        local = rt[r, p, 0:8] - (me * (e_local * cap) + e * cap).astype(F32)
        hit = (local >= 0.0) & (local < float(cap))
        slot = jnp.max(jnp.where(hit, local, -1.0), axis=0, keepdims=True)
        gate = jnp.sum(jnp.where(hit, rt[r, p, 8:16], 0.0), axis=0, keepdims=True)
        return slot, gate

    def on(table, t):
        for step, slots in table.items():
            @pl.when(t == step)
            def _(slots=slots):
                for k in slots:
                    service(k)

    slot_iota = lax.broadcasted_iota(jnp.int32, (cap, tok), 0).astype(F32)

    @pl.loop(0, steps)
    def _(t):
        on(BEFORE, t)
        odd = lax.rem(t, 2)
        half = pl.multiple_of(odd * rows_s, rows_s)
        here = pl.ds(half, rows_s)
        dy_here = pl.ds(pl.multiple_of(rows_s + half, rows_s), rows_s)

        @pl.loop(0, STEP_BLOCKS)
        def _(i):
            p = t * STEP_BLOCKS + i
            for q in range(QUARTERS):
                sib_copy(p, q).wait_recv()
            sib_route(p).wait_recv()
            for r in range(2):
                picks, gates = [], []
                for e in range(e_local):
                    slot, gate = hits(r, p, e)
                    pick = slot_iota == slot
                    gates.append(jnp.sum(jnp.where(pick, gate, 0.0), axis=1, keepdims=True))
                    picks.append(jnp.where(pick, 1.0, 0.0).astype(BF16))
                pick = jnp.concatenate(picks, axis=0)
                row = pl.multiple_of((2 * i + r) * cap, cap)
                for n in range(model // 512):
                    cols = pl.ds(n * 512, 512)
                    d = jnp.dot(pick, ag[r, p, :, cols], preferred_element_type=F32)
                    for e in range(e_local):
                        d_e = d[e * cap:(e + 1) * cap]
                        db[e, pl.ds(row, cap), cols] = d_e.astype(BF16)
                        db[e, pl.ds(pl.multiple_of(rows_s + half + row, cap), cap), cols] = (d_e * gates[e]).astype(BF16)

        @pl.loop(0, e_local)
        def _(e):
            @pl.when(odd == 0)
            def _():
                for c in unit_fill(t // 2, e):
                    c.wait()

            @pl.when(t > 0)
            def _():
                for j in range(per_step):
                    dadb_copy(t, e, j).wait()

            part = jnp.zeros((rows_s, 128), F32)
            for n in range(ft_count):
                lo, hi = pl.ds(n * tile, tile), pl.ds(ffn + n * tile, tile)
                lhs = jnp.concatenate([db[e, 0:rows_s], db[e, dy_here]], axis=0)
                both = lax.dot_general(lhs, wd[e, lo, :], NT, preferred_element_type=F32)
                prod = hb[e, here, lo].astype(F32) * both[:rows_s]
                part += prod[:, :128] + prod[:, 128:]
                dh = both[rows_s:].astype(BF16).astype(F32)
                dadb[e, here, lo] = (dh * pq[e, here, lo]).astype(BF16)
                dadb[e, here, hi] = (dh * pq[e, here, hi]).astype(BF16)

            total = jnp.broadcast_to(jnp.sum(part, axis=1, keepdims=True), part.shape)
            for j in range(per_step):
                slot, _ = hits(j % 2, t * STEP_BLOCKS + j // 2, e)
                value = jnp.concatenate([total[j * cap:(j + 1) * cap]] * (tok // 128), axis=1)
                gsend[t * per_step + j, e] = jnp.sum(
                    jnp.where(slot_iota == slot, value, 0.0), axis=0, keepdims=True)

            for j in range(per_step):
                dadb_copy(t, e, j).start()

            @pl.when((t == 0) & (e == e_local - 1))
            def _():
                grecv[me] = gsend[0]

            @pl.when(e == e_local - 1)
            def _():
                @pl.loop(jnp.where(t == 0, 1, 0), per_step)
                def _(j):
                    to = origin(t * STEP_BLOCKS + j // 2, lax.rem(j, 2))
                    pltpu.make_async_remote_copy(
                        src_ref=gsend.at[t * per_step + j], dst_ref=grecv.at[me], send_sem=gsend_sem,
                        recv_sem=grecv_sem, device_id={'ep': to}, device_id_type=MESH).start()

            def weight_grads(rows, dy_rows):
                @pl.loop(0, 2)
                def _(m):
                    out = pl.ds(pl.multiple_of(m * (model // 2), model // 2), model // 2)
                    for n in range(2):
                        cols = pl.ds(n * ffn, ffn)
                        acc_gu[e, out, cols] += lax.dot_general(
                            xb[e, rows, out], dadb[e, rows, cols], TN, preferred_element_type=F32)

                for n in range(model // 512):
                    cols = pl.ds(n * 512, 512)
                    acc_d[e, :, cols] += lax.dot_general(
                        hb[e, rows, :], db[e, dy_rows, cols], TN, preferred_element_type=F32)

            @pl.when((odd == 1) & (t < steps - 2))
            def _():
                weight_grads(pl.ds(0, rows_u), pl.ds(rows_s, rows_u))
                for c in unit_fill(t // 2 + 1, e):
                    c.start()

            @pl.when(t >= steps - 2)
            def _():
                weight_grads(here, dy_here)

            for step, slots in BETWEEN.items():
                @pl.when((t == step) & (e == 0))
                def _(slots=slots):
                    for k in slots:
                        service(k)

        on(AFTER, t)

    def drain(ref, sem):
        pltpu.make_async_copy(ref, ref, sem).wait()

    drain(ag.at[0, pl.ds(0, n_blocks - 1)], send_sem)
    drain(rt.at[0, pl.ds(0, n_blocks - 1)], rsend_sem)
    drain(ag.at[0], ssend_sem)
    drain(rt.at[0], srsend_sem)
    drain(gsend.at[pl.ds(0, group_size - 1)], gsend_sem)
    drain(grecv.at[pl.ds(0, group_size - 1)], grecv_sem)
    for e in range(e_local):
        for j in range(per_step):
            dadb_copy(jnp.int32(steps - 1), e, j).wait()


def run_experts(x_disp, w_gate, w_up, w_down, d_out, slots, ids, gates, group_size):
    sources, e_local, cap, model = x_disp.shape
    ffn = w_gate.shape[2]
    tok = d_out.shape[0]
    n_blocks = group_size // 2
    per_unit = 2 * UNIT_BLOCKS
    rows_u = per_unit * cap
    per_step = 2 * STEP_BLOCKS
    rows_s = per_step * cap
    units = n_blocks // UNIT_BLOCKS * e_local
    dma = pltpu.SemaphoreType.DMA
    any_spec = pl.BlockSpec(memory_space=pl.ANY)
    vmem_spec = pl.BlockSpec(memory_space=pltpu.VMEM)
    out_shape = [
        jax.ShapeDtypeStruct((sources, e_local, cap, 2 * ffn), BF16),
        pltpu.VMEM((e_local, model, 2 * ffn), F32),
        pltpu.VMEM((e_local, ffn, model), F32),
        pltpu.VMEM((group_size, e_local, 1, tok), F32),
        jax.ShapeDtypeStruct((units, rows_u, 2 * ffn), F32),
        jax.ShapeDtypeStruct((units, rows_u, ffn), BF16),
    ]
    scratch = [
        pltpu.VMEM((2, n_blocks, tok, model), BF16),
        pltpu.VMEM((2, n_blocks, 16, tok), F32),
        pltpu.VMEM((e_local, model, 2 * ffn), BF16),
        pltpu.VMEM((e_local, ffn, model), BF16),
        pltpu.VMEM((e_local, rows_u, model), BF16),
        pltpu.VMEM((e_local, rows_s + rows_u, model), BF16),
        pltpu.VMEM((e_local, rows_u, 2 * ffn), F32),
        pltpu.VMEM((e_local, rows_u, ffn), BF16),
        pltpu.VMEM((group_size, e_local, 1, tok), F32),
        dma((3,)), dma, dma((e_local, per_unit)), dma((e_local, 2)), dma((e_local, 2)),
        dma((e_local, per_step)),
        dma((n_blocks, QUARTERS)), dma((n_blocks,)), dma, dma,
        dma((n_blocks, QUARTERS)), dma((n_blocks,)), dma, dma, dma, dma,
    ]
    return pl.pallas_call(
        functools.partial(expert_kernel, group_size),
        out_shape=out_shape, in_specs=[any_spec] * 5 + [vmem_spec] * 3,
        out_specs=[any_spec, vmem_spec, vmem_spec, vmem_spec, any_spec, any_spec], scratch_shapes=scratch,
        compiler_params=pltpu.CompilerParams(collective_id=0, has_side_effects=True, vmem_limit_bytes=VMEM_A),
    )(x_disp, w_gate, w_up, w_down, d_out, slots, ids, gates)


def finish_kernel(group_size, chunk, dadb, wg, wu, back, acc_gu, acc_d, ids, slots,
                  gx, g_gate, g_up, g_down, gate_out,
                  wbuf, dbuf, obuf, st_g, st_u, st_d, w_sem, d_sem, o_sem, s_sem):
    sources, e_local, cap, width = dadb.shape
    ffn = width // 2
    model = gx.shape[3]
    per_e = sources // chunk
    chunks = e_local * per_e
    m_blk, f_blk = model // per_e, ffn // per_e
    depth = dbuf.shape[0]

    def load(c):
        slot = lax.rem(c, depth)
        return pltpu.make_async_copy(
            dadb.at[pl.ds(lax.rem(c, per_e) * chunk, chunk), c // per_e], dbuf.at[slot], d_sem.at[slot])

    def store(c):
        slot = lax.rem(c, 2)
        return pltpu.make_async_copy(
            obuf.at[slot], gx.at[pl.ds(lax.rem(c, per_e) * chunk, chunk), c // per_e], o_sem.at[slot])

    def weights(e):
        return [pltpu.make_async_copy(wg.at[e], wbuf.at[e, :, pl.ds(0, ffn)], w_sem.at[e, 0]),
                pltpu.make_async_copy(wu.at[e], wbuf.at[e, :, pl.ds(ffn, ffn)], w_sem.at[e, 1])]

    def staged(c):
        e, i = c // per_e, lax.rem(c, per_e)
        m = pl.ds(pl.multiple_of(i * m_blk, m_blk), m_blk)
        f = pl.ds(pl.multiple_of(i * f_blk, f_blk), f_blk)
        return e, m, f, [pltpu.make_async_copy(st_g.at[e, m], g_gate.at[e, m], s_sem.at[c, 0]),
                         pltpu.make_async_copy(st_u.at[e, m], g_up.at[e, m], s_sem.at[c, 1]),
                         pltpu.make_async_copy(st_d.at[e, f], g_down.at[e, f], s_sem.at[c, 2])]

    for c in weights(0):
        c.start()
    for k in range(depth):
        load(jnp.int32(k)).start()
    for e in range(1, e_local):
        for c in weights(e):
            c.start()

    def cast(c):
        e, m, f, copies = staged(c)
        st_g[e, m] = acc_gu[e, m, 0:ffn].astype(BF16)
        st_u[e, m] = acc_gu[e, m, ffn:width].astype(BF16)
        st_d[e, f] = acc_d[e, f].astype(BF16)
        return copies

    @pl.loop(0, per_e)
    def _(c):
        for s in cast(c):
            s.start()

    for e in range(e_local):
        for w in weights(e):
            w.wait()

        @pl.loop(e * per_e, (e + 1) * per_e)
        def _(c, e=e):
            load(c).wait()

            @pl.when(c >= 2)
            def _():
                store(c - 2).wait()

            slot, out_slot = lax.rem(c, depth), lax.rem(c, 2)
            copies = cast(c + per_e) if e + 1 < e_local else []
            both = dbuf[slot].reshape(chunk * cap, width)
            for n in range(model // 512):
                rows = pl.ds(n * 512, 512)
                out = lax.dot_general(both, wbuf[e, rows], NT, preferred_element_type=F32)
                obuf[out_slot, :, :, rows] = out.astype(BF16).reshape(chunk, cap, 512)
            store(c).start()
            for s in copies:
                s.start()

            @pl.when(c + depth < chunks)
            def _():
                load(c + depth).start()

    total = jnp.zeros(gate_out.shape, F32)
    for d in range(group_size):
        for e in range(e_local):
            total += jnp.where(ids[...] == d * e_local + e, back[d, e], 0.0)
    gate_out[...] = jnp.where(slots[...] >= 0, total, 0.0)

    for c in range(chunks - 2, chunks):
        store(jnp.int32(c)).wait()
    for c in range(chunks):
        for s in staged(jnp.int32(c))[3]:
            s.wait()


def run_finish(dadb, w_gate, w_up, acc_gu, acc_d, back, ids, slots, group_size):
    sources, e_local, cap, width = dadb.shape
    model, ffn = w_gate.shape[1:]
    top_k, tok = ids.shape
    chunk = 8
    dma = pltpu.SemaphoreType.DMA
    any_spec = pl.BlockSpec(memory_space=pl.ANY)
    vmem_spec = pl.BlockSpec(memory_space=pltpu.VMEM)
    return pl.pallas_call(
        functools.partial(finish_kernel, group_size, chunk),
        in_specs=[any_spec] * 3 + [vmem_spec] * 5,
        out_specs=[any_spec] * 4 + [vmem_spec],
        out_shape=[
            jax.ShapeDtypeStruct((sources, e_local, cap, model), BF16),
            jax.ShapeDtypeStruct((e_local, model, ffn), BF16),
            jax.ShapeDtypeStruct((e_local, model, ffn), BF16),
            jax.ShapeDtypeStruct((e_local, ffn, model), BF16),
            jax.ShapeDtypeStruct((top_k, tok), F32),
        ],
        scratch_shapes=[
            pltpu.VMEM((e_local, model, width), BF16),
            pltpu.VMEM((3, chunk, cap, width), BF16),
            pltpu.VMEM((2, chunk, cap, model), BF16),
            pltpu.VMEM((e_local, model, ffn), BF16),
            pltpu.VMEM((e_local, model, ffn), BF16),
            pltpu.VMEM((e_local, ffn, model), BF16),
            dma((e_local, 2)), dma((3,)), dma((2,)), dma((e_local * sources // chunk, 3)),
        ],
        compiler_params=pltpu.CompilerParams(vmem_limit_bytes=VMEM_B),
    )(*[pltpu.with_memory_space_constraint(a, pltpu.HBM) for a in (dadb, w_gate, w_up)],
      *[pltpu.with_memory_space_constraint(a, pltpu.VMEM) for a in (back, acc_gu, acc_d)], ids, slots)


def solution(mesh):
    group_size = mesh.shape['ep']

    def local_step(x_disp, w_gate, w_up, w_down, d_out, slot_idx, expert_id, gate_wt):
        slots, ids = slot_idx.T, expert_id.T
        dadb, acc_gu, acc_d, back, _, _ = run_experts(
            x_disp, w_gate, w_up, w_down, d_out, slots, ids, gate_wt.T, group_size)
        grad_x, grad_w_gate, grad_w_up, grad_w_down, gate = run_finish(
            dadb, w_gate, w_up, acc_gu, acc_d, back, ids, slots, group_size)
        return grad_x, grad_w_gate, grad_w_up, grad_w_down, gate.T

    token_place = P(('dp', 'ep'), None)
    weight_place = P('ep', None, None)
    slot_place = P('dp', 'ep', None, None)
    grad_place = P(('dp', 'ep'), None, None)
    return jax.shard_map(local_step, mesh=mesh,
                         in_specs=(slot_place, weight_place, weight_place, weight_place, token_place, token_place, token_place, token_place),
                         out_specs=(slot_place, grad_place, grad_place, grad_place, token_place),
                         check_vma=False)
```

```python
import functools
import math

import jax
import jax.numpy as jnp
from jax import lax
from jax.experimental import pallas as pl
from jax.experimental.pallas import tpu as pltpu
from jax.sharding import PartitionSpec as P

F32 = jnp.float32
BF16 = jnp.bfloat16
MESH = pl.DeviceIdType.MESH

ORDER = [(0, 0), (0, 1), (0, 3), (1, 0), (3, 0), (0, 2), (2, 0), (1, 1),
         (1, 3), (3, 1), (3, 3), (1, 2), (2, 1), (2, 3), (3, 2), (2, 2)]
PLACE = {block: place for place, block in enumerate(ORDER)}


def packed(values):
    total = sum(v << (2 * k) for k, v in enumerate(values))
    return total - 2 ** 32 if total >= 2 ** 31 else total


ORIGIN_Y, ORIGIN_X = packed([b[0] for b in ORDER]), packed([b[1] for b in ORDER])
QUARTERS = 4
VMEM_A = 45 * 1024 * 1024 + 832 * 1024
VMEM_B = 22 * 1024 * 1024
UNIT_BLOCKS = 4
STEP_BLOCKS = 2
BEFORE = {0: (3,), 3: (7,), 4: (9,), 5: (11,), 6: (13,)}
BETWEEN = {0: (4,), 1: (5,), 2: (6,), 3: (8,)}
LATE = {4: (10,), 5: (12,), 6: (14,)}
NT = (((1,), (1,)), ((), ()))
TN = (((0,), (0,)), ((), ()))


def send_lists():
    flip = (1, 0, 3, 2)
    plus_x = [(0, 0, 1), (0, 0, 0), (0, 0, 2), (0, 0, 3), (0, 1, 0), (0, 1, 2), (1, 0, 3), (1, 0, 2),
              (3, 0, 2), (3, 0, 3), (2, 0, 2), (1, 1, 2), (2, 0, 3), (3, 1, 2), (2, 1, 2)]
    plus_y = [(0, 0, 0), (0, 0, 3), (0, 0, 2), (0, 0, 1), (1, 0, 0), (1, 0, 2), (0, 1, 1), (0, 1, 0),
              (0, 3, 1), (0, 3, 0), (0, 2, 0), (0, 2, 1), (1, 1, 0), (1, 3, 0), (1, 2, 0)]
    minus_x = [(oy, -ox % 4, flip[q]) for oy, ox, q in plus_x]
    minus_y = [(-oy % 4, ox, flip[q]) for oy, ox, q in plus_y]
    return {(0, 1): plus_x, (0, 3): minus_x, (1, 0): plus_y, (3, 0): minus_y}


SENDS = send_lists()
SLOTS = len(SENDS[(0, 1)])


def expert_kernel(group_size, x_hbm, wg_hbm, wu_hbm, wd_hbm, dout_hbm, slots_ref, ids_ref, gates_ref,
                  dadb_hbm, acc_gu, acc_d, grecv, pq_hbm, h_hbm,
                  ag, rt, wgu, wd, xb, db, pq, hb, gsend,
                  w_sem, own_sem, x_sem, spill_sem, fill_sem, dadb_sem,
                  recv_sem, rrecv_sem, send_sem, rsend_sem,
                  srecv_sem, srrecv_sem, ssend_sem, srsend_sem, gsend_sem, grecv_sem):
    side = math.isqrt(group_size // 2)
    me = lax.axis_index('ep')
    core = lax.rem(me, 2)
    my_x = lax.rem(me // 2, side)
    my_y = me // (2 * side)
    e_local, rows_u, model = xb.shape
    rows_s = rows_u // (UNIT_BLOCKS // STEP_BLOCKS)
    ffn = hb.shape[2]
    cap = x_hbm.shape[2]
    tok = ag.shape[2]
    qrows = tok // QUARTERS
    n_blocks = side * side
    units = n_blocks // UNIT_BLOCKS
    steps = n_blocks // STEP_BLOCKS
    per_unit = 2 * UNIT_BLOCKS
    per_step = 2 * STEP_BLOCKS
    tile = 256
    mt_count = model // tile
    dadb = wgu
    ft_count = ffn // tile

    def device(y, x, c):
        return (y * side + x) * 2 + c

    def neighbour(dy, dx):
        return device(lax.rem(my_y + dy, side), lax.rem(my_x + dx, side), core)

    sibling = device(my_y, my_x, 1 - core)

    def origin(p, r):
        oy = lax.shift_right_logical(jnp.int32(ORIGIN_Y), 2 * p) & 3
        ox = lax.shift_right_logical(jnp.int32(ORIGIN_X), 2 * p) & 3
        c = core + r - 2 * core * r
        return device(lax.rem(my_y + side - oy, side), lax.rem(my_x + side - ox, side), c)

    def quarter(r, p, q):
        return ag.at[r, p, pl.ds(q * qrows, qrows)]

    def ici_copy(p_from, p_to, q, to):
        return pltpu.make_async_remote_copy(
            src_ref=quarter(0, p_from, q), dst_ref=quarter(0, p_to, q), send_sem=send_sem,
            recv_sem=recv_sem.at[p_to, q], device_id={'ep': to}, device_id_type=MESH)

    def ici_route(p_from, p_to, to):
        return pltpu.make_async_remote_copy(
            src_ref=rt.at[0, p_from], dst_ref=rt.at[0, p_to], send_sem=rsend_sem,
            recv_sem=rrecv_sem.at[p_to], device_id={'ep': to}, device_id_type=MESH)

    def sib_copy(p, q):
        return pltpu.make_async_remote_copy(
            src_ref=quarter(0, p, q), dst_ref=quarter(1, p, q), send_sem=ssend_sem,
            recv_sem=srecv_sem.at[p, q], device_id={'ep': sibling}, device_id_type=MESH)

    def sib_route(p):
        return pltpu.make_async_remote_copy(
            src_ref=rt.at[0, p], dst_ref=rt.at[1, p], send_sem=srsend_sem,
            recv_sem=srrecv_sem.at[p], device_id={'ep': sibling}, device_id_type=MESH)

    def issue(slot):
        for (dy, dx), sends in SENDS.items():
            oy, ox, q = sends[slot]
            p_from, p_to = PLACE[(oy, ox)], PLACE[((oy + dy) % 4, (ox + dx) % 4)]
            to = neighbour(dy, dx)
            ici_copy(p_from, p_to, q, to).start()
            if q == 0:
                ici_route(p_from, p_to, to).start()

    def service(slot):
        for (dy, dx), sends in SENDS.items():
            oy, ox, q = sends[slot]
            p_to = PLACE[((oy + dy) % 4, (ox + dx) % 4)]
            ici_copy(p_to, p_to, q, me).wait_recv()
            if q == 0:
                ici_route(p_to, p_to, me).wait_recv()
        if slot + 3 < SLOTS:
            issue(slot + 3)
        for (dy, dx), sends in SENDS.items():
            oy, ox, q = sends[slot]
            p_to = PLACE[((oy + dy) % 4, (ox + dx) % 4)]
            sib_copy(p_to, q).start()
            if q == 0:
                sib_route(p_to).start()

    def x_copy(block, j, e, row, sem):
        src = origin(block + j // 2, j % 2)
        return pltpu.make_async_copy(x_hbm.at[src, e], xb.at[e, pl.ds(row + j * cap, cap)], x_sem.at[e, sem + j])

    def unit_x(g, e):
        return [x_copy(g * UNIT_BLOCKS, j, e, 0, 0) for j in range(per_unit)]

    def unit_fill(g, e):
        u = g * e_local + e
        return unit_x(g, e) + [pltpu.make_async_copy(pq_hbm.at[u], pq.at[e], fill_sem.at[e, 0]),
                               pltpu.make_async_copy(h_hbm.at[u], hb.at[e], fill_sem.at[e, 1])]

    def dadb_copy(t, e, j):
        src = origin(t * STEP_BLOCKS + j // 2, j % 2)
        row = pl.multiple_of(lax.rem(t, 2) * rows_s + j * cap, cap)
        return pltpu.make_async_copy(dadb.at[e, pl.ds(row, cap)], dadb_hbm.at[src, e], dadb_sem.at[e, j])

    def spill_copies(u, e):
        return (pltpu.make_async_copy(pq.at[e], pq_hbm.at[u], spill_sem.at[e, 0]),
                pltpu.make_async_copy(hb.at[e], h_hbm.at[u], spill_sem.at[e, 1]))

    w_copies = [pltpu.make_async_copy(wg_hbm, wgu.at[:, :, pl.ds(0, ffn)], w_sem.at[0]),
                pltpu.make_async_copy(wu_hbm, wgu.at[:, :, pl.ds(ffn, ffn)], w_sem.at[1]),
                pltpu.make_async_copy(wd_hbm, wd, w_sem.at[2])]
    own = pltpu.make_async_copy(dout_hbm, ag.at[0, 0], own_sem)

    own.start()
    barrier = pltpu.get_barrier_semaphore()

    partners = [neighbour(dy, dx) for dy, dx in SENDS] + [sibling]
    for to in partners:
        pl.semaphore_signal(barrier, inc=1, device_id={'ep': to}, device_id_type=MESH)

    for c in w_copies[:2]:
        c.start()
    for e in range(e_local):
        for c in unit_x(1, e):
            c.start()
    w_copies[2].start()
    top_k = slots_ref.shape[0]
    rt[0, 0] = jnp.concatenate([jnp.full((8, tok), -1.0, F32), jnp.zeros((8, tok), F32)], axis=0)
    slots = slots_ref[...]
    rt[0, 0, 0:top_k] = jnp.where(slots >= 0, ids_ref[...] * cap + slots, -1).astype(F32)
    rt[0, 0, 8:8 + top_k] = gates_ref[...]
    own.wait()
    pl.semaphore_wait(barrier, len(partners))
    for slot in range(3):
        issue(slot)
    for q in range(QUARTERS):
        sib_copy(0, q).start()
    sib_route(0).start()

    @pl.loop(0, mt_count)
    def _(m):
        rows = pl.ds(pl.multiple_of(m * tile, tile), tile)
        for e in range(e_local):
            acc_gu[e, rows] = jnp.zeros((tile, 2 * ffn), F32)

    @pl.loop(0, ft_count)
    def _(m):
        rows = pl.ds(pl.multiple_of(m * tile, tile), tile)
        for e in range(e_local):
            acc_d[e, rows] = jnp.zeros((tile, model), F32)

    for c in w_copies[:2]:
        c.wait()

    @pl.loop(0, units * e_local)
    def _(u):
        turn, e = u // e_local, lax.rem(u, e_local)
        g = lax.rem(turn + 1, units)
        for c in unit_x(g, e):
            c.wait()

        @pl.when(u >= e_local)
        def _():
            for c in spill_copies(g * e_local + e, e):
                c.wait()

        @pl.loop(0, ft_count)
        def _(n):
            lo = pl.ds(pl.multiple_of(n * tile, tile), tile)
            hi = pl.ds(pl.multiple_of(ffn + n * tile, tile), tile)
            x = xb[e]
            a = jnp.dot(x, wgu[e, :, lo], preferred_element_type=F32)
            b = jnp.dot(x, wgu[e, :, hi], preferred_element_type=F32)
            sg = jax.nn.sigmoid(a)
            silu = a * sg
            hb[e, :, lo] = (silu * b).astype(BF16)
            pq[e, :, lo] = b * sg * (1.0 + a * (1.0 - sg))
            pq[e, :, hi] = silu

        @pl.when(turn + 1 < units)
        def _():
            for c in spill_copies(g * e_local + e, e):
                c.start()
            for c in unit_x(lax.rem(turn + 2, units), e):
                c.start()

        for k, at in ((0, 2), (1, 4), (2, 6)):
            @pl.when(u == at)
            def _(k=k):
                service(k)

    w_copies[2].wait()

    def hits(r, p, e):
        local = rt[r, p, 0:8] - (me * (e_local * cap) + e * cap).astype(F32)
        hit = (local >= 0.0) & (local < float(cap))
        slot = jnp.max(jnp.where(hit, local, -1.0), axis=0, keepdims=True)
        gate = jnp.sum(jnp.where(hit, rt[r, p, 8:16], 0.0), axis=0, keepdims=True)
        return slot, gate

    def on(table, t):
        for step, slots in table.items():
            @pl.when(t == step)
            def _(slots=slots):
                for k in slots:
                    service(k)

    slot_iota = lax.broadcasted_iota(jnp.int32, (cap, tok), 0).astype(F32)

    @pl.loop(0, steps)
    def _(t):
        on(BEFORE, t)
        odd = lax.rem(t, 2)
        half = pl.multiple_of(odd * rows_s, rows_s)
        here = pl.ds(half, rows_s)
        dy_here = pl.ds(pl.multiple_of(rows_s + half, rows_s), rows_s)

        @pl.loop(0, 2)
        def _(r):
            @pl.when(r == 1)
            def _():
                for i in range(STEP_BLOCKS):
                    for q in range(QUARTERS):
                        sib_copy(t * STEP_BLOCKS + i, q).wait_recv()
                    sib_route(t * STEP_BLOCKS + i).wait_recv()

            for i in range(STEP_BLOCKS):
                p = t * STEP_BLOCKS + i
                picks, gates = [], []
                for e in range(e_local):
                    slot, gate = hits(r, p, e)
                    pick = slot_iota == slot
                    gates.append(jnp.sum(jnp.where(pick, gate, 0.0), axis=1, keepdims=True))
                    picks.append(jnp.where(pick, 1.0, 0.0).astype(BF16))
                pick = jnp.concatenate(picks, axis=0)
                row = pl.multiple_of((2 * i + r) * cap, cap)
                for n in range(model // 512):
                    cols = pl.ds(n * 512, 512)
                    d = jnp.dot(pick, ag[r, p, :, cols], preferred_element_type=F32)
                    for e in range(e_local):
                        d_e = d[e * cap:(e + 1) * cap]
                        db[e, pl.ds(row, cap), cols] = d_e.astype(BF16)
                        db[e, pl.ds(pl.multiple_of(rows_s + half + row, cap), cap), cols] = (
                            d_e * gates[e]).astype(BF16)

        @pl.loop(0, e_local)
        def _(e):
            @pl.when((odd == 0) & (t > 0))
            def _():
                for c in unit_fill(t // 2, e):
                    c.wait()

            @pl.when(t > 0)
            def _():
                for j in range(per_step):
                    dadb_copy(t, e, j).wait()

            part = jnp.zeros((rows_s, 128), F32)
            for n in range(ft_count):
                lo, hi = pl.ds(n * tile, tile), pl.ds(ffn + n * tile, tile)
                lhs = jnp.concatenate([db[e, 0:rows_s], db[e, dy_here]], axis=0)
                both = lax.dot_general(lhs, wd[e, lo, :], NT, preferred_element_type=F32)
                prod = hb[e, here, lo].astype(F32) * both[:rows_s]
                part += prod[:, :128] + prod[:, 128:]
                dh = both[rows_s:].astype(BF16).astype(F32)
                dadb[e, here, lo] = (dh * pq[e, here, lo]).astype(BF16)
                dadb[e, here, hi] = (dh * pq[e, here, hi]).astype(BF16)

            total = jnp.broadcast_to(jnp.sum(part, axis=1, keepdims=True), part.shape)
            for j in range(per_step):
                slot, _ = hits(j % 2, t * STEP_BLOCKS + j // 2, e)
                value = jnp.concatenate([total[j * cap:(j + 1) * cap]] * (tok // 128), axis=1)
                gsend[t * per_step + j, e] = jnp.sum(
                    jnp.where(slot_iota == slot, value, 0.0), axis=0, keepdims=True)

            for j in range(per_step):
                dadb_copy(t, e, j).start()

            @pl.when((t == 0) & (e == e_local - 1))
            def _():
                grecv[me] = gsend[0]

            @pl.when(e == e_local - 1)
            def _():
                @pl.loop(jnp.where(t == 0, 1, 0), per_step)
                def _(j):
                    to = origin(t * STEP_BLOCKS + j // 2, lax.rem(j, 2))
                    pltpu.make_async_remote_copy(
                        src_ref=gsend.at[t * per_step + j], dst_ref=grecv.at[me], send_sem=gsend_sem,
                        recv_sem=grecv_sem, device_id={'ep': to}, device_id_type=MESH).start()

            def weight_grads(rows, dy_rows):
                @pl.loop(0, 2)
                def _(m):
                    out = pl.ds(pl.multiple_of(m * (model // 2), model // 2), model // 2)
                    for n in range(2):
                        cols = pl.ds(n * ffn, ffn)
                        acc_gu[e, out, cols] += lax.dot_general(
                            xb[e, rows, out], dadb[e, rows, cols], TN, preferred_element_type=F32)

                for n in range(model // 512):
                    cols = pl.ds(n * 512, 512)
                    acc_d[e, :, cols] += lax.dot_general(
                        hb[e, rows, :], db[e, dy_rows, cols], TN, preferred_element_type=F32)

            for step, slots in LATE.items():
                @pl.when((t == step) & (e == e_local - 1))
                def _(slots=slots):
                    for k in slots:
                        service(k)

            @pl.when((odd == 1) & (t < steps - 2))
            def _():
                weight_grads(pl.ds(0, rows_u), pl.ds(rows_s, rows_u))
                for c in unit_fill(t // 2 + 1, e):
                    c.start()

            @pl.when(t >= steps - 2)
            def _():
                weight_grads(here, dy_here)

            for step, slots in BETWEEN.items():
                @pl.when((t == step) & (e == 0))
                def _(slots=slots):
                    for k in slots:
                        service(k)


    def drain(ref, sem):
        pltpu.make_async_copy(ref, ref, sem).wait()

    drain(ag.at[0, pl.ds(0, n_blocks - 1)], send_sem)
    drain(rt.at[0, pl.ds(0, n_blocks - 1)], rsend_sem)
    drain(ag.at[0], ssend_sem)
    drain(rt.at[0], srsend_sem)
    drain(gsend.at[pl.ds(0, group_size - 1)], gsend_sem)
    drain(grecv.at[pl.ds(0, group_size - 1)], grecv_sem)
    for e in range(e_local):
        for j in range(per_step):
            dadb_copy(jnp.int32(steps - 1), e, j).wait()


def run_experts(x_disp, w_gate, w_up, w_down, d_out, slots, ids, gates, group_size):
    sources, e_local, cap, model = x_disp.shape
    ffn = w_gate.shape[2]
    tok = d_out.shape[0]
    n_blocks = group_size // 2
    per_unit = 2 * UNIT_BLOCKS
    rows_u = per_unit * cap
    per_step = 2 * STEP_BLOCKS
    rows_s = per_step * cap
    units = n_blocks // UNIT_BLOCKS * e_local
    dma = pltpu.SemaphoreType.DMA
    any_spec = pl.BlockSpec(memory_space=pl.ANY)
    vmem_spec = pl.BlockSpec(memory_space=pltpu.VMEM)
    out_shape = [
        jax.ShapeDtypeStruct((sources, e_local, cap, 2 * ffn), BF16),
        pltpu.VMEM((e_local, model, 2 * ffn), F32),
        pltpu.VMEM((e_local, ffn, model), F32),
        pltpu.VMEM((group_size, e_local, 1, tok), F32),
        jax.ShapeDtypeStruct((units, rows_u, 2 * ffn), F32),
        jax.ShapeDtypeStruct((units, rows_u, ffn), BF16),
    ]
    scratch = [
        pltpu.VMEM((2, n_blocks, tok, model), BF16),
        pltpu.VMEM((2, n_blocks, 16, tok), F32),
        pltpu.VMEM((e_local, model, 2 * ffn), BF16),
        pltpu.VMEM((e_local, ffn, model), BF16),
        pltpu.VMEM((e_local, rows_u, model), BF16),
        pltpu.VMEM((e_local, rows_s + rows_u, model), BF16),
        pltpu.VMEM((e_local, rows_u, 2 * ffn), F32),
        pltpu.VMEM((e_local, rows_u, ffn), BF16),
        pltpu.VMEM((group_size, e_local, 1, tok), F32),
        dma((3,)), dma, dma((e_local, per_unit)), dma((e_local, 2)), dma((e_local, 2)),
        dma((e_local, per_step)),
        dma((n_blocks, QUARTERS)), dma((n_blocks,)), dma, dma,
        dma((n_blocks, QUARTERS)), dma((n_blocks,)), dma, dma, dma, dma,
    ]
    return pl.pallas_call(
        functools.partial(expert_kernel, group_size),
        out_shape=out_shape, in_specs=[any_spec] * 5 + [vmem_spec] * 3,
        out_specs=[any_spec, vmem_spec, vmem_spec, vmem_spec, any_spec, any_spec], scratch_shapes=scratch,
        compiler_params=pltpu.CompilerParams(collective_id=0, has_side_effects=True, vmem_limit_bytes=VMEM_A),
    )(x_disp, w_gate, w_up, w_down, d_out, slots, ids, gates)


def finish_kernel(group_size, chunk, dadb, wg, wu, back, acc_gu, acc_d, ids, slots,
                  gx, g_gate, g_up, g_down, gate_out,
                  wbuf, dbuf, obuf, st_g, st_u, st_d, w_sem, d_sem, o_sem, s_sem):
    sources, e_local, cap, width = dadb.shape
    ffn = width // 2
    model = gx.shape[3]
    per_e = sources // chunk
    chunks = e_local * per_e
    m_blk, f_blk = model // per_e, ffn // per_e
    depth = dbuf.shape[0]

    def load(c):
        slot = lax.rem(c, depth)
        return pltpu.make_async_copy(
            dadb.at[pl.ds(lax.rem(c, per_e) * chunk, chunk), c // per_e], dbuf.at[slot], d_sem.at[slot])

    def store(c):
        slot = lax.rem(c, 2)
        return pltpu.make_async_copy(
            obuf.at[slot], gx.at[pl.ds(lax.rem(c, per_e) * chunk, chunk), c // per_e], o_sem.at[slot])

    def weights(e):
        return [pltpu.make_async_copy(wg.at[e], wbuf.at[e, :, pl.ds(0, ffn)], w_sem.at[e, 0]),
                pltpu.make_async_copy(wu.at[e], wbuf.at[e, :, pl.ds(ffn, ffn)], w_sem.at[e, 1])]

    def staged(c):
        e, i = c // per_e, lax.rem(c, per_e)
        m = pl.ds(pl.multiple_of(i * m_blk, m_blk), m_blk)
        f = pl.ds(pl.multiple_of(i * f_blk, f_blk), f_blk)
        return e, m, f, [pltpu.make_async_copy(st_g.at[e, m], g_gate.at[e, m], s_sem.at[c, 0]),
                         pltpu.make_async_copy(st_u.at[e, m], g_up.at[e, m], s_sem.at[c, 1]),
                         pltpu.make_async_copy(st_d.at[e, f], g_down.at[e, f], s_sem.at[c, 2])]

    for c in weights(0):
        c.start()
    for k in range(depth):
        load(jnp.int32(k)).start()
    for e in range(1, e_local):
        for c in weights(e):
            c.start()

    def cast(c):
        e, m, f, copies = staged(c)
        st_g[e, m] = acc_gu[e, m, 0:ffn].astype(BF16)
        st_u[e, m] = acc_gu[e, m, ffn:width].astype(BF16)
        st_d[e, f] = acc_d[e, f].astype(BF16)
        return copies

    for e in range(e_local):
        for w in weights(e):
            w.wait()

        @pl.loop(e * per_e, (e + 1) * per_e)
        def _(c, e=e):
            load(c).wait()

            @pl.when(c >= 2)
            def _():
                store(c - 2).wait()

            slot, out_slot = lax.rem(c, depth), lax.rem(c, 2)
            copies = cast(c)
            both = dbuf[slot].reshape(chunk * cap, width)
            for n in range(model // 512):
                rows = pl.ds(n * 512, 512)
                out = lax.dot_general(both, wbuf[e, rows], NT, preferred_element_type=F32)
                obuf[out_slot, :, :, rows] = out.astype(BF16).reshape(chunk, cap, 512)
            store(c).start()
            for s in copies:
                s.start()

            @pl.when(c + depth < chunks)
            def _():
                load(c + depth).start()

    total = jnp.zeros(gate_out.shape, F32)
    for d in range(group_size):
        for e in range(e_local):
            total += jnp.where(ids[...] == d * e_local + e, back[d, e], 0.0)
    gate_out[...] = jnp.where(slots[...] >= 0, total, 0.0)

    for c in range(chunks - 2, chunks):
        store(jnp.int32(c)).wait()
    for c in range(chunks):
        for s in staged(jnp.int32(c))[3]:
            s.wait()


def run_finish(dadb, w_gate, w_up, acc_gu, acc_d, back, ids, slots, group_size):
    sources, e_local, cap, width = dadb.shape
    model, ffn = w_gate.shape[1:]
    top_k, tok = ids.shape
    chunk = 8
    dma = pltpu.SemaphoreType.DMA
    any_spec = pl.BlockSpec(memory_space=pl.ANY)
    vmem_spec = pl.BlockSpec(memory_space=pltpu.VMEM)
    return pl.pallas_call(
        functools.partial(finish_kernel, group_size, chunk),
        in_specs=[any_spec] * 3 + [vmem_spec] * 5,
        out_specs=[any_spec] * 4 + [vmem_spec],
        out_shape=[
            jax.ShapeDtypeStruct((sources, e_local, cap, model), BF16),
            jax.ShapeDtypeStruct((e_local, model, ffn), BF16),
            jax.ShapeDtypeStruct((e_local, model, ffn), BF16),
            jax.ShapeDtypeStruct((e_local, ffn, model), BF16),
            jax.ShapeDtypeStruct((top_k, tok), F32),
        ],
        scratch_shapes=[
            pltpu.VMEM((e_local, model, width), BF16),
            pltpu.VMEM((3, chunk, cap, width), BF16),
            pltpu.VMEM((2, chunk, cap, model), BF16),
            pltpu.VMEM((e_local, model, ffn), BF16),
            pltpu.VMEM((e_local, model, ffn), BF16),
            pltpu.VMEM((e_local, ffn, model), BF16),
            dma((e_local, 2)), dma((3,)), dma((2,)), dma((e_local * sources // chunk, 3)),
        ],
        compiler_params=pltpu.CompilerParams(vmem_limit_bytes=VMEM_B),
    )(*[pltpu.with_memory_space_constraint(a, pltpu.HBM) for a in (dadb, w_gate, w_up)],
      *[pltpu.with_memory_space_constraint(a, pltpu.VMEM) for a in (back, acc_gu, acc_d)], ids, slots)


def solution(mesh):
    group_size = mesh.shape['ep']

    def local_step(x_disp, w_gate, w_up, w_down, d_out, slot_idx, expert_id, gate_wt):
        slots, ids = slot_idx.T, expert_id.T
        dadb, acc_gu, acc_d, back, _, _ = run_experts(
            x_disp, w_gate, w_up, w_down, d_out, slots, ids, gate_wt.T, group_size)
        grad_x, grad_w_gate, grad_w_up, grad_w_down, gate = run_finish(
            dadb, w_gate, w_up, acc_gu, acc_d, back, ids, slots, group_size)
        return grad_x, grad_w_gate, grad_w_up, grad_w_down, gate.T

    token_place = P(('dp', 'ep'), None)
    weight_place = P('ep', None, None)
    slot_place = P('dp', 'ep', None, None)
    grad_place = P(('dp', 'ep'), None, None)
    return jax.shard_map(local_step, mesh=mesh,
                         in_specs=(slot_place, weight_place, weight_place, weight_place, token_place, token_place, token_place, token_place),
                         out_specs=(slot_place, grad_place, grad_place, grad_place, token_place),
                         check_vma=False)
```

```python
import functools
import math

import jax
import jax.numpy as jnp
from jax import lax
from jax.experimental import pallas as pl
from jax.experimental.pallas import tpu as pltpu
from jax.sharding import PartitionSpec as P

F32 = jnp.float32
BF16 = jnp.bfloat16
MESH = pl.DeviceIdType.MESH

ORDER = [(0, 0), (0, 1), (0, 3), (1, 0), (3, 0), (0, 2), (2, 0), (1, 1),
         (1, 3), (3, 1), (3, 3), (1, 2), (2, 1), (2, 3), (3, 2), (2, 2)]
PLACE = {block: place for place, block in enumerate(ORDER)}


def packed(values):
    total = sum(v << (2 * k) for k, v in enumerate(values))
    return total - 2 ** 32 if total >= 2 ** 31 else total


ORIGIN_Y, ORIGIN_X = packed([b[0] for b in ORDER]), packed([b[1] for b in ORDER])
QUARTERS = 4
VMEM_A = 45 * 1024 * 1024 + 832 * 1024
VMEM_B = 22 * 1024 * 1024
UNIT_BLOCKS = 4
STEP_BLOCKS = 2
BEFORE = {0: (3,), 3: (7,), 4: (9,), 5: (11,), 6: (13,)}
BETWEEN = {0: (4,), 1: (5,), 2: (6,), 3: (8,)}
LATE = {4: (10,), 5: (12,), 6: (14,)}
NT = (((1,), (1,)), ((), ()))
TN = (((0,), (0,)), ((), ()))


def send_lists():
    flip = (1, 0, 3, 2)
    plus_x = [(0, 0, 1), (0, 0, 0), (0, 0, 2), (0, 0, 3), (0, 1, 0), (0, 1, 2), (1, 0, 3), (1, 0, 2),
              (3, 0, 2), (3, 0, 3), (2, 0, 2), (1, 1, 2), (2, 0, 3), (3, 1, 2), (2, 1, 2)]
    plus_y = [(0, 0, 0), (0, 0, 3), (0, 0, 2), (0, 0, 1), (1, 0, 0), (1, 0, 2), (0, 1, 1), (0, 1, 0),
              (0, 3, 1), (0, 3, 0), (0, 2, 0), (0, 2, 1), (1, 1, 0), (1, 3, 0), (1, 2, 0)]
    minus_x = [(oy, -ox % 4, flip[q]) for oy, ox, q in plus_x]
    minus_y = [(-oy % 4, ox, flip[q]) for oy, ox, q in plus_y]
    return {(0, 1): plus_x, (0, 3): minus_x, (1, 0): plus_y, (3, 0): minus_y}


SENDS = send_lists()
SLOTS = len(SENDS[(0, 1)])


def expert_kernel(group_size, x_hbm, wg_hbm, wu_hbm, wd_hbm, dout_hbm, slots_ref, ids_ref, gates_ref,
                  dadb_hbm, acc_gu, acc_d, grecv, pq_hbm, h_hbm,
                  ag, rt, wgu, wd, xb, db, pq, hb, gsend,
                  w_sem, own_sem, x_sem, spill_sem, fill_sem, dadb_sem,
                  recv_sem, rrecv_sem, send_sem, rsend_sem,
                  srecv_sem, srrecv_sem, ssend_sem, srsend_sem, gsend_sem, grecv_sem):
    side = math.isqrt(group_size // 2)
    me = lax.axis_index('ep')
    core = lax.rem(me, 2)
    my_x = lax.rem(me // 2, side)
    my_y = me // (2 * side)
    e_local, rows_u, model = xb.shape
    rows_s = rows_u // (UNIT_BLOCKS // STEP_BLOCKS)
    ffn = hb.shape[2]
    cap = x_hbm.shape[2]
    tok = ag.shape[2]
    qrows = tok // QUARTERS
    n_blocks = side * side
    units = n_blocks // UNIT_BLOCKS
    steps = n_blocks // STEP_BLOCKS
    per_unit = 2 * UNIT_BLOCKS
    per_step = 2 * STEP_BLOCKS
    tile = 256
    mt_count = model // tile
    dadb = wgu
    ft_count = ffn // tile

    def device(y, x, c):
        return (y * side + x) * 2 + c

    def neighbour(dy, dx):
        return device(lax.rem(my_y + dy, side), lax.rem(my_x + dx, side), core)

    sibling = device(my_y, my_x, 1 - core)

    def origin(p, r):
        oy = lax.shift_right_logical(jnp.int32(ORIGIN_Y), 2 * p) & 3
        ox = lax.shift_right_logical(jnp.int32(ORIGIN_X), 2 * p) & 3
        c = core + r - 2 * core * r
        return device(lax.rem(my_y + side - oy, side), lax.rem(my_x + side - ox, side), c)

    def quarter(r, p, q):
        return ag.at[r, p, pl.ds(q * qrows, qrows)]

    def ici_copy(p_from, p_to, q, to):
        return pltpu.make_async_remote_copy(
            src_ref=quarter(0, p_from, q), dst_ref=quarter(0, p_to, q), send_sem=send_sem,
            recv_sem=recv_sem.at[p_to, q], device_id={'ep': to}, device_id_type=MESH)

    def ici_route(p_from, p_to, to):
        return pltpu.make_async_remote_copy(
            src_ref=rt.at[0, p_from], dst_ref=rt.at[0, p_to], send_sem=rsend_sem,
            recv_sem=rrecv_sem.at[p_to], device_id={'ep': to}, device_id_type=MESH)

    def sib_copy(p, q):
        return pltpu.make_async_remote_copy(
            src_ref=quarter(0, p, q), dst_ref=quarter(1, p, q), send_sem=ssend_sem,
            recv_sem=srecv_sem.at[p, q], device_id={'ep': sibling}, device_id_type=MESH)

    def sib_route(p):
        return pltpu.make_async_remote_copy(
            src_ref=rt.at[0, p], dst_ref=rt.at[1, p], send_sem=srsend_sem,
            recv_sem=srrecv_sem.at[p], device_id={'ep': sibling}, device_id_type=MESH)

    def issue(slot):
        for (dy, dx), sends in SENDS.items():
            oy, ox, q = sends[slot]
            p_from, p_to = PLACE[(oy, ox)], PLACE[((oy + dy) % 4, (ox + dx) % 4)]
            to = neighbour(dy, dx)
            ici_copy(p_from, p_to, q, to).start()
            if q == 0:
                ici_route(p_from, p_to, to).start()

    def service(slot):
        for (dy, dx), sends in SENDS.items():
            oy, ox, q = sends[slot]
            p_to = PLACE[((oy + dy) % 4, (ox + dx) % 4)]
            ici_copy(p_to, p_to, q, me).wait_recv()
            if q == 0:
                ici_route(p_to, p_to, me).wait_recv()
        if slot + 3 < SLOTS:
            issue(slot + 3)
        for (dy, dx), sends in SENDS.items():
            oy, ox, q = sends[slot]
            p_to = PLACE[((oy + dy) % 4, (ox + dx) % 4)]
            sib_copy(p_to, q).start()
            if q == 0:
                sib_route(p_to).start()

    def x_copy(block, j, e, row, sem):
        src = origin(block + j // 2, j % 2)
        return pltpu.make_async_copy(x_hbm.at[src, e], xb.at[e, pl.ds(row + j * cap, cap)], x_sem.at[e, sem + j])

    def unit_x(g, e):
        return [x_copy(g * UNIT_BLOCKS, j, e, 0, 0) for j in range(per_unit)]

    def unit_fill(g, e):
        u = g * e_local + e
        return unit_x(g, e) + [pltpu.make_async_copy(pq_hbm.at[u], pq.at[e], fill_sem.at[e, 0]),
                               pltpu.make_async_copy(h_hbm.at[u], hb.at[e], fill_sem.at[e, 1])]

    def dadb_copy(t, e, j):
        src = origin(t * STEP_BLOCKS + j // 2, j % 2)
        row = pl.multiple_of(lax.rem(t, 2) * rows_s + j * cap, cap)
        return pltpu.make_async_copy(dadb.at[e, pl.ds(row, cap)], dadb_hbm.at[src, e], dadb_sem.at[e, j])

    def spill_copies(u, e):
        return (pltpu.make_async_copy(pq.at[e], pq_hbm.at[u], spill_sem.at[e, 0]),
                pltpu.make_async_copy(hb.at[e], h_hbm.at[u], spill_sem.at[e, 1]))

    w_copies = [pltpu.make_async_copy(wg_hbm, wgu.at[:, :, pl.ds(0, ffn)], w_sem.at[0]),
                pltpu.make_async_copy(wu_hbm, wgu.at[:, :, pl.ds(ffn, ffn)], w_sem.at[1]),
                pltpu.make_async_copy(wd_hbm, wd, w_sem.at[2])]
    own = pltpu.make_async_copy(dout_hbm, ag.at[0, 0], own_sem)

    own.start()
    barrier = pltpu.get_barrier_semaphore()

    partners = [neighbour(dy, dx) for dy, dx in SENDS] + [sibling]
    for to in partners:
        pl.semaphore_signal(barrier, inc=1, device_id={'ep': to}, device_id_type=MESH)

    for c in w_copies[:2]:
        c.start()
    for e in range(e_local):
        for c in unit_x(1, e):
            c.start()
    w_copies[2].start()
    top_k = slots_ref.shape[0]
    rt[0, 0] = jnp.concatenate([jnp.full((8, tok), -1.0, F32), jnp.zeros((8, tok), F32)], axis=0)
    slots = slots_ref[...]
    rt[0, 0, 0:top_k] = jnp.where(slots >= 0, ids_ref[...] * cap + slots, -1).astype(F32)
    rt[0, 0, 8:8 + top_k] = gates_ref[...]
    own.wait()
    pl.semaphore_wait(barrier, len(partners))
    for slot in range(3):
        issue(slot)
    for q in range(QUARTERS):
        sib_copy(0, q).start()
    sib_route(0).start()

    @pl.loop(0, mt_count)
    def _(m):
        rows = pl.ds(pl.multiple_of(m * tile, tile), tile)
        for e in range(e_local):
            acc_gu[e, rows] = jnp.zeros((tile, 2 * ffn), F32)

    @pl.loop(0, ft_count)
    def _(m):
        rows = pl.ds(pl.multiple_of(m * tile, tile), tile)
        for e in range(e_local):
            acc_d[e, rows] = jnp.zeros((tile, model), F32)

    for c in w_copies[:2]:
        c.wait()

    @pl.loop(0, units * e_local)
    def _(u):
        turn, e = u // e_local, lax.rem(u, e_local)
        g = lax.rem(turn + 1, units)
        for c in unit_x(g, e):
            c.wait()

        @pl.when(u >= e_local)
        def _():
            for c in spill_copies(g * e_local + e, e):
                c.wait()

        @pl.loop(0, ft_count)
        def _(n):
            lo = pl.ds(pl.multiple_of(n * tile, tile), tile)
            hi = pl.ds(pl.multiple_of(ffn + n * tile, tile), tile)
            x = xb[e]
            a = jnp.dot(x, wgu[e, :, lo], preferred_element_type=F32)
            b = jnp.dot(x, wgu[e, :, hi], preferred_element_type=F32)
            sg = jax.nn.sigmoid(a)
            silu = a * sg
            hb[e, :, lo] = (silu * b).astype(BF16)
            pq[e, :, lo] = b * sg * (1.0 + a * (1.0 - sg))
            pq[e, :, hi] = silu

        @pl.when(turn + 1 < units)
        def _():
            for c in spill_copies(g * e_local + e, e):
                c.start()
            for c in unit_x(lax.rem(turn + 2, units), e):
                c.start()

        for k, at in ((0, 2), (1, 4), (2, 6)):
            @pl.when(u == at)
            def _(k=k):
                service(k)

    w_copies[2].wait()

    def hits(r, p, e):
        local = rt[r, p, 0:8] - (me * (e_local * cap) + e * cap).astype(F32)
        hit = (local >= 0.0) & (local < float(cap))
        slot = jnp.max(jnp.where(hit, local, -1.0), axis=0, keepdims=True)
        gate = jnp.sum(jnp.where(hit, rt[r, p, 8:16], 0.0), axis=0, keepdims=True)
        return slot, gate

    def on(table, t):
        for step, slots in table.items():
            @pl.when(t == step)
            def _(slots=slots):
                for k in slots:
                    service(k)

    slot_iota = lax.broadcasted_iota(jnp.int32, (cap, tok), 0).astype(F32)

    @pl.loop(0, steps)
    def _(t):
        on(BEFORE, t)
        odd = lax.rem(t, 2)
        half = pl.multiple_of(odd * rows_s, rows_s)
        here = pl.ds(half, rows_s)
        dy_here = pl.ds(pl.multiple_of(rows_s + half, rows_s), rows_s)

        @pl.loop(0, 2)
        def _(r):
            @pl.when(r == 1)
            def _():
                for i in range(STEP_BLOCKS):
                    for q in range(QUARTERS):
                        sib_copy(t * STEP_BLOCKS + i, q).wait_recv()
                    sib_route(t * STEP_BLOCKS + i).wait_recv()

            for i in range(STEP_BLOCKS):
                p = t * STEP_BLOCKS + i
                picks, gates = [], []
                for e in range(e_local):
                    slot, gate = hits(r, p, e)
                    pick = slot_iota == slot
                    gates.append(jnp.sum(jnp.where(pick, gate, 0.0), axis=1, keepdims=True))
                    picks.append(jnp.where(pick, 1.0, 0.0).astype(BF16))
                pick = jnp.concatenate(picks, axis=0)
                row = pl.multiple_of((2 * i + r) * cap, cap)
                for n in range(model // 512):
                    cols = pl.ds(n * 512, 512)
                    d = jnp.dot(pick, ag[r, p, :, cols], preferred_element_type=F32)
                    for e in range(e_local):
                        d_e = d[e * cap:(e + 1) * cap]
                        db[e, pl.ds(row, cap), cols] = d_e.astype(BF16)
                        db[e, pl.ds(pl.multiple_of(rows_s + half + row, cap), cap), cols] = (
                            d_e * gates[e]).astype(BF16)

        @pl.loop(0, e_local)
        def _(e):
            @pl.when((odd == 0) & (t > 0))
            def _():
                for c in unit_fill(t // 2, e):
                    c.wait()

            @pl.when(t > 0)
            def _():
                for j in range(per_step):
                    dadb_copy(t, e, j).wait()

            part = jnp.zeros((rows_s, 128), F32)
            for n in range(ft_count):
                lo, hi = pl.ds(n * tile, tile), pl.ds(ffn + n * tile, tile)
                lhs = jnp.concatenate([db[e, 0:rows_s], db[e, dy_here]], axis=0)
                both = lax.dot_general(lhs, wd[e, lo, :], NT, preferred_element_type=F32)
                prod = hb[e, here, lo].astype(F32) * both[:rows_s]
                part += prod[:, :128] + prod[:, 128:]
                dh = both[rows_s:].astype(BF16).astype(F32)
                dadb[e, here, lo] = (dh * pq[e, here, lo]).astype(BF16)
                dadb[e, here, hi] = (dh * pq[e, here, hi]).astype(BF16)

            total = jnp.broadcast_to(jnp.sum(part, axis=1, keepdims=True), part.shape)
            for j in range(per_step):
                slot, _ = hits(j % 2, t * STEP_BLOCKS + j // 2, e)
                value = jnp.concatenate([total[j * cap:(j + 1) * cap]] * (tok // 128), axis=1)
                gsend[t * per_step + j, e] = jnp.sum(
                    jnp.where(slot_iota == slot, value, 0.0), axis=0, keepdims=True)

            for j in range(per_step):
                dadb_copy(t, e, j).start()

            @pl.when((t == 0) & (e == e_local - 1))
            def _():
                grecv[me] = gsend[0]

            @pl.when(e == e_local - 1)
            def _():
                @pl.loop(jnp.where(t == 0, 1, 0), per_step)
                def _(j):
                    to = origin(t * STEP_BLOCKS + j // 2, lax.rem(j, 2))
                    pltpu.make_async_remote_copy(
                        src_ref=gsend.at[t * per_step + j], dst_ref=grecv.at[me], send_sem=gsend_sem,
                        recv_sem=grecv_sem, device_id={'ep': to}, device_id_type=MESH).start()

            def weight_grads(rows, dy_rows):
                @pl.loop(0, 2)
                def _(m):
                    out = pl.ds(pl.multiple_of(m * (model // 2), model // 2), model // 2)
                    for n in range(2):
                        cols = pl.ds(n * ffn, ffn)
                        acc_gu[e, out, cols] += lax.dot_general(
                            xb[e, rows, out], dadb[e, rows, cols], TN, preferred_element_type=F32)

                for n in range(model // 512):
                    cols = pl.ds(n * 512, 512)
                    acc_d[e, :, cols] += lax.dot_general(
                        hb[e, rows, :], db[e, dy_rows, cols], TN, preferred_element_type=F32)

            for step, slots in LATE.items():
                @pl.when((t == step) & (e == e_local - 1))
                def _(slots=slots):
                    for k in slots:
                        service(k)

            @pl.when(t == 1)
            def _():
                weight_grads(pl.ds(0, rows_u), pl.ds(rows_s, rows_u))

            @pl.when(t > 1)
            def _():
                weight_grads(here, dy_here)

            @pl.when((odd == 1) & (t < steps - 1))
            def _():
                for c in unit_fill(t // 2 + 1, e):
                    c.start()

            for step, slots in BETWEEN.items():
                @pl.when((t == step) & (e == 0))
                def _(slots=slots):
                    for k in slots:
                        service(k)


    def drain(ref, sem):
        pltpu.make_async_copy(ref, ref, sem).wait()

    drain(ag.at[0, pl.ds(0, n_blocks - 1)], send_sem)
    drain(rt.at[0, pl.ds(0, n_blocks - 1)], rsend_sem)
    drain(ag.at[0], ssend_sem)
    drain(rt.at[0], srsend_sem)
    drain(gsend.at[pl.ds(0, group_size - 1)], gsend_sem)
    drain(grecv.at[pl.ds(0, group_size - 1)], grecv_sem)
    for e in range(e_local):
        for j in range(per_step):
            dadb_copy(jnp.int32(steps - 1), e, j).wait()


def run_experts(x_disp, w_gate, w_up, w_down, d_out, slots, ids, gates, group_size):
    sources, e_local, cap, model = x_disp.shape
    ffn = w_gate.shape[2]
    tok = d_out.shape[0]
    n_blocks = group_size // 2
    per_unit = 2 * UNIT_BLOCKS
    rows_u = per_unit * cap
    per_step = 2 * STEP_BLOCKS
    rows_s = per_step * cap
    units = n_blocks // UNIT_BLOCKS * e_local
    dma = pltpu.SemaphoreType.DMA
    any_spec = pl.BlockSpec(memory_space=pl.ANY)
    vmem_spec = pl.BlockSpec(memory_space=pltpu.VMEM)
    out_shape = [
        jax.ShapeDtypeStruct((sources, e_local, cap, 2 * ffn), BF16),
        pltpu.VMEM((e_local, model, 2 * ffn), F32),
        pltpu.VMEM((e_local, ffn, model), F32),
        pltpu.VMEM((group_size, e_local, 1, tok), F32),
        jax.ShapeDtypeStruct((units, rows_u, 2 * ffn), F32),
        jax.ShapeDtypeStruct((units, rows_u, ffn), BF16),
    ]
    scratch = [
        pltpu.VMEM((2, n_blocks, tok, model), BF16),
        pltpu.VMEM((2, n_blocks, 16, tok), F32),
        pltpu.VMEM((e_local, model, 2 * ffn), BF16),
        pltpu.VMEM((e_local, ffn, model), BF16),
        pltpu.VMEM((e_local, rows_u, model), BF16),
        pltpu.VMEM((e_local, rows_s + rows_u, model), BF16),
        pltpu.VMEM((e_local, rows_u, 2 * ffn), F32),
        pltpu.VMEM((e_local, rows_u, ffn), BF16),
        pltpu.VMEM((group_size, e_local, 1, tok), F32),
        dma((3,)), dma, dma((e_local, per_unit)), dma((e_local, 2)), dma((e_local, 2)),
        dma((e_local, per_step)),
        dma((n_blocks, QUARTERS)), dma((n_blocks,)), dma, dma,
        dma((n_blocks, QUARTERS)), dma((n_blocks,)), dma, dma, dma, dma,
    ]
    return pl.pallas_call(
        functools.partial(expert_kernel, group_size),
        out_shape=out_shape, in_specs=[any_spec] * 5 + [vmem_spec] * 3,
        out_specs=[any_spec, vmem_spec, vmem_spec, vmem_spec, any_spec, any_spec], scratch_shapes=scratch,
        compiler_params=pltpu.CompilerParams(collective_id=0, has_side_effects=True, vmem_limit_bytes=VMEM_A),
    )(x_disp, w_gate, w_up, w_down, d_out, slots, ids, gates)


def finish_kernel(group_size, chunk, dadb, wg, wu, back, acc_gu, acc_d, ids, slots,
                  gx, g_gate, g_up, g_down, gate_out,
                  wbuf, dbuf, obuf, st_g, st_u, st_d, w_sem, d_sem, o_sem, s_sem):
    sources, e_local, cap, width = dadb.shape
    ffn = width // 2
    model = gx.shape[3]
    per_e = sources // chunk
    chunks = e_local * per_e
    m_blk, f_blk = model // per_e, ffn // per_e
    depth = dbuf.shape[0]

    def load(c):
        slot = lax.rem(c, depth)
        return pltpu.make_async_copy(
            dadb.at[pl.ds(lax.rem(c, per_e) * chunk, chunk), c // per_e], dbuf.at[slot], d_sem.at[slot])

    def store(c):
        slot = lax.rem(c, 2)
        return pltpu.make_async_copy(
            obuf.at[slot], gx.at[pl.ds(lax.rem(c, per_e) * chunk, chunk), c // per_e], o_sem.at[slot])

    tiles = [pl.ds(n * 512, 512) for n in range(model // 512)]

    def weights(e, n):
        rows = tiles[n]
        return [pltpu.make_async_copy(wg.at[e, rows], wbuf.at[e, rows, pl.ds(0, ffn)], w_sem.at[e, n, 0]),
                pltpu.make_async_copy(wu.at[e, rows], wbuf.at[e, rows, pl.ds(ffn, ffn)], w_sem.at[e, n, 1])]

    def staged(c):
        e, i = c // per_e, lax.rem(c, per_e)
        m = pl.ds(pl.multiple_of(i * m_blk, m_blk), m_blk)
        f = pl.ds(pl.multiple_of(i * f_blk, f_blk), f_blk)
        return e, m, f, [pltpu.make_async_copy(st_g.at[e, m], g_gate.at[e, m], s_sem.at[c, 0]),
                         pltpu.make_async_copy(st_u.at[e, m], g_up.at[e, m], s_sem.at[c, 1]),
                         pltpu.make_async_copy(st_d.at[e, f], g_down.at[e, f], s_sem.at[c, 2])]

    load(jnp.int32(0)).start()
    for e in range(e_local):
        for n in range(len(tiles)):
            for c in weights(e, n):
                c.start()
        if e == 0:
            for k in range(1, depth):
                load(jnp.int32(k)).start()

    def cast(c):
        e, m, f, copies = staged(c)
        st_g[e, m] = acc_gu[e, m, 0:ffn].astype(BF16)
        st_u[e, m] = acc_gu[e, m, ffn:width].astype(BF16)
        st_d[e, f] = acc_d[e, f].astype(BF16)
        return copies

    def product(c, e, wait):
        load(c).wait()

        @pl.when(c >= 2)
        def _():
            store(c - 2).wait()

        slot, out_slot = lax.rem(c, depth), lax.rem(c, 2)
        copies = cast(c)
        both = dbuf[slot].reshape(chunk * cap, width)
        for n, rows in enumerate(tiles):
            if wait:
                for w in weights(e, n):
                    w.wait()
            out = lax.dot_general(both, wbuf[e, rows], NT, preferred_element_type=F32)
            obuf[out_slot, :, :, rows] = out.astype(BF16).reshape(chunk, cap, 512)
        store(c).start()
        for s in copies:
            s.start()

        @pl.when(c + depth < chunks)
        def _():
            load(c + depth).start()

    for e in range(e_local):
        product(jnp.int32(e * per_e), e, True)

        @pl.loop(e * per_e + 1, (e + 1) * per_e)
        def _(c, e=e):
            product(c, e, False)

    total = jnp.zeros(gate_out.shape, F32)
    for d in range(group_size):
        for e in range(e_local):
            total += jnp.where(ids[...] == d * e_local + e, back[d, e], 0.0)
    gate_out[...] = jnp.where(slots[...] >= 0, total, 0.0)

    for c in range(chunks - 2, chunks):
        store(jnp.int32(c)).wait()
    for c in range(chunks):
        for s in staged(jnp.int32(c))[3]:
            s.wait()


def run_finish(dadb, w_gate, w_up, acc_gu, acc_d, back, ids, slots, group_size):
    sources, e_local, cap, width = dadb.shape
    model, ffn = w_gate.shape[1:]
    top_k, tok = ids.shape
    chunk = 8
    dma = pltpu.SemaphoreType.DMA
    any_spec = pl.BlockSpec(memory_space=pl.ANY)
    vmem_spec = pl.BlockSpec(memory_space=pltpu.VMEM)
    return pl.pallas_call(
        functools.partial(finish_kernel, group_size, chunk),
        in_specs=[any_spec] * 3 + [vmem_spec] * 5,
        out_specs=[any_spec] * 4 + [vmem_spec],
        out_shape=[
            jax.ShapeDtypeStruct((sources, e_local, cap, model), BF16),
            jax.ShapeDtypeStruct((e_local, model, ffn), BF16),
            jax.ShapeDtypeStruct((e_local, model, ffn), BF16),
            jax.ShapeDtypeStruct((e_local, ffn, model), BF16),
            jax.ShapeDtypeStruct((top_k, tok), F32),
        ],
        scratch_shapes=[
            pltpu.VMEM((e_local, model, width), BF16),
            pltpu.VMEM((3, chunk, cap, width), BF16),
            pltpu.VMEM((2, chunk, cap, model), BF16),
            pltpu.VMEM((e_local, model, ffn), BF16),
            pltpu.VMEM((e_local, model, ffn), BF16),
            pltpu.VMEM((e_local, ffn, model), BF16),
            dma((e_local, model // 512, 2)), dma((3,)), dma((2,)), dma((e_local * sources // chunk, 3)),
        ],
        compiler_params=pltpu.CompilerParams(vmem_limit_bytes=VMEM_B),
    )(*[pltpu.with_memory_space_constraint(a, pltpu.HBM) for a in (dadb, w_gate, w_up)],
      *[pltpu.with_memory_space_constraint(a, pltpu.VMEM) for a in (back, acc_gu, acc_d)], ids, slots)


def solution(mesh):
    group_size = mesh.shape['ep']

    def local_step(x_disp, w_gate, w_up, w_down, d_out, slot_idx, expert_id, gate_wt):
        slots, ids = slot_idx.T, expert_id.T
        dadb, acc_gu, acc_d, back, _, _ = run_experts(
            x_disp, w_gate, w_up, w_down, d_out, slots, ids, gate_wt.T, group_size)
        grad_x, grad_w_gate, grad_w_up, grad_w_down, gate = run_finish(
            dadb, w_gate, w_up, acc_gu, acc_d, back, ids, slots, group_size)
        return grad_x, grad_w_gate, grad_w_up, grad_w_down, gate.T

    token_place = P(('dp', 'ep'), None)
    weight_place = P('ep', None, None)
    slot_place = P('dp', 'ep', None, None)
    grad_place = P(('dp', 'ep'), None, None)
    return jax.shard_map(local_step, mesh=mesh,
                         in_specs=(slot_place, weight_place, weight_place, weight_place, token_place, token_place, token_place, token_place),
                         out_specs=(slot_place, grad_place, grad_place, grad_place, token_place),
                         check_vma=False)
```

```python
import functools
import math

import jax
import jax.numpy as jnp
from jax import lax
from jax.experimental import pallas as pl
from jax.experimental.pallas import tpu as pltpu
from jax.sharding import PartitionSpec as P

F32 = jnp.float32
BF16 = jnp.bfloat16
MESH = pl.DeviceIdType.MESH

ORDER = [(0, 0), (0, 1), (0, 3), (1, 0), (3, 0), (0, 2), (2, 0), (1, 1),
         (1, 3), (3, 1), (3, 3), (1, 2), (2, 1), (2, 3), (3, 2), (2, 2)]
PLACE = {block: place for place, block in enumerate(ORDER)}


def packed(values):
    total = sum(v << (2 * k) for k, v in enumerate(values))
    return total - 2 ** 32 if total >= 2 ** 31 else total


ORIGIN_Y, ORIGIN_X = packed([b[0] for b in ORDER]), packed([b[1] for b in ORDER])
QUARTERS = 4
VMEM_A = 45 * 1024 * 1024 + 832 * 1024
VMEM_B = 22 * 1024 * 1024
UNIT_BLOCKS = 4
STEP_BLOCKS = 2
BEFORE = {0: (3,), 3: (7,), 4: (9,), 5: (11,), 6: (13,)}
BETWEEN = {0: (4,), 1: (5,), 2: (6,), 3: (8,)}
LATE = {4: (10,), 5: (12,), 6: (14,)}
NT = (((1,), (1,)), ((), ()))
TN = (((0,), (0,)), ((), ()))


def send_lists():
    flip = (1, 0, 3, 2)
    plus_x = [(0, 0, 1), (0, 0, 0), (0, 0, 2), (0, 0, 3), (0, 1, 0), (0, 1, 2), (1, 0, 3), (1, 0, 2),
              (3, 0, 2), (3, 0, 3), (2, 0, 2), (1, 1, 2), (2, 0, 3), (3, 1, 2), (2, 1, 2)]
    plus_y = [(0, 0, 0), (0, 0, 3), (0, 0, 2), (0, 0, 1), (1, 0, 0), (1, 0, 2), (0, 1, 1), (0, 1, 0),
              (0, 3, 1), (0, 3, 0), (0, 2, 0), (0, 2, 1), (1, 1, 0), (1, 3, 0), (1, 2, 0)]
    minus_x = [(oy, -ox % 4, flip[q]) for oy, ox, q in plus_x]
    minus_y = [(-oy % 4, ox, flip[q]) for oy, ox, q in plus_y]
    return {(0, 1): plus_x, (0, 3): minus_x, (1, 0): plus_y, (3, 0): minus_y}


SENDS = send_lists()
SLOTS = len(SENDS[(0, 1)])


def expert_kernel(group_size, x_hbm, wg_hbm, wu_hbm, wd_hbm, dout_hbm, slots_ref, ids_ref, gates_ref,
                  dadb_hbm, acc_gu, acc_d, grecv, pq_hbm, h_hbm,
                  ag, rt, wgu, wd, xb, db, pq, hb, gsend,
                  w_sem, own_sem, x_sem, spill_sem, fill_sem, dadb_sem,
                  recv_sem, rrecv_sem, send_sem, rsend_sem,
                  srecv_sem, srrecv_sem, ssend_sem, srsend_sem, gsend_sem, grecv_sem):
    side = math.isqrt(group_size // 2)
    me = lax.axis_index('ep')
    core = lax.rem(me, 2)
    my_x = lax.rem(me // 2, side)
    my_y = me // (2 * side)
    e_local, rows_u, model = xb.shape
    rows_s = rows_u // (UNIT_BLOCKS // STEP_BLOCKS)
    ffn = hb.shape[2]
    cap = x_hbm.shape[2]
    tok = ag.shape[2]
    qrows = tok // QUARTERS
    n_blocks = side * side
    units = n_blocks // UNIT_BLOCKS
    steps = n_blocks // STEP_BLOCKS
    per_unit = 2 * UNIT_BLOCKS
    per_step = 2 * STEP_BLOCKS
    tile = 256
    mt_count = model // tile
    dadb = wgu
    ft_count = ffn // tile

    def device(y, x, c):
        return (y * side + x) * 2 + c

    def neighbour(dy, dx):
        return device(lax.rem(my_y + dy, side), lax.rem(my_x + dx, side), core)

    sibling = device(my_y, my_x, 1 - core)

    def origin(p, r):
        oy = lax.shift_right_logical(jnp.int32(ORIGIN_Y), 2 * p) & 3
        ox = lax.shift_right_logical(jnp.int32(ORIGIN_X), 2 * p) & 3
        c = core + r - 2 * core * r
        return device(lax.rem(my_y + side - oy, side), lax.rem(my_x + side - ox, side), c)

    def quarter(r, p, q):
        return ag.at[r, p, pl.ds(q * qrows, qrows)]

    def ici_copy(p_from, p_to, q, to):
        return pltpu.make_async_remote_copy(
            src_ref=quarter(0, p_from, q), dst_ref=quarter(0, p_to, q), send_sem=send_sem,
            recv_sem=recv_sem.at[p_to, q], device_id={'ep': to}, device_id_type=MESH)

    def ici_route(p_from, p_to, to):
        return pltpu.make_async_remote_copy(
            src_ref=rt.at[0, p_from], dst_ref=rt.at[0, p_to], send_sem=rsend_sem,
            recv_sem=rrecv_sem.at[p_to], device_id={'ep': to}, device_id_type=MESH)

    def sib_copy(p, q):
        return pltpu.make_async_remote_copy(
            src_ref=quarter(0, p, q), dst_ref=quarter(1, p, q), send_sem=ssend_sem,
            recv_sem=srecv_sem.at[p, q], device_id={'ep': sibling}, device_id_type=MESH)

    def sib_route(p):
        return pltpu.make_async_remote_copy(
            src_ref=rt.at[0, p], dst_ref=rt.at[1, p], send_sem=srsend_sem,
            recv_sem=srrecv_sem.at[p], device_id={'ep': sibling}, device_id_type=MESH)

    def issue(slot):
        for (dy, dx), sends in SENDS.items():
            oy, ox, q = sends[slot]
            p_from, p_to = PLACE[(oy, ox)], PLACE[((oy + dy) % 4, (ox + dx) % 4)]
            to = neighbour(dy, dx)
            ici_copy(p_from, p_to, q, to).start()
            if q == 0:
                ici_route(p_from, p_to, to).start()

    def service(slot):
        for (dy, dx), sends in SENDS.items():
            oy, ox, q = sends[slot]
            p_to = PLACE[((oy + dy) % 4, (ox + dx) % 4)]
            ici_copy(p_to, p_to, q, me).wait_recv()
            if q == 0:
                ici_route(p_to, p_to, me).wait_recv()
        if slot + 3 < SLOTS:
            issue(slot + 3)
        for (dy, dx), sends in SENDS.items():
            oy, ox, q = sends[slot]
            p_to = PLACE[((oy + dy) % 4, (ox + dx) % 4)]
            sib_copy(p_to, q).start()
            if q == 0:
                sib_route(p_to).start()

    def x_copy(block, j, e, row, sem):
        src = origin(block + j // 2, j % 2)
        return pltpu.make_async_copy(x_hbm.at[src, e], xb.at[e, pl.ds(row + j * cap, cap)], x_sem.at[e, sem + j])

    def unit_x(g, e):
        return [x_copy(g * UNIT_BLOCKS, j, e, 0, 0) for j in range(per_unit)]

    def unit_fill(g, e):
        u = g * e_local + e
        return unit_x(g, e) + [pltpu.make_async_copy(pq_hbm.at[u], pq.at[e], fill_sem.at[e, 0]),
                               pltpu.make_async_copy(h_hbm.at[u], hb.at[e], fill_sem.at[e, 1])]

    def dadb_copy(t, e, j):
        src = origin(t * STEP_BLOCKS + j // 2, j % 2)
        row = pl.multiple_of(lax.rem(t, 2) * rows_s + j * cap, cap)
        return pltpu.make_async_copy(dadb.at[e, pl.ds(row, cap)], dadb_hbm.at[src, e], dadb_sem.at[e, j])

    def spill_copies(u, e):
        return (pltpu.make_async_copy(pq.at[e], pq_hbm.at[u], spill_sem.at[e, 0]),
                pltpu.make_async_copy(hb.at[e], h_hbm.at[u], spill_sem.at[e, 1]))

    w_copies = [pltpu.make_async_copy(wg_hbm, wgu.at[:, :, pl.ds(0, ffn)], w_sem.at[0]),
                pltpu.make_async_copy(wu_hbm, wgu.at[:, :, pl.ds(ffn, ffn)], w_sem.at[1]),
                pltpu.make_async_copy(wd_hbm, wd, w_sem.at[2])]
    own = pltpu.make_async_copy(dout_hbm, ag.at[0, 0], own_sem)

    own.start()
    barrier = pltpu.get_barrier_semaphore()

    partners = [neighbour(dy, dx) for dy, dx in SENDS] + [sibling]
    for to in partners:
        pl.semaphore_signal(barrier, inc=1, device_id={'ep': to}, device_id_type=MESH)

    for c in w_copies[:2]:
        c.start()
    for e in range(e_local):
        for c in unit_x(1, e):
            c.start()
    w_copies[2].start()
    top_k = slots_ref.shape[0]
    rt[0, 0] = jnp.concatenate([jnp.full((8, tok), -1.0, F32), jnp.zeros((8, tok), F32)], axis=0)
    slots = slots_ref[...]
    rt[0, 0, 0:top_k] = jnp.where(slots >= 0, ids_ref[...] * cap + slots, -1).astype(F32)
    rt[0, 0, 8:8 + top_k] = gates_ref[...]
    own.wait()
    pl.semaphore_wait(barrier, len(partners))
    for slot in range(3):
        issue(slot)
    for q in range(QUARTERS):
        sib_copy(0, q).start()
    sib_route(0).start()

    @pl.loop(0, mt_count)
    def _(m):
        rows = pl.ds(pl.multiple_of(m * tile, tile), tile)
        for e in range(e_local):
            acc_gu[e, rows] = jnp.zeros((tile, 2 * ffn), F32)

    @pl.loop(0, ft_count)
    def _(m):
        rows = pl.ds(pl.multiple_of(m * tile, tile), tile)
        for e in range(e_local):
            acc_d[e, rows] = jnp.zeros((tile, model), F32)

    for c in w_copies[:2]:
        c.wait()

    @pl.loop(0, units * e_local)
    def _(u):
        turn, e = u // e_local, lax.rem(u, e_local)
        g = lax.rem(turn + 1, units)
        for c in unit_x(g, e):
            c.wait()

        @pl.when(u >= e_local)
        def _():
            for c in spill_copies(g * e_local + e, e):
                c.wait()

        @pl.loop(0, ft_count)
        def _(n):
            lo = pl.ds(pl.multiple_of(n * tile, tile), tile)
            hi = pl.ds(pl.multiple_of(ffn + n * tile, tile), tile)
            x = xb[e]
            a = jnp.dot(x, wgu[e, :, lo], preferred_element_type=F32)
            b = jnp.dot(x, wgu[e, :, hi], preferred_element_type=F32)
            sg = jax.nn.sigmoid(a)
            silu = a * sg
            hb[e, :, lo] = (silu * b).astype(BF16)
            pq[e, :, lo] = b * sg * (1.0 + a * (1.0 - sg))
            pq[e, :, hi] = silu

        @pl.when(turn + 1 < units)
        def _():
            for c in spill_copies(g * e_local + e, e):
                c.start()
            for c in unit_x(lax.rem(turn + 2, units), e):
                c.start()

        for k, at in ((0, 2), (1, 4), (2, 6)):
            @pl.when(u == at)
            def _(k=k):
                service(k)

    w_copies[2].wait()

    def hits(r, p, e):
        local = rt[r, p, 0:8] - (me * (e_local * cap) + e * cap).astype(F32)
        hit = (local >= 0.0) & (local < float(cap))
        slot = jnp.max(jnp.where(hit, local, -1.0), axis=0, keepdims=True)
        gate = jnp.sum(jnp.where(hit, rt[r, p, 8:16], 0.0), axis=0, keepdims=True)
        return slot, gate

    def on(table, t):
        for step, slots in table.items():
            @pl.when(t == step)
            def _(slots=slots):
                for k in slots:
                    service(k)

    slot_iota = lax.broadcasted_iota(jnp.int32, (cap, tok), 0).astype(F32)

    @pl.loop(0, steps)
    def _(t):
        on(BEFORE, t)
        odd = lax.rem(t, 2)
        half = pl.multiple_of(odd * rows_s, rows_s)
        here = pl.ds(half, rows_s)
        dy_here = pl.ds(pl.multiple_of(rows_s + half, rows_s), rows_s)

        @pl.loop(0, 2)
        def _(r):
            @pl.when(r == 1)
            def _():
                for i in range(STEP_BLOCKS):
                    for q in range(QUARTERS):
                        sib_copy(t * STEP_BLOCKS + i, q).wait_recv()
                    sib_route(t * STEP_BLOCKS + i).wait_recv()

            for i in range(STEP_BLOCKS):
                p = t * STEP_BLOCKS + i
                picks, gates = [], []
                for e in range(e_local):
                    slot, gate = hits(r, p, e)
                    pick = slot_iota == slot
                    gates.append(jnp.sum(jnp.where(pick, gate, 0.0), axis=1, keepdims=True))
                    picks.append(jnp.where(pick, 1.0, 0.0).astype(BF16))
                pick = jnp.concatenate(picks, axis=0)
                row = pl.multiple_of((2 * i + r) * cap, cap)
                for n in range(model // 512):
                    cols = pl.ds(n * 512, 512)
                    d = jnp.dot(pick, ag[r, p, :, cols], preferred_element_type=F32)
                    for e in range(e_local):
                        d_e = d[e * cap:(e + 1) * cap]
                        db[e, pl.ds(row, cap), cols] = d_e.astype(BF16)
                        db[e, pl.ds(pl.multiple_of(rows_s + half + row, cap), cap), cols] = (
                            d_e * gates[e]).astype(BF16)

        @pl.loop(0, e_local)
        def _(e):
            @pl.when((odd == 0) & (t > 0))
            def _():
                for c in unit_fill(t // 2, e):
                    c.wait()

            @pl.when(t > 0)
            def _():
                for j in range(per_step):
                    dadb_copy(t, e, j).wait()

            part = jnp.zeros((rows_s, 128), F32)
            for n in range(ft_count):
                lo, hi = pl.ds(n * tile, tile), pl.ds(ffn + n * tile, tile)
                lhs = jnp.concatenate([db[e, 0:rows_s], db[e, dy_here]], axis=0)
                both = lax.dot_general(lhs, wd[e, lo, :], NT, preferred_element_type=F32)
                prod = hb[e, here, lo].astype(F32) * both[:rows_s]
                part += prod[:, :128] + prod[:, 128:]
                dh = both[rows_s:].astype(BF16).astype(F32)
                dadb[e, here, lo] = (dh * pq[e, here, lo]).astype(BF16)
                dadb[e, here, hi] = (dh * pq[e, here, hi]).astype(BF16)

            total = jnp.broadcast_to(jnp.sum(part, axis=1, keepdims=True), part.shape)
            for j in range(per_step):
                slot, _ = hits(j % 2, t * STEP_BLOCKS + j // 2, e)
                value = jnp.concatenate([total[j * cap:(j + 1) * cap]] * (tok // 128), axis=1)
                gsend[t * per_step + j, e] = jnp.sum(
                    jnp.where(slot_iota == slot, value, 0.0), axis=0, keepdims=True)

            for j in range(per_step):
                dadb_copy(t, e, j).start()

            @pl.when((t == 0) & (e == e_local - 1))
            def _():
                grecv[me] = gsend[0]

            @pl.when(e == e_local - 1)
            def _():
                @pl.loop(jnp.where(t == 0, 1, 0), per_step)
                def _(j):
                    to = origin(t * STEP_BLOCKS + j // 2, lax.rem(j, 2))
                    pltpu.make_async_remote_copy(
                        src_ref=gsend.at[t * per_step + j], dst_ref=grecv.at[me], send_sem=gsend_sem,
                        recv_sem=grecv_sem, device_id={'ep': to}, device_id_type=MESH).start()

            def weight_grads(rows, dy_rows):
                @pl.loop(0, 2)
                def _(m):
                    out = pl.ds(pl.multiple_of(m * (model // 2), model // 2), model // 2)
                    for n in range(2):
                        cols = pl.ds(n * ffn, ffn)
                        acc_gu[e, out, cols] += lax.dot_general(
                            xb[e, rows, out], dadb[e, rows, cols], TN, preferred_element_type=F32)

                for n in range(model // 512):
                    cols = pl.ds(n * 512, 512)
                    acc_d[e, :, cols] += lax.dot_general(
                        hb[e, rows, :], db[e, dy_rows, cols], TN, preferred_element_type=F32)

            for step, slots in LATE.items():
                @pl.when((t == step) & (e == e_local - 1))
                def _(slots=slots):
                    for k in slots:
                        service(k)

            @pl.when(odd == 1)
            def _():
                weight_grads(pl.ds(0, rows_u), pl.ds(rows_s, rows_u))

            @pl.when((odd == 1) & (t < steps - 1))
            def _():
                for c in unit_fill(t // 2 + 1, e):
                    c.start()

            for step, slots in BETWEEN.items():
                @pl.when((t == step) & (e == 0))
                def _(slots=slots):
                    for k in slots:
                        service(k)


    def drain(ref, sem):
        pltpu.make_async_copy(ref, ref, sem).wait()

    drain(ag.at[0, pl.ds(0, n_blocks - 1)], send_sem)
    drain(rt.at[0, pl.ds(0, n_blocks - 1)], rsend_sem)
    drain(ag.at[0], ssend_sem)
    drain(rt.at[0], srsend_sem)
    drain(gsend.at[pl.ds(0, group_size - 1)], gsend_sem)
    drain(grecv.at[pl.ds(0, group_size - 1)], grecv_sem)
    for e in range(e_local):
        for j in range(per_step):
            dadb_copy(jnp.int32(steps - 1), e, j).wait()


def run_experts(x_disp, w_gate, w_up, w_down, d_out, slots, ids, gates, group_size):
    sources, e_local, cap, model = x_disp.shape
    ffn = w_gate.shape[2]
    tok = d_out.shape[0]
    n_blocks = group_size // 2
    per_unit = 2 * UNIT_BLOCKS
    rows_u = per_unit * cap
    per_step = 2 * STEP_BLOCKS
    rows_s = per_step * cap
    units = n_blocks // UNIT_BLOCKS * e_local
    dma = pltpu.SemaphoreType.DMA
    any_spec = pl.BlockSpec(memory_space=pl.ANY)
    vmem_spec = pl.BlockSpec(memory_space=pltpu.VMEM)
    out_shape = [
        jax.ShapeDtypeStruct((sources, e_local, cap, 2 * ffn), BF16),
        pltpu.VMEM((e_local, model, 2 * ffn), F32),
        pltpu.VMEM((e_local, ffn, model), F32),
        pltpu.VMEM((group_size, e_local, 1, tok), F32),
        jax.ShapeDtypeStruct((units, rows_u, 2 * ffn), F32),
        jax.ShapeDtypeStruct((units, rows_u, ffn), BF16),
    ]
    scratch = [
        pltpu.VMEM((2, n_blocks, tok, model), BF16),
        pltpu.VMEM((2, n_blocks, 16, tok), F32),
        pltpu.VMEM((e_local, model, 2 * ffn), BF16),
        pltpu.VMEM((e_local, ffn, model), BF16),
        pltpu.VMEM((e_local, rows_u, model), BF16),
        pltpu.VMEM((e_local, rows_s + rows_u, model), BF16),
        pltpu.VMEM((e_local, rows_u, 2 * ffn), F32),
        pltpu.VMEM((e_local, rows_u, ffn), BF16),
        pltpu.VMEM((group_size, e_local, 1, tok), F32),
        dma((3,)), dma, dma((e_local, per_unit)), dma((e_local, 2)), dma((e_local, 2)),
        dma((e_local, per_step)),
        dma((n_blocks, QUARTERS)), dma((n_blocks,)), dma, dma,
        dma((n_blocks, QUARTERS)), dma((n_blocks,)), dma, dma, dma, dma,
    ]
    return pl.pallas_call(
        functools.partial(expert_kernel, group_size),
        out_shape=out_shape, in_specs=[any_spec] * 5 + [vmem_spec] * 3,
        out_specs=[any_spec, vmem_spec, vmem_spec, vmem_spec, any_spec, any_spec], scratch_shapes=scratch,
        compiler_params=pltpu.CompilerParams(collective_id=0, has_side_effects=True, vmem_limit_bytes=VMEM_A),
    )(x_disp, w_gate, w_up, w_down, d_out, slots, ids, gates)


def finish_kernel(group_size, chunk, dadb, wg, wu, back, acc_gu, acc_d, ids, slots,
                  gx, g_gate, g_up, g_down, gate_out,
                  wbuf, dbuf, obuf, st_g, st_u, st_d, w_sem, d_sem, o_sem, s_sem):
    sources, e_local, cap, width = dadb.shape
    ffn = width // 2
    model = gx.shape[3]
    per_e = sources // chunk
    chunks = e_local * per_e
    m_blk, f_blk = model // per_e, ffn // per_e
    depth = dbuf.shape[0]

    def load(c):
        slot = lax.rem(c, depth)
        return pltpu.make_async_copy(
            dadb.at[pl.ds(lax.rem(c, per_e) * chunk, chunk), c // per_e], dbuf.at[slot], d_sem.at[slot])

    def store(c):
        slot = lax.rem(c, 2)
        return pltpu.make_async_copy(
            obuf.at[slot], gx.at[pl.ds(lax.rem(c, per_e) * chunk, chunk), c // per_e], o_sem.at[slot])

    def weights(e):
        return [pltpu.make_async_copy(wg.at[e], wbuf.at[e, :, pl.ds(0, ffn)], w_sem.at[e, 0]),
                pltpu.make_async_copy(wu.at[e], wbuf.at[e, :, pl.ds(ffn, ffn)], w_sem.at[e, 1])]

    def staged(c):
        e, i = c // per_e, lax.rem(c, per_e)
        m = pl.ds(pl.multiple_of(i * m_blk, m_blk), m_blk)
        f = pl.ds(pl.multiple_of(i * f_blk, f_blk), f_blk)
        return e, m, f, [pltpu.make_async_copy(st_g.at[e, m], g_gate.at[e, m], s_sem.at[c, 0]),
                         pltpu.make_async_copy(st_u.at[e, m], g_up.at[e, m], s_sem.at[c, 1]),
                         pltpu.make_async_copy(st_d.at[e, f], g_down.at[e, f], s_sem.at[c, 2])]

    for c in weights(0):
        c.start()
    for k in range(depth):
        load(jnp.int32(k)).start()
    for e in range(1, e_local):
        for c in weights(e):
            c.start()

    def cast(c):
        e, m, f, copies = staged(c)
        st_g[e, m] = acc_gu[e, m, 0:ffn].astype(BF16)
        st_u[e, m] = acc_gu[e, m, ffn:width].astype(BF16)
        st_d[e, f] = acc_d[e, f].astype(BF16)
        return copies

    @pl.loop(0, chunks)
    def _(c):
        e = c // per_e

        @pl.when(lax.rem(c, per_e) == 0)
        def _():
            for w in weights(e):
                w.wait()

        load(c).wait()

        @pl.when(c >= 2)
        def _():
            store(c - 2).wait()

        slot, out_slot = lax.rem(c, depth), lax.rem(c, 2)
        copies = cast(c)
        both = dbuf[slot].reshape(chunk * cap, width)
        for n in range(model // 512):
            rows = pl.ds(n * 512, 512)
            out = lax.dot_general(both, wbuf[e, rows], NT, preferred_element_type=F32)
            obuf[out_slot, :, :, rows] = out.astype(BF16).reshape(chunk, cap, 512)
        store(c).start()
        for s in copies:
            s.start()

        @pl.when(c + depth < chunks)
        def _():
            load(c + depth).start()

    total = jnp.zeros(gate_out.shape, F32)
    for d in range(group_size):
        for e in range(e_local):
            total += jnp.where(ids[...] == d * e_local + e, back[d, e], 0.0)
    gate_out[...] = jnp.where(slots[...] >= 0, total, 0.0)

    for c in range(chunks - 2, chunks):
        store(jnp.int32(c)).wait()
    for c in range(chunks):
        for s in staged(jnp.int32(c))[3]:
            s.wait()


def run_finish(dadb, w_gate, w_up, acc_gu, acc_d, back, ids, slots, group_size):
    sources, e_local, cap, width = dadb.shape
    model, ffn = w_gate.shape[1:]
    top_k, tok = ids.shape
    chunk = 8
    dma = pltpu.SemaphoreType.DMA
    any_spec = pl.BlockSpec(memory_space=pl.ANY)
    vmem_spec = pl.BlockSpec(memory_space=pltpu.VMEM)
    return pl.pallas_call(
        functools.partial(finish_kernel, group_size, chunk),
        in_specs=[any_spec] * 3 + [vmem_spec] * 5,
        out_specs=[any_spec] * 4 + [vmem_spec],
        out_shape=[
            jax.ShapeDtypeStruct((sources, e_local, cap, model), BF16),
            jax.ShapeDtypeStruct((e_local, model, ffn), BF16),
            jax.ShapeDtypeStruct((e_local, model, ffn), BF16),
            jax.ShapeDtypeStruct((e_local, ffn, model), BF16),
            jax.ShapeDtypeStruct((top_k, tok), F32),
        ],
        scratch_shapes=[
            pltpu.VMEM((e_local, model, width), BF16),
            pltpu.VMEM((3, chunk, cap, width), BF16),
            pltpu.VMEM((2, chunk, cap, model), BF16),
            pltpu.VMEM((e_local, model, ffn), BF16),
            pltpu.VMEM((e_local, model, ffn), BF16),
            pltpu.VMEM((e_local, ffn, model), BF16),
            dma((e_local, 2)), dma((3,)), dma((2,)), dma((e_local * sources // chunk, 3)),
        ],
        compiler_params=pltpu.CompilerParams(vmem_limit_bytes=VMEM_B),
    )(*[pltpu.with_memory_space_constraint(a, pltpu.HBM) for a in (dadb, w_gate, w_up)],
      *[pltpu.with_memory_space_constraint(a, pltpu.VMEM) for a in (back, acc_gu, acc_d)], ids, slots)


def solution(mesh):
    group_size = mesh.shape['ep']

    def local_step(x_disp, w_gate, w_up, w_down, d_out, slot_idx, expert_id, gate_wt):
        slots, ids = slot_idx.T, expert_id.T
        dadb, acc_gu, acc_d, back, _, _ = run_experts(
            x_disp, w_gate, w_up, w_down, d_out, slots, ids, gate_wt.T, group_size)
        grad_x, grad_w_gate, grad_w_up, grad_w_down, gate = run_finish(
            dadb, w_gate, w_up, acc_gu, acc_d, back, ids, slots, group_size)
        return grad_x, grad_w_gate, grad_w_up, grad_w_down, gate.T

    token_place = P(('dp', 'ep'), None)
    weight_place = P('ep', None, None)
    slot_place = P('dp', 'ep', None, None)
    grad_place = P(('dp', 'ep'), None, None)
    return jax.shard_map(local_step, mesh=mesh,
                         in_specs=(slot_place, weight_place, weight_place, weight_place, token_place, token_place, token_place, token_place),
                         out_specs=(slot_place, grad_place, grad_place, grad_place, token_place),
                         check_vma=False)
```
